16 devices in a mesh: dp: 4 (over z, y), tp: 4 (over x, core).
Axes of the slice: x: 2, y: 2, z: 2, core: 2. Of those that a mesh axis runs over, the one named last changes fastest.
Arguments:
- tokens: int32 [4, 128], P('dp'), parts along dimension 0
- positions: int32 [4, 128], P('dp'), parts along dimension 0
- embedding: bfloat16 [8192, 2048], P('tp')
- gain_attn: float32 [2048], replicated
- gain_mlp: float32 [2048], replicated
- w_query: bfloat16 [2048, 32, 64], P(None, 'tp')
- w_key: bfloat16 [2048, 8, 64], P(None, 'tp')
- w_value: bfloat16 [2048, 8, 64], P(None, 'tp')
- w_out: bfloat16 [32, 64, 2048], P('tp')
- w_gate: bfloat16 [2048, 8192], P(None, 'tp')
- w_up: bfloat16 [2048, 8192], P(None, 'tp')
- w_down: bfloat16 [8192, 2048], P('tp')
- grad_hidden: bfloat16 [4, 128, 2048], P('dp', 'tp'), parts along dimension 0
Outputs:
- output 1: bfloat16 [4, 128, 2048], P('dp', 'tp'), parts along dimension 0
- output 2: float32 [32768, 2048], P(('dp', 'tp')), parts along dimension 0
- output 3: float32 [8192, 32, 64], P('dp', 'tp'), parts along dimension 0
- output 4: float32 [8192, 8, 64], P('dp', 'tp'), parts along dimension 0
- output 5: float32 [8192, 8, 64], P('dp', 'tp'), parts along dimension 0
- output 6: float32 [128, 64, 2048], P(('dp', 'tp')), parts along dimension 0
- output 7: float32 [8192, 8192], P('dp', 'tp'), parts along dimension 0
- output 8: float32 [8192, 8192], P('dp', 'tp'), parts along dimension 0
- output 9: float32 [32768, 2048], P(('dp', 'tp')), parts along dimension 0
- output 10: float32 [8192], P('dp'), parts along dimension 0
- output 11: float32 [8192], P('dp'), parts along dimension 0
There are 4 independent parts. The reference program is written for one: setup_inputs(seed, part) draws one part's arguments, and reference() takes and returns one part's arrays. A program takes and returns all parts, laid end to end along the dimension named above; an argument that names none is the same for every part.
All inputs are finite; a program needn't handle non-finite values.
Results may differ from the reference program's by a relative error of at most 0.0182023.
Values are sent between devices in bfloat16 or wider.
A program may use at most 1 GiB of HBM per device.

```python
import jax
import jax.numpy as jnp
from jax import lax

BATCH_SIZE = 1
SEQ_LEN = 128
VOCAB_SIZE = 8192
MODEL_DIM = 2048
NUM_HEADS = 32
KV_HEADS = 8
HEAD_DIM = 64
FFN_DIM = 8192
HOT_COUNT = 16
ROPE_THETA = 1000000.0
RMS_EPS = 1e-5


def draw_tokens(rng_key):
    sub_keys = jax.random.split(rng_key, 7)
    tok_shape = (BATCH_SIZE, SEQ_LEN)
    first_draw = jax.random.randint(sub_keys[0], tok_shape, 0, VOCAB_SIZE)
    second_draw = jax.random.randint(sub_keys[1], tok_shape, 0, VOCAB_SIZE)
    base_ids = jnp.minimum(first_draw, second_draw)
    hot_ids = jax.random.randint(sub_keys[2], (HOT_COUNT,), 0, VOCAB_SIZE)
    hot_pick = jax.random.randint(sub_keys[3], tok_shape, 0, HOT_COUNT)
    use_hot = jax.random.randint(sub_keys[4], tok_shape, 0, 4) == 0
    token_ids = jnp.where(use_hot, hot_ids[hot_pick], base_ids)
    top_place = jax.random.randint(sub_keys[5], (), 0, SEQ_LEN // 2)
    low_place = jax.random.randint(sub_keys[6], (), SEQ_LEN // 2, SEQ_LEN)
    token_ids = token_ids.at[0, top_place].set(VOCAB_SIZE - 1)
    token_ids = token_ids.at[0, low_place].set(0)
    return token_ids.astype(jnp.int32)


def draw_positions(rng_key):
    pos_steps = jax.random.randint(rng_key, (BATCH_SIZE, SEQ_LEN), 1, 4)
    return jnp.cumsum(pos_steps, axis=1).astype(jnp.int32)


def scaled_normal(rng_key, dim_shape, factor):
    return (jax.random.normal(rng_key, dim_shape, jnp.float32) * factor).astype(jnp.bfloat16)


def setup_inputs(seed: int = 0, part: int = 0) -> dict:
    shared = jax.random.split(jax.random.key(seed), 10)
    part_keys = jax.random.split(jax.random.fold_in(jax.random.key(seed + 1), part), 3)
    in_scale = MODEL_DIM ** -0.5
    return {
        'tokens': draw_tokens(part_keys[0]),
        'positions': draw_positions(part_keys[1]),
        'embedding': scaled_normal(shared[0], (VOCAB_SIZE, MODEL_DIM), 1.0),
        'gain_attn': 1.0 + 0.25 * jax.random.normal(shared[1], (MODEL_DIM,), jnp.float32),
        'gain_mlp': 1.0 + 0.25 * jax.random.normal(shared[2], (MODEL_DIM,), jnp.float32),
        'w_query': scaled_normal(shared[3], (MODEL_DIM, NUM_HEADS, HEAD_DIM), in_scale),
        'w_key': scaled_normal(shared[4], (MODEL_DIM, KV_HEADS, HEAD_DIM), in_scale),
        'w_value': scaled_normal(shared[5], (MODEL_DIM, KV_HEADS, HEAD_DIM), in_scale),
        'w_out': scaled_normal(shared[6], (NUM_HEADS, HEAD_DIM, MODEL_DIM), (NUM_HEADS * HEAD_DIM) ** -0.5),
        'w_gate': scaled_normal(shared[7], (MODEL_DIM, FFN_DIM), in_scale),
        'w_up': scaled_normal(shared[8], (MODEL_DIM, FFN_DIM), in_scale),
        'w_down': scaled_normal(shared[9], (FFN_DIM, MODEL_DIM), FFN_DIM ** -0.5),
        'grad_hidden': scaled_normal(part_keys[2], (BATCH_SIZE, SEQ_LEN, MODEL_DIM), 1.0),
    }


def rope_tables(positions, head_dim):
    half_dim = head_dim // 2
    inv_freq = ROPE_THETA ** (-jnp.arange(half_dim, dtype=jnp.float32) * (2.0 / head_dim))
    angles = positions.astype(jnp.float32)[:, :, None] * inv_freq
    return jnp.cos(angles)[:, :, None, :], jnp.sin(angles)[:, :, None, :]


def rotate(values, cos_tab, sin_tab):
    half_dim = values.shape[-1] // 2
    first_half = values[..., :half_dim]
    second_half = values[..., half_dim:]
    return jnp.concatenate([first_half * cos_tab - second_half * sin_tab, second_half * cos_tab + first_half * sin_tab], axis=-1)


def rms_norm(hidden, gain_vec):
    hidden_f = hidden.astype(jnp.float32)
    inv_rms = lax.rsqrt(jnp.mean(hidden_f * hidden_f, axis=-1, keepdims=True) + RMS_EPS)
    return (hidden_f * inv_rms * gain_vec).astype(jnp.bfloat16)


def layer(first_x, gain_pair, weight_mats, positions):
    w_query, w_key, w_value, w_out, w_gate, w_up, w_down = weight_mats
    batch_size, seq_len = positions.shape
    num_heads, head_dim = w_query.shape[1], w_query.shape[2]
    kv_heads = w_key.shape[1]
    group_size = num_heads // kv_heads
    cos_tab, sin_tab = rope_tables(positions, head_dim)
    normed1 = rms_norm(first_x, gain_pair[0]).astype(jnp.float32)
    queries = rotate(jnp.einsum('bsd,dhe->bshe', normed1, w_query), cos_tab, sin_tab)
    queries = queries.astype(jnp.bfloat16).astype(jnp.float32).reshape(batch_size, seq_len, kv_heads, group_size, head_dim)
    keys_rot = rotate(jnp.einsum('bsd,dhe->bshe', normed1, w_key), cos_tab, sin_tab).astype(jnp.bfloat16).astype(jnp.float32)
    values = jnp.einsum('bsd,dhe->bshe', normed1, w_value).astype(jnp.bfloat16).astype(jnp.float32)
    causal = jnp.arange(seq_len)[:, None] >= jnp.arange(seq_len)[None, :]
    scores = jnp.einsum('bqkgd,bskd->bkgqs', queries, keys_rot) * head_dim ** -0.5
    probs_f = jax.nn.softmax(jnp.where(causal, scores, -1e30), axis=-1)
    probs_r = probs_f.astype(jnp.bfloat16).astype(jnp.float32)
    attn_heads = jnp.einsum('bkgqs,bskd->bqkgd', probs_r, values).astype(jnp.bfloat16).astype(jnp.float32)
    attn_heads = attn_heads.reshape(batch_size, seq_len, num_heads, head_dim)
    attn_out = jnp.einsum('bshe,hed->bsd', attn_heads, w_out)
    hidden1 = (first_x.astype(jnp.float32) + attn_out).astype(jnp.bfloat16)
    normed2 = rms_norm(hidden1, gain_pair[1]).astype(jnp.float32)
    gate_pre = jnp.einsum('bsd,df->bsf', normed2, w_gate)
    up_pre = jnp.einsum('bsd,df->bsf', normed2, w_up)
    act_r = (jax.nn.silu(gate_pre) * up_pre).astype(jnp.bfloat16).astype(jnp.float32)
    mlp_out = jnp.einsum('bsf,fd->bsd', act_r, w_down)
    return (hidden1.astype(jnp.float32) + mlp_out).astype(jnp.bfloat16)


def reference(tokens, positions, embedding, gain_attn, gain_mlp, w_query, w_key, w_value, w_out, w_gate, w_up, w_down, grad_hidden):
    first_x = jnp.take(embedding, tokens, axis=0)
    weight_mats = tuple(weight.astype(jnp.float32) for weight in (w_query, w_key, w_value, w_out, w_gate, w_up, w_down))
    hidden_out, back_fn = jax.vjp(lambda x_in, gain_pair, mats_in: layer(x_in, gain_pair, mats_in, positions), first_x, (gain_attn, gain_mlp), weight_mats)
    grad_x, grad_gains, grad_mats = back_fn(grad_hidden)
    grad_embedding = jax.ops.segment_sum(grad_x.reshape(-1, MODEL_DIM).astype(jnp.float32), tokens.reshape(-1), num_segments=VOCAB_SIZE)
    return (hidden_out, grad_embedding, grad_mats[0], grad_mats[1], grad_mats[2], grad_mats[3], grad_mats[4], grad_mats[5], grad_mats[6], grad_gains[0], grad_gains[1])
```

```python
import functools

import jax
import jax.numpy as jnp
import numpy as np
from jax import lax
from jax.experimental import pallas as pl
from jax.experimental.pallas import tpu as pltpu
from jax.sharding import PartitionSpec as P

ROPE_THETA = 1000000.0
RMS_EPS = 1e-5
MESH = pl.DeviceIdType.MESH
BF = jnp.bfloat16
F32 = jnp.float32

SEQ = 128
DIM = 2048
VLOC = 2048
FLOC = 2048
HLOC = 8
KVLOC = 2
HD = 64
QC = HLOC * HD
KC = KVLOC * HD
QKV = QC + 2 * KC
GROUP = HLOC // KVLOC
SCALE = HD ** -0.5
NC = 4
W = DIM // NC
VMEM = pltpu.VMEM
HBM = pltpu.HBM


def nn(a, b):
    return lax.dot_general(a, b, (((1,), (0,)), ((), ())), preferred_element_type=F32)


def nt(a, b):
    return lax.dot_general(a, b, (((1,), (1,)), ((), ())), preferred_element_type=F32)


def tn(a, b):
    return lax.dot_general(a, b, (((0,), (0,)), ((), ())), preferred_element_type=F32)


def place():
    tp = lax.axis_index("tp")
    x = tp // 2
    c = tp - 2 * x
    return x, c, 2 * x + (1 - c), 2 * (1 - x) + c


def greet(*peers):
    sem = pltpu.get_barrier_semaphore()
    for peer in peers:
        pl.semaphore_signal(sem, inc=1, device_id={"tp": peer}, device_id_type=MESH)
    pl.semaphore_wait(sem, len(peers))


def remote(src, dst, send, recv, peer):
    return pltpu.make_async_remote_copy(
        src_ref=src, dst_ref=dst, send_sem=send, recv_sem=recv, device_id={"tp": peer}, device_id_type=MESH)


def cols(j):
    return pl.ds(pl.multiple_of(j * W, W), W)


class PairSum:
    def __init__(self, part, got, own, sems, c, partner):
        self.part, self.got, self.own, self.c, self.partner = part, got, own, c, partner
        self.send, self.recv = sems

    def copy(self, j):
        return remote(self.part.at[:, 1 - self.c, :, cols(j)], self.got.at[:, :, cols(j)],
                      self.send.at[j], self.recv.at[j], self.partner)

    def put(self, j, value):
        self.part[:, :, :, cols(j)] = value.astype(BF).reshape(2, 2, 32, W)
        self.copy(j).start()

    def take(self, j):
        self.copy(j).wait_recv()
        total = self.part[:, self.c, :, cols(j)].astype(F32) + self.got[:, :, cols(j)].astype(F32)
        self.own[:, :, cols(j)] = total.astype(BF)

    def run(self, chunk, then=lambda j: None):
        def body(j, carry):
            self.put(j, chunk(j))

            @pl.when(j > 0)
            def _():
                self.take(j - 1)
                then(j - 1)
            return carry
        lax.fori_loop(0, NC, body, 0)
        self.take(NC - 1)
        then(NC - 1)

    def drain(self):
        for j in range(NC):
            self.copy(j).wait_send()


def rows16(fn):
    for b in range(2):
        for r in range(0, 32, 16):
            fn(b, slice(r, r + 16))


def norm_rows(x, gain):
    inv = lax.rsqrt(jnp.mean(x * x, axis=-1, keepdims=True) + RMS_EPS)
    return (x * inv * gain).astype(BF)


def norm_back(grad, x, gain):
    inv = lax.rsqrt(jnp.mean(x * x, axis=-1, keepdims=True) + RMS_EPS)
    normed = x * inv
    scaled = grad * gain
    back = inv * (scaled - normed * jnp.mean(scaled * normed, axis=-1, keepdims=True))
    return back, jnp.sum(grad * normed, axis=0, keepdims=True)


def spread(row):
    return jnp.transpose(jnp.broadcast_to(row, (SEQ, SEQ)))


def rope_pair(values, cos_tab, sin_tab):
    lane = lax.broadcasted_iota(jnp.int32, (SEQ, 128), 1)
    low = (lane % HD) < HD // 2
    other = jnp.where(low, pltpu.roll(values, 128 - HD // 2, 1), pltpu.roll(values, HD // 2, 1))
    return values * cos_tab + other * jnp.where(low, -sin_tab, sin_tab)


def probs_of(q, k):
    scores = nt(q, k) * SCALE
    causal = (lax.broadcasted_iota(jnp.int32, (SEQ, SEQ), 0) >= lax.broadcasted_iota(jnp.int32, (SEQ, SEQ), 1))
    scores = jnp.where(causal, scores, -1e30)
    e = jnp.exp(scores - jnp.max(scores, axis=-1, keepdims=True))
    return e / jnp.sum(e, axis=-1, keepdims=True)


def front_kernel(tok, pos, freq, gain_a, gain_m, gh, emb, wq, wk, wv, wo, wd, wg, wu,
                 n1_o, x0_o, qkv_o, cs_o, heads_o, h1_o, n2_o, act_o, ggate_o, gup_o, gfull_o, gn2_o, mlp_o,
                 emb_v, wqkv_v, wo_v, wd_v, wg_v, wu_v, hot_v, gact_v,
                 p0, g0, s0, r0, p1, g1, s1, r1, p2, g2, p3, g3,
                 emb_sem, w_sem, ps, pr, xs, xr, hs, hr, qs, qr):
    x, c, partner, cross = place()
    tp = 2 * x + c

    def fetch_emb(j):
        return pltpu.make_async_copy(emb.at[:, cols(j)], emb_v.at[:, cols(j)], emb_sem.at[j])

    fetches = (
        pltpu.make_async_copy(wq, wqkv_v.at[pl.ds(0, QC)], w_sem.at[0]),
        pltpu.make_async_copy(wk, wqkv_v.at[pl.ds(QC, KC)], w_sem.at[1]),
        pltpu.make_async_copy(wv, wqkv_v.at[pl.ds(QC + KC, KC)], w_sem.at[2]),
        pltpu.make_async_copy(wo, wo_v, w_sem.at[3]),
        pltpu.make_async_copy(wd, wd_v, w_sem.at[4]),
        pltpu.make_async_copy(wg, wg_v, w_sem.at[5]),
        pltpu.make_async_copy(wu, wu_v, w_sem.at[6]),
    )
    for j in range(NC):
        fetch_emb(j).start()
    greet(partner, cross)

    ids = spread(tok[...].astype(F32))
    base = (tp * VLOC).astype(F32)
    lane = lax.broadcasted_iota(jnp.int32, (SEQ, 128), 1).astype(F32)
    for v in range(VLOC // 128):
        hot_v[:, v * 128:(v + 1) * 128] = jnp.where(ids == lane + (base + float(v * 128)), 1.0, 0.0).astype(BF)

    def cross_copy(k, src, dst, j):
        return remote(src.at[:, :, cols(j)], dst.at[:, :, cols(j)], xs.at[k, j], xr.at[k, j], cross)

    sum0 = PairSum(p0, g0, s0, (ps.at[0], pr.at[0]), c, partner)

    def lookup(j):
        fetch_emb(j).wait()
        return nn(hot_v[...], emb_v[:, cols(j)])

    sum0.run(lookup, lambda j: cross_copy(0, s0, r0, j).start())
    for f in fetches:
        f.start()
    gfull_o[x, c] = gh[...]
    to_cross = remote(gh, gfull_o.at[x, c], hs.at[0], hr.at[0], cross)
    to_partner = remote(gh, gfull_o.at[x, c], hs.at[1], hr.at[1], partner)
    to_cross.start()
    to_partner.start()
    angle = spread(pos[...].astype(F32)) * freq[...]
    cs_o[0] = jnp.cos(angle)
    cs_o[1] = jnp.sin(angle)

    for j in range(NC):
        cross_copy(0, s0, r0, j).wait_recv()

    def first(b, r):
        xv = s0[b, r].astype(F32) + r0[b, r].astype(F32)
        x0_o[b, r] = xv.astype(BF)
        n1_o[b, c, r] = norm_rows(xv, gain_a[...])
    rows16(first)
    share1 = remote(n1_o.at[:, c], n1_o.at[:, c], hs.at[2], hr.at[2], partner)
    share1.start()
    for f in fetches[:3]:
        f.wait()
    share1.wait_recv()

    n1 = n1_o[...].reshape(SEQ, DIM)
    cos_tab, sin_tab = cs_o[0], cs_o[1]

    for v in range(QKV // 256):
        lin = nt(n1, wqkv_v[v * 256:(v + 1) * 256, :])
        for h in range(2):
            lo = v * 256 + h * 128
            piece = lin[:, h * 128:(h + 1) * 128]
            if lo < QC + KC:
                piece = rope_pair(piece, cos_tab, sin_tab)
            qkv_o[:, lo:lo + 128] = piece.astype(BF)
    for pair in range(HLOC // 2):
        outs = []
        for h in (2 * pair, 2 * pair + 1):
            g = h // GROUP
            k = qkv_o[:, QC + g * HD:QC + (g + 1) * HD]
            v = qkv_o[:, QC + KC + g * HD:QC + KC + (g + 1) * HD]
            probs = probs_of(qkv_o[:, h * HD:(h + 1) * HD], k).astype(BF)
            outs.append(nn(probs, v).astype(BF))
        heads_o[:, pair * 128:(pair + 1) * 128] = jnp.concatenate(outs, axis=1)
    to_cross.wait_recv()
    onward = remote(gfull_o.at[1 - x, c], gfull_o.at[1 - x, c], hs.at[3], hr.at[3], partner)
    onward.start()
    fetches[3].wait()

    sum1 = PairSum(p1, g1, s1, (ps.at[1], pr.at[1]), c, partner)
    sum1.run(lambda j: nn(heads_o[...], wo_v[:, cols(j)]), lambda j: cross_copy(1, s1, r1, j).start())

    to_partner.wait_recv()
    onward.wait_recv()
    fetches[4].wait()
    gfull = gfull_o[...].reshape(SEQ, DIM)

    def grad_act(j, carry):
        gact_v[:, cols(j)] = nt(gfull, wd_v[pl.ds(pl.multiple_of(j * W, W), W), :]).astype(BF)
        return carry
    lax.fori_loop(0, FLOC // W, grad_act, 0)

    for j in range(NC):
        cross_copy(1, s1, r1, j).wait_recv()

    def second(b, r):
        total = s1[b, r].astype(F32) + r1[b, r].astype(F32)
        h1 = (x0_o[b, r].astype(F32) + total).astype(BF)
        h1_o[b, r] = h1
        n2_o[b, c, r] = norm_rows(h1.astype(F32), gain_m[...])
    rows16(second)
    share2 = remote(n2_o.at[:, c], n2_o.at[:, c], hs.at[4], hr.at[4], partner)
    share2.start()
    fetches[5].wait()
    fetches[6].wait()
    share2.wait_recv()
    n2 = n2_o[...].reshape(SEQ, DIM)

    def mlp(j, carry):
        cj = pl.ds(pl.multiple_of(j * 256, 256), 256)
        gate = nn(n2, wg_v[:, cj])
        up = nn(n2, wu_v[:, cj])
        sig = jax.nn.sigmoid(gate)
        gate_act = gate * sig
        act_o[:, cj] = (gate_act * up).astype(BF)
        grad = gact_v[:, cj].astype(F32)
        gup_o[:, cj] = (grad * gate_act).astype(BF)
        ggate_o[:, cj] = (grad * up * sig * (1.0 + gate * (1.0 - sig))).astype(BF)
        return carry
    lax.fori_loop(0, FLOC // 256, mlp, 0)

    sum2 = PairSum(p2, g2, gn2_o, (ps.at[2], pr.at[2]), c, partner)

    def back_n2(j):
        rj = pl.ds(pl.multiple_of(j * W, W), W)
        return nt(ggate_o[...], wg_v[rj, :]) + nt(gup_o[...], wu_v[rj, :])
    sum2.run(back_n2)
    sum3 = PairSum(p3, g3, mlp_o, (ps.at[3], pr.at[3]), c, partner)
    sum3.run(lambda j: nn(act_o[...], wd_v[:, cols(j)]))

    for s in (sum0, sum1, sum2, sum3):
        s.drain()
    for j in range(NC):
        cross_copy(0, s0, r0, j).wait_send()
        cross_copy(1, s1, r1, j).wait_send()
    for copy in (to_cross, to_partner, share1, onward, share2):
        copy.wait_send()


def middle_kernel(gn2_own, gn2_got, mlp, h1, gfull, gain_m, qkv, cs, wq, wk, wv, wo,
                  gh1_o, gqkv_o, gn1_o, hid_o, gain_o,
                  wqkv_v, wo_v, gheads_v, mlp_got, p0, g0,
                  w_sem, ps, pr, hs, hr):
    x, c, partner, cross = place()
    fetches = (
        pltpu.make_async_copy(wo, wo_v, w_sem.at[3]),
        pltpu.make_async_copy(wq, wqkv_v.at[pl.ds(0, QC)], w_sem.at[0]),
        pltpu.make_async_copy(wk, wqkv_v.at[pl.ds(QC, KC)], w_sem.at[1]),
        pltpu.make_async_copy(wv, wqkv_v.at[pl.ds(QC + KC, KC)], w_sem.at[2]),
    )
    for f in fetches:
        f.start()
    greet(partner, cross)
    out_send = remote(mlp.at[1 - x], mlp_got, hs.at[0], hr.at[0], cross)
    out_send.start()

    gains = []

    def first(b, r):
        grad = (gn2_own[b, r].astype(F32) + gn2_got[b, r].astype(F32)).astype(BF).astype(F32)
        back, part = norm_back(grad, h1[b, r].astype(F32), gain_m[...])
        gh1_o[b, c, r] = (gfull[b, c, r].astype(F32) + back).astype(BF)
        gains.append(part)
    rows16(first)
    share = remote(gh1_o.at[:, c], gh1_o.at[:, c], hs.at[1], hr.at[1], partner)
    share.start()
    gain_o[...] = gains[0] + gains[1] + gains[2] + gains[3]
    fetches[0].wait()
    share.wait_recv()

    gh1 = gh1_o[...].reshape(SEQ, DIM)
    for v in range(QC // 256):
        gheads_v[:, v * 256:(v + 1) * 256] = nt(gh1, wo_v[v * 256:(v + 1) * 256, :]).astype(BF)

    cos_tab, sin_tab = cs[0], -cs[1]
    gks, gvs = [], []
    for g in range(KVLOC):
        k = qkv[:, QC + g * HD:QC + (g + 1) * HD]
        v = qkv[:, QC + KC + g * HD:QC + KC + (g + 1) * HD]
        gk = gv = None
        for pair in range(GROUP // 2):
            outs = []
            for h in (g * GROUP + 2 * pair, g * GROUP + 2 * pair + 1):
                q = qkv[:, h * HD:(h + 1) * HD]
                probs = probs_of(q, k)
                gh = gheads_v[:, h * HD:(h + 1) * HD]
                gp = nt(gh, v).astype(BF).astype(F32)
                gvh = tn(probs.astype(BF), gh)
                gs = (probs * (gp - jnp.sum(gp * probs, axis=-1, keepdims=True)) * SCALE).astype(BF)
                outs.append(nn(gs, k).astype(BF).astype(F32))
                gkh = tn(gs, q)
                gk = gkh if gk is None else gk + gkh
                gv = gvh if gv is None else gv + gvh
            lo = (g * GROUP + 2 * pair) * HD
            gqkv_o[:, lo:lo + 128] = rope_pair(jnp.concatenate(outs, axis=1), cos_tab, sin_tab).astype(BF)
        gks.append(gk.astype(BF).astype(F32))
        gvs.append(gv.astype(BF))
    gqkv_o[:, QC:QC + KC] = rope_pair(jnp.concatenate(gks, axis=1), cos_tab, sin_tab).astype(BF)
    gqkv_o[:, QC + KC:] = jnp.concatenate(gvs, axis=1)

    for f in fetches[1:]:
        f.wait()
    sum0 = PairSum(p0, g0, gn1_o, (ps, pr), c, partner)
    sum0.run(lambda j: nn(gqkv_o[...], wqkv_v[:, cols(j)]))
    out_send.wait_recv()
    hid_o[...] = (h1[x].astype(F32) + (mlp[x].astype(F32) + mlp_got[...].astype(F32))).astype(BF)
    sum0.drain()
    out_send.wait_send()
    share.wait_send()


def back_kernel(gn1_own, gn1_got, x0, gh1, gain_a, gain_mp, gx_o, gain_o, gbuf, hs, hr):
    x, c, partner, cross = place()
    greet(partner)
    gains = []

    def first(b, r):
        grad = (gn1_own[b, r].astype(F32) + gn1_got[b, r].astype(F32)).astype(BF).astype(F32)
        back, part = norm_back(grad, x0[b, r].astype(F32), gain_a[...])
        gx_o[b, c, r] = (gh1[b, c, r].astype(F32) + back).astype(BF)
        gains.append(part)
    rows16(first)
    gbuf[c, 0:1] = gains[0] + gains[1] + gains[2] + gains[3]
    gbuf[c, 1:2] = gain_mp[...]
    share = remote(gx_o.at[:, c], gx_o.at[:, c], hs.at[0], hr.at[0], partner)
    share.start()
    share_gain = remote(gbuf.at[c], gbuf.at[c], hs.at[1], hr.at[1], partner)
    share_gain.start()
    share_gain.wait_recv()
    gain_o[...] = gbuf[0, 0:2] + gbuf[1, 0:2]
    share.wait_recv()
    share.wait_send()
    share_gain.wait_send()


NB = 4
BM = 256


def outer_kernel(spec, *refs):
    n_in = 1 + max(max(l, r) for l, r, _ in spec)
    ins, outs = refs[:n_in], refs[n_in:n_in + len(spec)]
    buf, sem = refs[n_in + len(spec):]

    done = 0
    copies = []
    for (l, r, off), out in zip(spec, outs):
        lhs, rhs = ins[l], ins[r]
        steps = out.shape[0] // BM if lhs is not None else 0
        bm = min(BM, out.shape[0])
        steps = out.shape[0] // bm
        if bm == BM:
            def copy(i, out=out, done=done):
                slot = lax.rem(i + done, NB)
                return pltpu.make_async_copy(buf.at[slot], out.at[pl.ds(pl.multiple_of(i * BM, BM), BM)], sem.at[slot])

            def step(i, carry, copy=copy, lhs=lhs, rhs=rhs, off=off, done=done):
                slot = lax.rem(i + done, NB)

                @pl.when(i + done >= NB)
                def _():
                    copy(i).wait()
                a = lhs[:, pl.ds(pl.multiple_of(off + i * BM, 128), BM)]
                buf[slot] = tn(a, rhs[...])
                copy(i).start()
                return carry
            lax.fori_loop(0, steps, step, 0)
            done += steps
        else:
            slot = done % NB
            if done >= NB:
                pltpu.make_async_copy(buf.at[slot], outs[0].at[pl.ds(0, BM)], sem.at[slot]).wait()
            buf[slot, 0:bm] = tn(lhs[:, off:off + bm], rhs[...])
            copies.append(pltpu.make_async_copy(buf.at[slot, pl.ds(0, bm)], out, sem.at[slot]))
            copies[-1].start()
            done += 1
    small = len(copies)
    for k in range(max(0, done - NB), done - small):
        slot = k % NB
        pltpu.make_async_copy(buf.at[slot], outs[0].at[pl.ds(0, BM)], sem.at[slot]).wait()
    for copy in copies:
        copy.wait()


def outer(ins, spec, rows):
    total = sum(rows)
    return pl.pallas_call(
        functools.partial(outer_kernel, spec),
        out_shape=tuple(jax.ShapeDtypeStruct((m, DIM), F32) for m in rows),
        in_specs=[pl.BlockSpec(memory_space=VMEM)] * len(ins),
        out_specs=tuple(pl.BlockSpec(memory_space=HBM) for _ in rows),
        scratch_shapes=[pltpu.VMEM((NB, BM, DIM), F32), pltpu.SemaphoreType.DMA((NB,))],
        cost_estimate=pl.CostEstimate(flops=2 * total * DIM * SEQ, bytes_accessed=4 * total * DIM, transcendentals=0),
        compiler_params=pltpu.CompilerParams(vmem_limit_bytes=24 * 2 ** 20),
    )(*ins)


def emb_kernel(tok, gx, out, buf, sem):
    base = lax.axis_index("tp") * VLOC
    ids = jnp.broadcast_to(tok[...], (BM, SEQ)) - base
    row = lax.broadcasted_iota(jnp.int32, (BM, SEQ), 0)
    grad = gx[...].reshape(SEQ, DIM)

    def copy(i):
        slot = lax.rem(i, NB)
        return pltpu.make_async_copy(buf.at[slot], out.at[pl.ds(pl.multiple_of(i * BM, BM), BM)], sem.at[slot])

    def step(i, carry):
        @pl.when(i >= NB)
        def _():
            copy(i).wait()
        hot = jnp.where(ids == row + i * BM, 1.0, 0.0).astype(BF)
        buf[lax.rem(i, NB)] = nn(hot, grad)
        copy(i).start()
        return carry
    steps = VLOC // BM
    lax.fori_loop(0, steps, step, 0)
    for k in range(steps - NB, steps):
        copy(k).wait()


def vm(n):
    return [pl.BlockSpec(memory_space=VMEM)] * n


def hb(n):
    return [pl.BlockSpec(memory_space=HBM)] * n


def sds(shape, dtype=BF):
    return jax.ShapeDtypeStruct(shape, dtype)


FULL = (2, 2, 32, DIM)
MINE = (2, 32, DIM)


def dma(*shape):
    return pltpu.SemaphoreType.DMA(shape)


def device_fn(tokens, positions, emb, gain_a, gain_m, wq, wk, wv, wo, wg, wu, wd, gh):
    inv_freq = (ROPE_THETA ** (-np.arange(HD // 2, dtype=np.float32) * np.float32(2.0 / HD))).astype(np.float32)
    freq = jnp.asarray(np.tile(inv_freq, 4)[None, :])
    ga, gm = gain_a.reshape(1, DIM), gain_m.reshape(1, DIM)
    flat = lambda w: jnp.transpose(w, (1, 2, 0)).reshape(-1, DIM)
    wqt, wkt, wvt = flat(wq), flat(wk), flat(wv)
    wo2 = wo.reshape(QC, DIM)
    gh2 = gh.reshape(32, DIM)

    n1, x0, qkv, cs, heads, h1, n2, act, ggate, gup, gfull, gn2, mlp = pl.pallas_call(
        front_kernel,
        out_shape=(sds(FULL), sds(MINE), sds((SEQ, QKV)), sds((2, SEQ, 128), F32), sds((SEQ, QC)), sds(MINE),
                   sds(FULL), sds((SEQ, FLOC)), sds((SEQ, FLOC)), sds((SEQ, FLOC)), sds(FULL), sds(MINE), sds(MINE)),
        in_specs=vm(6) + hb(8),
        out_specs=tuple(vm(13)),
        scratch_shapes=[
            pltpu.VMEM((VLOC, DIM), BF), pltpu.VMEM((QKV, DIM), BF), pltpu.VMEM((QC, DIM), BF),
            pltpu.VMEM((FLOC, DIM), BF), pltpu.VMEM((DIM, FLOC), BF), pltpu.VMEM((DIM, FLOC), BF),
            pltpu.VMEM((SEQ, VLOC), BF), pltpu.VMEM((SEQ, FLOC), BF),
            pltpu.VMEM(FULL, BF), pltpu.VMEM(MINE, BF), pltpu.VMEM(MINE, BF), pltpu.VMEM(MINE, BF),
            pltpu.VMEM(FULL, BF), pltpu.VMEM(MINE, BF), pltpu.VMEM(MINE, BF), pltpu.VMEM(MINE, BF),
            pltpu.VMEM(FULL, BF), pltpu.VMEM(MINE, BF), pltpu.VMEM(FULL, BF), pltpu.VMEM(MINE, BF),
            dma(NC), dma(7), dma(4, NC), dma(4, NC), dma(2, NC), dma(2, NC), dma(5), dma(5), dma(1), dma(1)],
        compiler_params=pltpu.CompilerParams(collective_id=0, has_side_effects=True, vmem_limit_bytes=52 * 2 ** 20),
    )(tokens, positions, freq, ga, gm, gh2, emb, wqt, wkt, wvt, wo2, wd, wg, wu)

    swap = [(i, i ^ 2) for i in range(4)]
    gn2_got = lax.ppermute(gn2, 'tp', swap)
    gfull2 = gfull.reshape(SEQ, DIM)
    n2f = n2.reshape(SEQ, DIM)
    g_gate, = outer((n2f, ggate), ((0, 1, 0),), (DIM,))

    gh1, gqkv, gn1, hidden, gain_mp = pl.pallas_call(
        middle_kernel,
        out_shape=(sds(FULL), sds((SEQ, QKV)), sds(MINE), sds((32, DIM)), sds((1, DIM), F32)),
        in_specs=vm(8) + hb(4),
        out_specs=tuple(vm(5)),
        scratch_shapes=[
            pltpu.VMEM((QKV, DIM), BF), pltpu.VMEM((QC, DIM), BF), pltpu.VMEM((SEQ, QC), BF), pltpu.VMEM((32, DIM), BF),
            pltpu.VMEM(FULL, BF), pltpu.VMEM(MINE, BF), dma(4), dma(NC), dma(NC), dma(2), dma(2)],
        compiler_params=pltpu.CompilerParams(collective_id=1, has_side_effects=True, vmem_limit_bytes=24 * 2 ** 20),
    )(gn2, gn2_got, mlp, h1, gfull, gm, qkv, cs, wqt, wkt, wvt, wo2)

    gn1_got = lax.ppermute(gn1, 'tp', swap)
    g_up, g_down, g_out, g_q, g_k, g_v = outer(
        (n2f, gup, act, gfull2, heads, gh1.reshape(SEQ, DIM), gqkv, n1.reshape(SEQ, DIM)),
        ((0, 1, 0), (2, 3, 0), (4, 5, 0), (6, 7, 0), (6, 7, QC), (6, 7, QC + KC)),
        (DIM, FLOC, QC, QC, KC, KC))

    gx, gains = pl.pallas_call(
        back_kernel,
        out_shape=(sds(FULL), sds((2, DIM), F32)),
        in_specs=vm(6),
        out_specs=tuple(vm(2)),
        scratch_shapes=[pltpu.VMEM((2, 8, DIM), F32), dma(2), dma(2)],
        compiler_params=pltpu.CompilerParams(collective_id=2, has_side_effects=True, vmem_limit_bytes=16 * 2 ** 20),
    )(gn1, gn1_got, x0, gh1, ga, gain_mp)

    g_emb = pl.pallas_call(
        emb_kernel,
        out_shape=sds((VLOC, DIM), F32),
        in_specs=vm(2),
        out_specs=hb(1)[0],
        scratch_shapes=[pltpu.VMEM((NB, BM, DIM), F32), dma(NB)],
        compiler_params=pltpu.CompilerParams(vmem_limit_bytes=24 * 2 ** 20),
    )(tokens, gx)

    back3 = lambda g: jnp.transpose(g.reshape(-1, HD, DIM), (2, 0, 1))
    return (hidden.reshape(1, 32, DIM), g_emb, back3(g_q), back3(g_k), back3(g_v), g_out.reshape(HLOC, HD, DIM),
            g_gate, g_up, g_down, gains[0], gains[1])


def solution(mesh):
    in_specs = (P('dp', None), P('dp', None), P('tp', None), P(None), P(None),
                P(None, 'tp', None), P(None, 'tp', None), P(None, 'tp', None), P('tp', None, None),
                P(None, 'tp'), P(None, 'tp'), P('tp', None), P('dp', 'tp', None))
    out_specs = (P('dp', 'tp', None), P(('dp', 'tp'), None),
                 P('dp', 'tp', None), P('dp', 'tp', None), P('dp', 'tp', None), P(('dp', 'tp'), None, None),
                 P('dp', 'tp'), P('dp', 'tp'), P(('dp', 'tp'), None), P('dp'), P('dp'))
    return jax.shard_map(device_fn, mesh=mesh, in_specs=in_specs, out_specs=out_specs, check_vma=False)
```

```python
import functools

import jax
import jax.numpy as jnp
import numpy as np
from jax import lax
from jax.experimental import pallas as pl
from jax.experimental.pallas import tpu as pltpu
from jax.sharding import PartitionSpec as P

ROPE_THETA = 1000000.0
RMS_EPS = 1e-5
MESH = pl.DeviceIdType.MESH
BF = jnp.bfloat16
F32 = jnp.float32

SEQ = 128
DIM = 2048
VLOC = 2048
FLOC = 2048
HLOC = 8
KVLOC = 2
HD = 64
QC = HLOC * HD
KC = KVLOC * HD
QKV = QC + 2 * KC
GROUP = HLOC // KVLOC
SCALE = HD ** -0.5
NC = 4
W = DIM // NC
VMEM = pltpu.VMEM
HBM = pltpu.HBM


def nn(a, b):
    return lax.dot_general(a, b, (((1,), (0,)), ((), ())), preferred_element_type=F32)


def nt(a, b):
    return lax.dot_general(a, b, (((1,), (1,)), ((), ())), preferred_element_type=F32)


def tn(a, b):
    return lax.dot_general(a, b, (((0,), (0,)), ((), ())), preferred_element_type=F32)


def place():
    tp = lax.axis_index("tp")
    x = tp // 2
    c = tp - 2 * x
    return x, c, 2 * x + (1 - c), 2 * (1 - x) + c


def greet(*peers):
    sem = pltpu.get_barrier_semaphore()
    for peer in peers:
        pl.semaphore_signal(sem, inc=1, device_id={"tp": peer}, device_id_type=MESH)
    pl.semaphore_wait(sem, len(peers))


def remote(src, dst, send, recv, peer):
    return pltpu.make_async_remote_copy(
        src_ref=src, dst_ref=dst, send_sem=send, recv_sem=recv, device_id={"tp": peer}, device_id_type=MESH)


def cols(j):
    return pl.ds(pl.multiple_of(j * W, W), W)


class PairSum:
    def __init__(self, part, got, own, sems, c, partner):
        self.part, self.got, self.own, self.c, self.partner = part, got, own, c, partner
        self.send, self.recv = sems

    def copy(self, j):
        return remote(self.part.at[:, 1 - self.c, :, cols(j)], self.got.at[:, :, cols(j)],
                      self.send.at[j], self.recv.at[j], self.partner)

    def put(self, j, value):
        self.part[:, :, :, cols(j)] = value.astype(BF).reshape(2, 2, 32, W)
        self.copy(j).start()

    def take(self, j):
        self.copy(j).wait_recv()
        total = self.part[:, self.c, :, cols(j)].astype(F32) + self.got[:, :, cols(j)].astype(F32)
        self.own[0:2, :, cols(j)] = total.astype(BF)

    def run(self, chunk, then=lambda j: None):
        def body(j, carry):
            self.put(j, chunk(j))

            @pl.when(j > 0)
            def _():
                self.take(j - 1)
                then(j - 1)
            return carry
        lax.fori_loop(0, NC, body, 0)
        self.take(NC - 1)
        then(NC - 1)

    def drain(self):
        for j in range(NC):
            self.copy(j).wait_send()


def rows16(fn):
    for b in range(2):
        for r in range(0, 32, 16):
            fn(b, slice(r, r + 16))


def norm_rows(x, gain):
    inv = lax.rsqrt(jnp.mean(x * x, axis=-1, keepdims=True) + RMS_EPS)
    return (x * inv * gain).astype(BF)


def norm_back(grad, x, gain):
    inv = lax.rsqrt(jnp.mean(x * x, axis=-1, keepdims=True) + RMS_EPS)
    normed = x * inv
    scaled = grad * gain
    back = inv * (scaled - normed * jnp.mean(scaled * normed, axis=-1, keepdims=True))
    return back, jnp.sum(grad * normed, axis=0, keepdims=True)


def spread(row):
    return jnp.transpose(jnp.broadcast_to(row, (SEQ, SEQ)))


def rope_pair(values, cos_tab, sin_tab):
    lane = lax.broadcasted_iota(jnp.int32, (SEQ, 128), 1)
    low = (lane % HD) < HD // 2
    other = jnp.where(low, pltpu.roll(values, 128 - HD // 2, 1), pltpu.roll(values, HD // 2, 1))
    return values * cos_tab + other * jnp.where(low, -sin_tab, sin_tab)


def probs_of(q, k):
    scores = nt(q, k) * SCALE
    causal = (lax.broadcasted_iota(jnp.int32, (SEQ, SEQ), 0) >= lax.broadcasted_iota(jnp.int32, (SEQ, SEQ), 1))
    scores = jnp.where(causal, scores, -1e30)
    e = jnp.exp(scores - jnp.max(scores, axis=-1, keepdims=True))
    return e / jnp.sum(e, axis=-1, keepdims=True)


def front_kernel(tok, pos, freq, gain_a, gain_m, gh, emb, wq, wk, wv, wo, wd, wg, wu,
                 n1_o, x0_o, qkv_o, cs_o, heads_o, h1_o, n2_o, act_o, ggate_o, gup_o, gfull_o, gn2_o,
                 wqkv_v, wo_v, wd_v,
                 tok_v, pos_v, freq_v, ga_v, gm_v, emb_v, wg_v, wu_v, wut_v, wqkvt_v, hot_v, gact_v,
                 p0, g0, s0, r0, p1, g1, s1, r1, p2, g2,
                 in_sem, emb_sem, w_sem, ps, pr, xs, xr, hs, hr):
    x, c, partner, cross = place()
    tp = 2 * x + c

    def fetch_emb(j):
        return pltpu.make_async_copy(emb.at[:, cols(j)], emb_v.at[:, cols(j)], emb_sem.at[j])

    get_q = pltpu.make_async_copy(wq, wqkv_v.at[pl.ds(0, QC)], w_sem.at[0])
    get_k = pltpu.make_async_copy(wk, wqkv_v.at[pl.ds(QC, KC)], w_sem.at[1])
    get_v = pltpu.make_async_copy(wv, wqkv_v.at[pl.ds(QC + KC, KC)], w_sem.at[2])
    get_out = pltpu.make_async_copy(wo, wo_v, w_sem.at[3])
    get_down = pltpu.make_async_copy(wd, wd_v, w_sem.at[4])
    get_gate = pltpu.make_async_copy(wg, wg_v, w_sem.at[5])
    get_up = pltpu.make_async_copy(wu, wu_v, w_sem.at[6])
    get_small = [pltpu.make_async_copy(src, dst, in_sem.at[i]) for i, (src, dst) in enumerate(
        ((tok, tok_v), (pos, pos_v), (freq, freq_v), (gain_a, ga_v), (gain_m, gm_v), (gh, gfull_o.at[x, c])))]
    get_small[0].start()
    fetch_emb(0).start()
    fetch_emb(1).start()
    for g in get_small[1:]:
        g.start()
    greet(partner, cross)

    get_small[0].wait()
    ids = spread(tok_v[...].astype(F32))
    base = (tp * VLOC).astype(F32)
    lane = lax.broadcasted_iota(jnp.int32, (SEQ, 128), 1).astype(F32)
    for v in range(VLOC // 128):
        hot_v[:, v * 128:(v + 1) * 128] = jnp.where(ids == lane + (base + float(v * 128)), 1.0, 0.0).astype(BF)

    def cross_copy(k, src, dst, j):
        return remote(src.at[:, :, cols(j)], dst.at[:, :, cols(j)], xs.at[k, j], xr.at[k, j], cross)

    sum0 = PairSum(p0, g0, s0, (ps.at[0], pr.at[0]), c, partner)

    def lookup(j):
        fetch_emb(j).wait()

        @pl.when(j + 2 < NC)
        def _():
            fetch_emb(j + 2).start()

        @pl.when(j == 2)
        def _():
            for g in (get_q, get_k, get_v):
                g.start()
        return nn(hot_v[...], emb_v[:, cols(j)])

    sum0.run(lookup, lambda j: cross_copy(0, s0, r0, j).start())
    for g in (get_up, get_out, get_down, get_gate):
        g.start()
    for g in get_small[1:]:
        g.wait()
    mine = gfull_o.at[x, c]
    to_cross = remote(mine, mine, hs.at[0], hr.at[0], cross)
    to_partner = remote(mine, mine, hs.at[1], hr.at[1], partner)
    to_cross.start()
    to_partner.start()
    angle = spread(pos_v[...].astype(F32)) * freq_v[...]
    cs_o[0] = jnp.cos(angle)
    cs_o[1] = jnp.sin(angle)

    for g in (get_q, get_k, get_v):
        g.wait()

    def turn_qkv(j, carry):
        rj = pl.ds(pl.multiple_of(j * 256, 256), 256)
        wqkvt_v[:, rj] = jnp.transpose(wqkv_v[rj, :])
        return carry
    lax.fori_loop(0, QKV // 256, turn_qkv, 0)
    get_up.wait()

    def turn_up(j, carry):
        wut_v[:, cols(j)] = jnp.transpose(wu_v[cols(j), :])
        return carry
    lax.fori_loop(0, NC, turn_up, 0)

    for j in range(NC):
        cross_copy(0, s0, r0, j).wait_recv()

    def first(b, r):
        xv = s0[b, r].astype(F32) + r0[b, r].astype(F32)
        x0_o[b, r] = xv.astype(BF)
        n1_o[b, c, r] = norm_rows(xv, ga_v[...])
    rows16(first)
    share1 = remote(n1_o.at[:, c], n1_o.at[:, c], hs.at[2], hr.at[2], partner)
    share1.start()
    share1.wait_recv()

    n1 = n1_o[...].reshape(SEQ, DIM)
    cos_tab, sin_tab = cs_o[0], cs_o[1]

    for v in range(QKV // 256):
        lin = nn(n1, wqkvt_v[:, v * 256:(v + 1) * 256])
        for h in range(2):
            lo = v * 256 + h * 128
            piece = lin[:, h * 128:(h + 1) * 128]
            if lo < QC + KC:
                piece = rope_pair(piece, cos_tab, sin_tab)
            qkv_o[:, lo:lo + 128] = piece.astype(BF)
    for pair in range(HLOC // 2):
        outs = []
        for h in (2 * pair, 2 * pair + 1):
            g = h // GROUP
            k = qkv_o[:, QC + g * HD:QC + (g + 1) * HD]
            v = qkv_o[:, QC + KC + g * HD:QC + KC + (g + 1) * HD]
            probs = probs_of(qkv_o[:, h * HD:(h + 1) * HD], k).astype(BF)
            outs.append(nn(probs, v).astype(BF))
        heads_o[:, pair * 128:(pair + 1) * 128] = jnp.concatenate(outs, axis=1)
    to_cross.wait_recv()
    onward = remote(gfull_o.at[1 - x, c], gfull_o.at[1 - x, c], hs.at[3], hr.at[3], partner)
    onward.start()
    get_out.wait()

    sum1 = PairSum(p1, g1, s1, (ps.at[1], pr.at[1]), c, partner)
    sum1.run(lambda j: nn(heads_o[...], wo_v[:, cols(j)]), lambda j: cross_copy(1, s1, r1, j).start())

    to_partner.wait_recv()
    onward.wait_recv()
    get_down.wait()
    get_gate.wait()
    gfull = gfull_o[...].reshape(SEQ, DIM)
    wgt_v = emb_v

    def grad_act(j, carry):
        gact_v[:, cols(j)] = nt(gfull, wd_v[cols(j), :]).astype(BF)
        wgt_v[:, cols(j)] = jnp.transpose(wg_v[cols(j), :])
        return carry
    lax.fori_loop(0, NC, grad_act, 0)

    for j in range(NC):
        cross_copy(1, s1, r1, j).wait_recv()

    def second(b, r):
        total = s1[b, r].astype(F32) + r1[b, r].astype(F32)
        h1 = (x0_o[b, r].astype(F32) + total).astype(BF)
        h1_o[b, r] = h1
        n2_o[b, c, r] = norm_rows(h1.astype(F32), gm_v[...])
    rows16(second)
    share2 = remote(n2_o.at[:, c], n2_o.at[:, c], hs.at[4], hr.at[4], partner)
    share2.start()
    share2.wait_recv()
    n2 = n2_o[...].reshape(SEQ, DIM)

    def mlp(j, carry):
        cj = pl.ds(pl.multiple_of(j * 256, 256), 256)
        gate = nn(n2, wg_v[:, cj])
        up = nn(n2, wu_v[:, cj])
        sig = jax.nn.sigmoid(gate)
        gate_act = gate * sig
        act_o[:, cj] = (gate_act * up).astype(BF)
        grad = gact_v[:, cj].astype(F32)
        gup_o[:, cj] = (grad * gate_act).astype(BF)
        ggate_o[:, cj] = (grad * up * sig * (1.0 + gate * (1.0 - sig))).astype(BF)
        return carry
    lax.fori_loop(0, FLOC // 256, mlp, 0)

    sum2 = PairSum(p2, g2, gn2_o, (ps.at[2], pr.at[2]), c, partner)
    sum2.run(lambda j: nn(ggate_o[...], wgt_v[:, cols(j)]) + nn(gup_o[...], wut_v[:, cols(j)]))

    for s in (sum0, sum1, sum2):
        s.drain()
    for j in range(NC):
        cross_copy(0, s0, r0, j).wait_send()
        cross_copy(1, s1, r1, j).wait_send()
    for copy in (to_cross, to_partner, share1, onward, share2):
        copy.wait_send()


def middle_kernel(gn2_own, gn2_got, act, h1, gfull, gain_m, qkv, cs, wqkv, wo, wd,
                  gh1_o, gqkv_o, give_o, keep_o, gain_o,
                  gheads_v, p0, g0, s0, p1, g1, ps, pr, hs, hr):
    x, c, partner, cross = place()
    greet(partner)
    gains = []

    def first(b, r):
        grad = (gn2_own[b, r].astype(F32) + gn2_got[b, r].astype(F32)).astype(BF).astype(F32)
        back, part = norm_back(grad, h1[b, r].astype(F32), gain_m[...])
        gh1_o[b, c, r] = (gfull[b, c, r].astype(F32) + back).astype(BF)
        gains.append(part)
    rows16(first)
    share = remote(gh1_o.at[:, c], gh1_o.at[:, c], hs.at[0], hr.at[0], partner)
    share.start()
    gain_o[...] = gains[0] + gains[1] + gains[2] + gains[3]
    sum0 = PairSum(p0, g0, s0, (ps.at[0], pr.at[0]), c, partner)
    sum0.run(lambda j: nn(act[...], wd[:, cols(j)]))
    give_o[2] = s0[1 - x]
    keep_o[...] = s0[x]
    share.wait_recv()

    gh1 = gh1_o[...].reshape(SEQ, DIM)
    for v in range(QC // 256):
        gheads_v[:, v * 256:(v + 1) * 256] = nt(gh1, wo[v * 256:(v + 1) * 256, :]).astype(BF)

    cos_tab, sin_tab = cs[0], -cs[1]
    gks, gvs = [], []
    for g in range(KVLOC):
        k = qkv[:, QC + g * HD:QC + (g + 1) * HD]
        v = qkv[:, QC + KC + g * HD:QC + KC + (g + 1) * HD]
        gk = gv = None
        for pair in range(GROUP // 2):
            outs = []
            for h in (g * GROUP + 2 * pair, g * GROUP + 2 * pair + 1):
                q = qkv[:, h * HD:(h + 1) * HD]
                probs = probs_of(q, k)
                gh = gheads_v[:, h * HD:(h + 1) * HD]
                gp = nt(gh, v).astype(BF).astype(F32)
                gvh = tn(probs.astype(BF), gh)
                gs = (probs * (gp - jnp.sum(gp * probs, axis=-1, keepdims=True)) * SCALE).astype(BF)
                outs.append(nn(gs, k).astype(BF).astype(F32))
                gkh = tn(gs, q)
                gk = gkh if gk is None else gk + gkh
                gv = gvh if gv is None else gv + gvh
            lo = (g * GROUP + 2 * pair) * HD
            gqkv_o[:, lo:lo + 128] = rope_pair(jnp.concatenate(outs, axis=1), cos_tab, sin_tab).astype(BF)
        gks.append(gk.astype(BF).astype(F32))
        gvs.append(gv.astype(BF))
    gqkv_o[:, QC:QC + KC] = rope_pair(jnp.concatenate(gks, axis=1), cos_tab, sin_tab).astype(BF)
    gqkv_o[:, QC + KC:] = jnp.concatenate(gvs, axis=1)

    sum1 = PairSum(p1, g1, give_o, (ps.at[1], pr.at[1]), c, partner)
    sum1.run(lambda j: nn(gqkv_o[...], wqkv[:, cols(j)]))
    sum0.drain()
    sum1.drain()
    share.wait_send()


def back_kernel(give, got, keep, h1, x0, gh1, gain_a, gain_mp, gx_o, gain_o, hid_o, gbuf, hs, hr):
    x, c, partner, cross = place()
    greet(partner)
    gains = []

    def first(b, r):
        grad = (give[b, r].astype(F32) + got[b, r].astype(F32)).astype(BF).astype(F32)
        back, part = norm_back(grad, x0[b, r].astype(F32), gain_a[...])
        gx_o[b, c, r] = (gh1[b, c, r].astype(F32) + back).astype(BF)
        gains.append(part)
    rows16(first)
    share = remote(gx_o.at[:, c], gx_o.at[:, c], hs.at[0], hr.at[0], partner)
    share.start()
    gbuf[c, 0:1] = gains[0] + gains[1] + gains[2] + gains[3]
    gbuf[c, 1:2] = gain_mp[...]
    share_gain = remote(gbuf.at[c], gbuf.at[c], hs.at[1], hr.at[1], partner)
    share_gain.start()
    hid_o[...] = (h1[x].astype(F32) + (keep[...].astype(F32) + got[2].astype(F32))).astype(BF)
    share_gain.wait_recv()
    gain_o[...] = gbuf[0, 0:2] + gbuf[1, 0:2]
    share.wait_recv()
    share.wait_send()
    share_gain.wait_send()


NB = 4
BM = 256


def outer_kernel(spec, *refs):
    n_in = 1 + max(max(l, r) for l, r, _ in spec)
    ins, outs = refs[:n_in], refs[n_in:n_in + len(spec)]
    buf, sem = refs[n_in + len(spec):]

    done = 0
    copies = []
    for (l, r, off), out in zip(spec, outs):
        lhs, rhs = ins[l], ins[r]
        steps = out.shape[0] // BM if lhs is not None else 0
        bm = min(BM, out.shape[0])
        steps = out.shape[0] // bm
        if bm == BM:
            def copy(i, out=out, done=done):
                slot = lax.rem(i + done, NB)
                return pltpu.make_async_copy(buf.at[slot], out.at[pl.ds(pl.multiple_of(i * BM, BM), BM)], sem.at[slot])

            def step(i, carry, copy=copy, lhs=lhs, rhs=rhs, off=off, done=done):
                slot = lax.rem(i + done, NB)

                @pl.when(i + done >= NB)
                def _():
                    copy(i).wait()
                a = lhs[:, pl.ds(pl.multiple_of(off + i * BM, 128), BM)]
                buf[slot] = tn(a, rhs[...])
                copy(i).start()
                return carry
            lax.fori_loop(0, steps, step, 0)
            done += steps
        else:
            slot = done % NB
            if done >= NB:
                pltpu.make_async_copy(buf.at[slot], outs[0].at[pl.ds(0, BM)], sem.at[slot]).wait()
            buf[slot, 0:bm] = tn(lhs[:, off:off + bm], rhs[...])
            copies.append(pltpu.make_async_copy(buf.at[slot, pl.ds(0, bm)], out, sem.at[slot]))
            copies[-1].start()
            done += 1
    small = len(copies)
    for k in range(max(0, done - NB), done - small):
        slot = k % NB
        pltpu.make_async_copy(buf.at[slot], outs[0].at[pl.ds(0, BM)], sem.at[slot]).wait()
    for copy in copies:
        copy.wait()


def outer(ins, spec, rows):
    total = sum(rows)
    return pl.pallas_call(
        functools.partial(outer_kernel, spec),
        out_shape=tuple(jax.ShapeDtypeStruct((m, DIM), F32) for m in rows),
        in_specs=[pl.BlockSpec(memory_space=VMEM)] * len(ins),
        out_specs=tuple(pl.BlockSpec(memory_space=HBM) for _ in rows),
        scratch_shapes=[pltpu.VMEM((NB, BM, DIM), F32), pltpu.SemaphoreType.DMA((NB,))],
        cost_estimate=pl.CostEstimate(flops=2 * total * DIM * SEQ, bytes_accessed=4 * total * DIM, transcendentals=0),
        compiler_params=pltpu.CompilerParams(vmem_limit_bytes=24 * 2 ** 20),
    )(*ins)


def emb_kernel(tok, gx, gains, hid, out, ga_o, gm_o, hid_o, buf, sem, out_sem):
    extra = (
        pltpu.make_async_copy(gains.at[pl.ds(0, 1)], ga_o, out_sem.at[0]),
        pltpu.make_async_copy(gains.at[pl.ds(1, 1)], gm_o, out_sem.at[1]),
        pltpu.make_async_copy(hid, hid_o, out_sem.at[2]),
    )
    for e in extra:
        e.start()
    base = lax.axis_index("tp") * VLOC
    ids = jnp.broadcast_to(tok[...], (BM, SEQ)) - base
    row = lax.broadcasted_iota(jnp.int32, (BM, SEQ), 0)
    grad = gx[...].reshape(SEQ, DIM)

    def copy(i):
        slot = lax.rem(i, NB)
        return pltpu.make_async_copy(buf.at[slot], out.at[pl.ds(pl.multiple_of(i * BM, BM), BM)], sem.at[slot])

    def step(i, carry):
        @pl.when(i >= NB)
        def _():
            copy(i).wait()
        hot = jnp.where(ids == row + i * BM, 1.0, 0.0).astype(BF)
        buf[lax.rem(i, NB)] = nn(hot, grad)
        copy(i).start()
        return carry
    steps = VLOC // BM
    lax.fori_loop(0, steps, step, 0)
    for k in range(steps - NB, steps):
        copy(k).wait()
    for e in extra:
        e.wait()


def vm(n):
    return [pl.BlockSpec(memory_space=VMEM)] * n


def hb(n):
    return [pl.BlockSpec(memory_space=HBM)] * n


def sds(shape, dtype=BF):
    return jax.ShapeDtypeStruct(shape, dtype)


def on(shape, dtype=BF):
    return pltpu.VMEM(shape, dtype)


FULL = (2, 2, 32, DIM)
MINE = (2, 32, DIM)


def dma(*shape):
    return pltpu.SemaphoreType.DMA(shape)


def device_fn(tokens, positions, emb, gain_a, gain_m, wq, wk, wv, wo, wg, wu, wd, gh):
    inv_freq = (ROPE_THETA ** (-np.arange(HD // 2, dtype=np.float32) * np.float32(2.0 / HD))).astype(np.float32)
    freq = jnp.asarray(np.tile(inv_freq, 4)[None, :])
    ga, gm = gain_a.reshape(1, DIM), gain_m.reshape(1, DIM)
    flat = lambda w: jnp.transpose(w, (1, 2, 0)).reshape(-1, DIM)
    wqt, wkt, wvt = flat(wq), flat(wk), flat(wv)
    wo2 = wo.reshape(QC, DIM)
    gh2 = gh.reshape(32, DIM)

    n1, x0, qkv, cs, heads, h1, n2, act, ggate, gup, gfull, gn2, wqkv_v, wo_v, wd_v = pl.pallas_call(
        front_kernel,
        out_shape=(on(FULL), on(MINE), on((SEQ, QKV)), on((2, SEQ, 128), F32), on((SEQ, QC)), on(MINE),
                   on(FULL), on((SEQ, FLOC)), on((SEQ, FLOC)), on((SEQ, FLOC)), on(FULL), on(MINE),
                   on((QKV, DIM)), on((QC, DIM)), on((FLOC, DIM))),
        in_specs=hb(14),
        out_specs=tuple(vm(15)),
        scratch_shapes=[
            pltpu.VMEM((1, SEQ), jnp.int32), pltpu.VMEM((1, SEQ), jnp.int32), pltpu.VMEM((1, SEQ), F32),
            pltpu.VMEM((1, DIM), F32), pltpu.VMEM((1, DIM), F32),
            pltpu.VMEM((VLOC, DIM), BF), pltpu.VMEM((DIM, FLOC), BF), pltpu.VMEM((DIM, FLOC), BF),
            pltpu.VMEM((FLOC, DIM), BF), pltpu.VMEM((DIM, QKV), BF),
            pltpu.VMEM((SEQ, VLOC), BF), pltpu.VMEM((SEQ, FLOC), BF),
            pltpu.VMEM(FULL, BF), pltpu.VMEM(MINE, BF), pltpu.VMEM(MINE, BF), pltpu.VMEM(MINE, BF),
            pltpu.VMEM(FULL, BF), pltpu.VMEM(MINE, BF), pltpu.VMEM(MINE, BF), pltpu.VMEM(MINE, BF),
            pltpu.VMEM(FULL, BF), pltpu.VMEM(MINE, BF),
            dma(6), dma(NC), dma(7), dma(3, NC), dma(3, NC), dma(2, NC), dma(2, NC), dma(5), dma(5)],
        compiler_params=pltpu.CompilerParams(collective_id=0, has_side_effects=True, vmem_limit_bytes=42 * 2 ** 20),
    )(tokens, positions, freq, ga, gm, gh2, emb, wqt, wkt, wvt, wo2, wd, wg, wu)

    swap = [(i, i ^ 2) for i in range(4)]
    gn2_got = lax.ppermute(gn2, 'tp', swap)
    gfull2 = gfull.reshape(SEQ, DIM)
    n2f = n2.reshape(SEQ, DIM)
    g_gate, = outer((n2f, ggate), ((0, 1, 0),), (DIM,))

    gh1, gqkv, give, keep, gain_mp = pl.pallas_call(
        middle_kernel,
        out_shape=(on(FULL), on((SEQ, QKV)), on((3, 32, DIM)), on((32, DIM)), on((1, DIM), F32)),
        in_specs=vm(11),
        out_specs=tuple(vm(5)),
        scratch_shapes=[
            pltpu.VMEM((SEQ, QC), BF),
            pltpu.VMEM(FULL, BF), pltpu.VMEM(MINE, BF), pltpu.VMEM(MINE, BF), pltpu.VMEM(FULL, BF), pltpu.VMEM(MINE, BF),
            dma(2, NC), dma(2, NC), dma(1), dma(1)],
        compiler_params=pltpu.CompilerParams(collective_id=1, has_side_effects=True, vmem_limit_bytes=8 * 2 ** 20),
    )(gn2, gn2_got, act, h1, gfull, gm, qkv, cs, wqkv_v, wo_v, wd_v)

    got = lax.ppermute(give, 'tp', swap)
    g_up, g_down, g_out, g_q, g_k, g_v = outer(
        (n2f, gup, act, gfull2, heads, gh1.reshape(SEQ, DIM), gqkv, n1.reshape(SEQ, DIM)),
        ((0, 1, 0), (2, 3, 0), (4, 5, 0), (6, 7, 0), (6, 7, QC), (6, 7, QC + KC)),
        (DIM, FLOC, QC, QC, KC, KC))

    gx, gains, hid = pl.pallas_call(
        back_kernel,
        out_shape=(on(FULL), on((2, DIM), F32), on((32, DIM))),
        in_specs=vm(8),
        out_specs=tuple(vm(3)),
        scratch_shapes=[pltpu.VMEM((2, 8, DIM), F32), dma(2), dma(2)],
        compiler_params=pltpu.CompilerParams(collective_id=2, has_side_effects=True, vmem_limit_bytes=8 * 2 ** 20),
    )(give, got, keep, h1, x0, gh1, ga, gain_mp)

    g_emb, gain_1, gain_2, hidden = pl.pallas_call(
        emb_kernel,
        out_shape=(sds((VLOC, DIM), F32), sds((1, DIM), F32), sds((1, DIM), F32), sds((32, DIM))),
        in_specs=vm(4),
        out_specs=tuple(hb(4)),
        scratch_shapes=[pltpu.VMEM((NB, BM, DIM), F32), dma(NB), dma(3)],
        compiler_params=pltpu.CompilerParams(vmem_limit_bytes=24 * 2 ** 20),
    )(tokens, gx, gains, hid)

    back3 = lambda g: jnp.transpose(g.reshape(-1, HD, DIM), (2, 0, 1))
    return (hidden.reshape(1, 32, DIM), g_emb, back3(g_q), back3(g_k), back3(g_v), g_out.reshape(HLOC, HD, DIM),
            g_gate, g_up, g_down, gain_1.reshape(DIM), gain_2.reshape(DIM))


def solution(mesh):
    in_specs = (P('dp', None), P('dp', None), P('tp', None), P(None), P(None),
                P(None, 'tp', None), P(None, 'tp', None), P(None, 'tp', None), P('tp', None, None),
                P(None, 'tp'), P(None, 'tp'), P('tp', None), P('dp', 'tp', None))
    out_specs = (P('dp', 'tp', None), P(('dp', 'tp'), None),
                 P('dp', 'tp', None), P('dp', 'tp', None), P('dp', 'tp', None), P(('dp', 'tp'), None, None),
                 P('dp', 'tp'), P('dp', 'tp'), P(('dp', 'tp'), None), P('dp'), P('dp'))
    return jax.shard_map(device_fn, mesh=mesh, in_specs=in_specs, out_specs=out_specs, check_vma=False)
```

```python
import functools

import jax
import jax.numpy as jnp
import numpy as np
from jax import lax
from jax.experimental import pallas as pl
from jax.experimental.pallas import tpu as pltpu
from jax.sharding import PartitionSpec as P

ROPE_THETA = 1000000.0
RMS_EPS = 1e-5
MESH = pl.DeviceIdType.MESH
BF = jnp.bfloat16
F32 = jnp.float32

SEQ = 128
DIM = 2048
VLOC = 2048
FLOC = 2048
HLOC = 8
KVLOC = 2
HD = 64
QC = HLOC * HD
KC = KVLOC * HD
QKV = QC + 2 * KC
GROUP = HLOC // KVLOC
SCALE = HD ** -0.5
NC = 4
W = DIM // NC
VMEM = pltpu.VMEM
HBM = pltpu.HBM


def nn(a, b):
    return lax.dot_general(a, b, (((1,), (0,)), ((), ())), preferred_element_type=F32)


def nt(a, b):
    return lax.dot_general(a, b, (((1,), (1,)), ((), ())), preferred_element_type=F32)


def tn(a, b):
    return lax.dot_general(a, b, (((0,), (0,)), ((), ())), preferred_element_type=F32)


def place():
    tp = lax.axis_index("tp")
    x = tp // 2
    c = tp - 2 * x
    return x, c, 2 * x + (1 - c), 2 * (1 - x) + c


def greet(*peers):
    sem = pltpu.get_barrier_semaphore()
    for peer in peers:
        pl.semaphore_signal(sem, inc=1, device_id={"tp": peer}, device_id_type=MESH)
    pl.semaphore_wait(sem, len(peers))


def remote(src, dst, send, recv, peer):
    return pltpu.make_async_remote_copy(
        src_ref=src, dst_ref=dst, send_sem=send, recv_sem=recv, device_id={"tp": peer}, device_id_type=MESH)


def cols(j):
    return pl.ds(pl.multiple_of(j * W, W), W)


class PairSum:
    def __init__(self, part, got, own, sems, c, partner):
        self.part, self.got, self.own, self.c, self.partner = part, got, own, c, partner
        self.send, self.recv = sems

    def copy(self, j):
        return remote(self.part.at[:, 1 - self.c, :, cols(j)], self.got.at[:, :, cols(j)],
                      self.send.at[j], self.recv.at[j], self.partner)

    def put(self, j, value):
        self.part[:, :, :, cols(j)] = value.astype(BF).reshape(2, 2, 32, W)
        self.copy(j).start()

    def take(self, j):
        self.copy(j).wait_recv()
        total = self.part[:, self.c, :, cols(j)].astype(F32) + self.got[:, :, cols(j)].astype(F32)
        self.own[0:2, :, cols(j)] = total.astype(BF)

    def send_all(self, chunk):
        def body(j, carry):
            self.put(j, chunk(j))
            return carry
        lax.fori_loop(0, NC, body, 0)

    def run(self, chunk, then=lambda j: None, lag=NC):
        def finish(j):
            self.take(j)
            then(j)

        def body(j, carry):
            self.put(j, chunk(j))
            if lag < NC:
                @pl.when(j >= lag)
                def _():
                    finish(j - lag)
            return carry
        lax.fori_loop(0, NC, body, 0)
        for j in range(NC - lag, NC):
            finish(j)

    def drain(self):
        for j in range(NC):
            self.copy(j).wait_send()


def rows16(fn):
    for b in range(2):
        for r in range(0, 32, 16):
            fn(b, slice(r, r + 16))


def norm_rows(x, gain):
    inv = lax.rsqrt(jnp.mean(x * x, axis=-1, keepdims=True) + RMS_EPS)
    return (x * inv * gain).astype(BF)


def norm_back(grad, x, gain):
    inv = lax.rsqrt(jnp.mean(x * x, axis=-1, keepdims=True) + RMS_EPS)
    normed = x * inv
    scaled = grad * gain
    back = inv * (scaled - normed * jnp.mean(scaled * normed, axis=-1, keepdims=True))
    return back, jnp.sum(grad * normed, axis=0, keepdims=True)


def spread(row):
    return jnp.transpose(jnp.broadcast_to(row, (SEQ, SEQ)))


def rope_pair(values, cos_tab, sin_tab):
    lane = lax.broadcasted_iota(jnp.int32, (SEQ, 128), 1)
    low = (lane % HD) < HD // 2
    other = jnp.where(low, pltpu.roll(values, 128 - HD // 2, 1), pltpu.roll(values, HD // 2, 1))
    return values * cos_tab + other * jnp.where(low, -sin_tab, sin_tab)


def probs_of(q, k):
    scores = nt(q, k) * SCALE
    causal = (lax.broadcasted_iota(jnp.int32, (SEQ, SEQ), 0) >= lax.broadcasted_iota(jnp.int32, (SEQ, SEQ), 1))
    scores = jnp.where(causal, scores, -1e30)
    e = jnp.exp(scores - jnp.max(scores, axis=-1, keepdims=True))
    return e / jnp.sum(e, axis=-1, keepdims=True)


def front_kernel(tok, pos, freq, gain_a, gain_m, gh, emb, wq, wk, wv, wo, wd, wg, wu,
                 n1_o, x0_o, qkv_o, cs_o, heads_o, h1_o, n2_o, act_o, ggate_o, gup_o, gfull_o, gn2_o,
                 wqkv_v, wo_v, wd_v,
                 tok_v, pos_v, freq_v, ga_v, gm_v, emb_v, wg_v, wu_v, wut_v, wqkvt_v, hot_v, gact_v,
                 p0, g0, s0, r0, p1, g1, s1, r1, p2, g2,
                 in_sem, emb_sem, w_sem, ps, pr, xs, xr, hs, hr):
    x, c, partner, cross = place()
    tp = 2 * x + c

    def fetch_emb(j):
        return pltpu.make_async_copy(emb.at[:, cols(j)], emb_v.at[:, cols(j)], emb_sem.at[j])

    get_q = pltpu.make_async_copy(wq, wqkv_v.at[pl.ds(0, QC)], w_sem.at[0])
    get_k = pltpu.make_async_copy(wk, wqkv_v.at[pl.ds(QC, KC)], w_sem.at[1])
    get_v = pltpu.make_async_copy(wv, wqkv_v.at[pl.ds(QC + KC, KC)], w_sem.at[2])
    get_out = pltpu.make_async_copy(wo, wo_v, w_sem.at[3])
    get_down = pltpu.make_async_copy(wd, wd_v, w_sem.at[4])
    get_gate = pltpu.make_async_copy(wg, wg_v, w_sem.at[5])
    get_up = pltpu.make_async_copy(wu, wu_v, w_sem.at[6])
    get_small = [pltpu.make_async_copy(src, dst, in_sem.at[i]) for i, (src, dst) in enumerate(
        ((tok, tok_v), (pos, pos_v), (freq, freq_v), (gain_a, ga_v), (gain_m, gm_v), (gh, gfull_o.at[x, c])))]
    get_small[0].start()
    fetch_emb(0).start()
    fetch_emb(1).start()
    for g in get_small[1:]:
        g.start()
    greet(partner, cross)

    get_small[0].wait()
    ids = spread(tok_v[...].astype(F32))
    base = (tp * VLOC).astype(F32)
    lane = lax.broadcasted_iota(jnp.int32, (SEQ, 128), 1).astype(F32)
    for v in range(VLOC // 128):
        hot_v[:, v * 128:(v + 1) * 128] = jnp.where(ids == lane + (base + float(v * 128)), 1.0, 0.0).astype(BF)

    def cross_copy(k, src, dst, j):
        return remote(src.at[:, :, cols(j)], dst.at[:, :, cols(j)], xs.at[k, j], xr.at[k, j], cross)

    sum0 = PairSum(p0, g0, s0, (ps.at[0], pr.at[0]), c, partner)

    def lookup(j):
        fetch_emb(j).wait()

        @pl.when(j + 2 < NC)
        def _():
            fetch_emb(j + 2).start()

        @pl.when(j == 2)
        def _():
            for g in (get_q, get_k, get_v):
                g.start()
        return nn(hot_v[...], emb_v[:, cols(j)])

    sum0.run(lookup, lambda j: cross_copy(0, s0, r0, j).start(), 1)
    for g in (get_out, get_down, get_gate, get_up):
        g.start()
    for g in get_small[1:]:
        g.wait()
    mine = gfull_o.at[x, c]
    to_cross = remote(mine, mine, hs.at[0], hr.at[0], cross)
    to_partner = remote(mine, mine, hs.at[1], hr.at[1], partner)
    to_cross.start()
    to_partner.start()
    angle = spread(pos_v[...].astype(F32)) * freq_v[...]
    cs_o[0] = jnp.cos(angle)
    cs_o[1] = jnp.sin(angle)

    for g in (get_q, get_k, get_v):
        g.wait()

    def turn_qkv(j, carry):
        rj = pl.ds(pl.multiple_of(j * 256, 256), 256)
        wqkvt_v[:, rj] = jnp.transpose(wqkv_v[rj, :])
        return carry
    lax.fori_loop(0, QKV // 256, turn_qkv, 0)

    for j in range(NC):
        cross_copy(0, s0, r0, j).wait_recv()

    def first(b, r):
        xv = s0[b, r].astype(F32) + r0[b, r].astype(F32)
        x0_o[b, r] = xv.astype(BF)
        n1_o[b, c, r] = norm_rows(xv, ga_v[...])
    rows16(first)
    share1 = remote(n1_o.at[:, c], n1_o.at[:, c], hs.at[2], hr.at[2], partner)
    share1.start()
    share1.wait_recv()

    n1 = n1_o[...].reshape(SEQ, DIM)
    cos_tab, sin_tab = cs_o[0], cs_o[1]

    for v in range(QKV // 256):
        lin = nn(n1, wqkvt_v[:, v * 256:(v + 1) * 256])
        for h in range(2):
            lo = v * 256 + h * 128
            piece = lin[:, h * 128:(h + 1) * 128]
            if lo < QC + KC:
                piece = rope_pair(piece, cos_tab, sin_tab)
            qkv_o[:, lo:lo + 128] = piece.astype(BF)
    for pair in range(HLOC // 2):
        outs = []
        for h in (2 * pair, 2 * pair + 1):
            g = h // GROUP
            k = qkv_o[:, QC + g * HD:QC + (g + 1) * HD]
            v = qkv_o[:, QC + KC + g * HD:QC + KC + (g + 1) * HD]
            probs = probs_of(qkv_o[:, h * HD:(h + 1) * HD], k).astype(BF)
            outs.append(nn(probs, v).astype(BF))
        heads_o[:, pair * 128:(pair + 1) * 128] = jnp.concatenate(outs, axis=1)
    to_cross.wait_recv()
    onward = remote(gfull_o.at[1 - x, c], gfull_o.at[1 - x, c], hs.at[3], hr.at[3], partner)
    onward.start()
    get_out.wait()

    sum1 = PairSum(p1, g1, s1, (ps.at[1], pr.at[1]), c, partner)
    sum1.run(lambda j: nn(heads_o[...], wo_v[:, cols(j)]), lambda j: cross_copy(1, s1, r1, j).start())

    to_partner.wait_recv()
    onward.wait_recv()
    get_down.wait()
    get_gate.wait()
    gfull = gfull_o[...].reshape(SEQ, DIM)
    wgt_v = emb_v

    def grad_act(j, carry):
        gact_v[:, cols(j)] = nt(gfull, wd_v[cols(j), :]).astype(BF)
        wgt_v[:, cols(j)] = jnp.transpose(wg_v[cols(j), :])
        return carry
    lax.fori_loop(0, NC, grad_act, 0)
    get_up.wait()

    def turn_up(j, carry):
        wut_v[:, cols(j)] = jnp.transpose(wu_v[cols(j), :])
        return carry
    lax.fori_loop(0, NC, turn_up, 0)

    for j in range(NC):
        cross_copy(1, s1, r1, j).wait_recv()

    def second(b, r):
        total = s1[b, r].astype(F32) + r1[b, r].astype(F32)
        h1 = (x0_o[b, r].astype(F32) + total).astype(BF)
        h1_o[b, r] = h1
        n2_o[b, c, r] = norm_rows(h1.astype(F32), gm_v[...])
    rows16(second)
    share2 = remote(n2_o.at[:, c], n2_o.at[:, c], hs.at[4], hr.at[4], partner)
    share2.start()
    share2.wait_recv()
    n2 = n2_o[...].reshape(SEQ, DIM)

    def mlp(j, carry):
        cj = pl.ds(pl.multiple_of(j * 256, 256), 256)
        gate = nn(n2, wg_v[:, cj])
        up = nn(n2, wu_v[:, cj])
        sig = jax.nn.sigmoid(gate)
        gate_act = gate * sig
        act_o[:, cj] = (gate_act * up).astype(BF)
        grad = gact_v[:, cj].astype(F32)
        gup_o[:, cj] = (grad * gate_act).astype(BF)
        ggate_o[:, cj] = (grad * up * sig * (1.0 + gate * (1.0 - sig))).astype(BF)
        return carry
    lax.fori_loop(0, FLOC // 256, mlp, 0)

    sum2 = PairSum(p2, g2, gn2_o, (ps.at[2], pr.at[2]), c, partner)
    sum2.run(lambda j: nn(ggate_o[...], wgt_v[:, cols(j)]) + nn(gup_o[...], wut_v[:, cols(j)]))

    for s in (sum0, sum1, sum2):
        s.drain()
    for j in range(NC):
        cross_copy(0, s0, r0, j).wait_send()
        cross_copy(1, s1, r1, j).wait_send()
    for copy in (to_cross, to_partner, share1, onward, share2):
        copy.wait_send()


def middle_kernel(gn2_own, gn2_got, act, h1, gfull, gain_m, qkv, cs, wqkv, wo, wd, token,
                  gh1_o, gqkv_o, give_o, keep_o, gain_o,
                  gheads_v, p0, g0, s0, p1, g1, ps, pr, hs, hr):
    x, c, partner, cross = place()
    greet(partner)
    gains = []

    def first(b, r):
        grad = (gn2_own[b, r].astype(F32) + gn2_got[b, r].astype(F32)).astype(BF).astype(F32)
        back, part = norm_back(grad, h1[b, r].astype(F32), gain_m[...])
        gh1_o[b, c, r] = (gfull[b, c, r].astype(F32) + back).astype(BF)
        gains.append(part)
    rows16(first)
    share = remote(gh1_o.at[:, c], gh1_o.at[:, c], hs.at[0], hr.at[0], partner)
    share.start()
    gain_o[...] = gains[0] + gains[1] + gains[2] + gains[3]
    sum0 = PairSum(p0, g0, s0, (ps.at[0], pr.at[0]), c, partner)
    sum0.send_all(lambda j: nn(act[...], wd[:, cols(j)]))
    share.wait_recv()

    gh1 = gh1_o[...].reshape(SEQ, DIM)
    for v in range(QC // 256):
        gheads_v[:, v * 256:(v + 1) * 256] = nt(gh1, wo[v * 256:(v + 1) * 256, :]).astype(BF)

    cos_tab, sin_tab = cs[0], -cs[1]
    gks, gvs = [], []
    for g in range(KVLOC):
        k = qkv[:, QC + g * HD:QC + (g + 1) * HD]
        v = qkv[:, QC + KC + g * HD:QC + KC + (g + 1) * HD]
        gk = gv = None
        for pair in range(GROUP // 2):
            outs = []
            for h in (g * GROUP + 2 * pair, g * GROUP + 2 * pair + 1):
                q = qkv[:, h * HD:(h + 1) * HD]
                probs = probs_of(q, k)
                gh = gheads_v[:, h * HD:(h + 1) * HD]
                gp = nt(gh, v).astype(BF).astype(F32)
                gvh = tn(probs.astype(BF), gh)
                gs = (probs * (gp - jnp.sum(gp * probs, axis=-1, keepdims=True)) * SCALE).astype(BF)
                outs.append(nn(gs, k).astype(BF).astype(F32))
                gkh = tn(gs, q)
                gk = gkh if gk is None else gk + gkh
                gv = gvh if gv is None else gv + gvh
            lo = (g * GROUP + 2 * pair) * HD
            gqkv_o[:, lo:lo + 128] = rope_pair(jnp.concatenate(outs, axis=1), cos_tab, sin_tab).astype(BF)
        gks.append(gk.astype(BF).astype(F32))
        gvs.append(gv.astype(BF))
    gqkv_o[:, QC:QC + KC] = rope_pair(jnp.concatenate(gks, axis=1), cos_tab, sin_tab).astype(BF)
    gqkv_o[:, QC + KC:] = jnp.concatenate(gvs, axis=1)

    sum1 = PairSum(p1, g1, give_o, (ps.at[1], pr.at[1]), c, partner)
    sum1.send_all(lambda j: nn(gqkv_o[...], wqkv[:, cols(j)]))
    for j in range(NC):
        sum0.take(j)
    give_o[2] = s0[1 - x]
    keep_o[...] = s0[x]
    for j in range(NC):
        sum1.take(j)
    sum0.drain()
    sum1.drain()
    share.wait_send()


def back_kernel(give, got, keep, h1, x0, gh1, gain_a, gain_mp, token, gx_o, gain_o, hid_o, gbuf, hs, hr):
    x, c, partner, cross = place()
    greet(partner)
    gains = []

    def first(b, r):
        grad = (give[b, r].astype(F32) + got[b, r].astype(F32)).astype(BF).astype(F32)
        back, part = norm_back(grad, x0[b, r].astype(F32), gain_a[...])
        gx_o[b, c, r] = (gh1[b, c, r].astype(F32) + back).astype(BF)
        gains.append(part)
    rows16(first)
    share = remote(gx_o.at[:, c], gx_o.at[:, c], hs.at[0], hr.at[0], partner)
    share.start()
    gbuf[c, 0:1] = gains[0] + gains[1] + gains[2] + gains[3]
    gbuf[c, 1:2] = gain_mp[...]
    share_gain = remote(gbuf.at[c], gbuf.at[c], hs.at[1], hr.at[1], partner)
    share_gain.start()
    hid_o[...] = (h1[x].astype(F32) + (keep[...].astype(F32) + got[2].astype(F32))).astype(BF)
    share_gain.wait_recv()
    gain_o[...] = gbuf[0, 0:2] + gbuf[1, 0:2]
    share.wait_recv()
    share.wait_send()
    share_gain.wait_send()


def vm(n):
    return [pl.BlockSpec(memory_space=VMEM)] * n


def hb(n):
    return [pl.BlockSpec(memory_space=HBM)] * n


def on(shape, dtype=BF):
    return pltpu.VMEM(shape, dtype)


NB = 4
UP_FIRST = 768
BM = 256


def outer_kernel(spec, n_in, n_held, *refs):
    n_out = 1 + max(o for _, _, _, o, _, _ in spec)
    ins, outs = refs[:n_in], refs[n_in + n_held:n_in + n_held + n_out]
    token, buf, sem = refs[n_in + n_held + n_out:]
    token[...] = jnp.zeros_like(token)
    done = 0
    flying = {}
    for l, r, off, o, row, rows in spec:
        lhs, rhs, out = ins[l], ins[r], outs[o]
        bm = min(BM, rows)
        steps = rows // bm

        def copy(i, out=out, done=done, bm=bm, row=row):
            slot = lax.rem(i + done, NB)
            where = pl.ds(pl.multiple_of(row + i * bm, bm), bm)
            return pltpu.make_async_copy(buf.at[slot, pl.ds(0, bm)], out.at[where], sem.at[slot])

        def compute(i, lhs=lhs, rhs=rhs, off=off, done=done, bm=bm):
            a = lhs[:, pl.ds(pl.multiple_of(off + i * bm, 128), bm)]
            buf[lax.rem(i + done, NB), 0:bm] = tn(a, rhs[...])

        free = [(done + i) % NB for i in range(min(NB, steps))]
        uniform = steps >= NB and all(flying.get(k, bm) == bm for k in range(NB)) and (not flying or len(flying) == NB)
        if uniform:
            def step(i, carry, copy=copy, compute=compute, waiting=bool(flying)):
                if waiting:
                    copy(i).wait()
                else:
                    @pl.when(i >= NB)
                    def _():
                        copy(i).wait()
                compute(i)
                copy(i).start()
                return carry
            lax.fori_loop(0, steps, step, 0)
            flying = {k: bm for k in range(NB)}
        else:
            for i in range(steps):
                slot = (done + i) % NB
                if slot in flying:
                    size = flying[slot]
                    pltpu.make_async_copy(buf.at[slot, pl.ds(0, size)], outs[0].at[pl.ds(0, size)], sem.at[slot]).wait()
                compute(i)
                copy(i).start()
                flying[slot] = bm
        done += steps
    for slot, size in flying.items():
        pltpu.make_async_copy(buf.at[slot, pl.ds(0, size)], outs[0].at[pl.ds(0, size)], sem.at[slot]).wait()


def outer(ins, spec, rows, held=()):
    total = sum(n for *_, n in spec)
    *outs, token = pl.pallas_call(
        functools.partial(outer_kernel, spec, len(ins), len(held)),
        out_shape=tuple(jax.ShapeDtypeStruct((m, DIM), F32) for m in rows) + (on((8, 128), F32),),
        in_specs=vm(len(ins)) + hb(len(held)),
        out_specs=tuple(hb(len(rows)) + vm(1)),
        scratch_shapes=[pltpu.VMEM((NB, BM, DIM), F32), pltpu.SemaphoreType.DMA((NB,))],
        input_output_aliases={len(ins) + i: o for i, (_, o) in enumerate(held)},
        cost_estimate=pl.CostEstimate(flops=2 * total * DIM * SEQ, bytes_accessed=4 * total * DIM, transcendentals=0),
        compiler_params=pltpu.CompilerParams(vmem_limit_bytes=16 * 2 ** 20),
    )(*ins, *[h for h, _ in held])
    return outs, token


def emb_kernel(tok, gx, gains, hid, out, ga_o, gm_o, hid_o, buf, sem, out_sem):
    extra = (
        pltpu.make_async_copy(gains.at[pl.ds(0, 1)], ga_o, out_sem.at[0]),
        pltpu.make_async_copy(gains.at[pl.ds(1, 1)], gm_o, out_sem.at[1]),
        pltpu.make_async_copy(hid, hid_o, out_sem.at[2]),
    )
    for e in extra:
        e.start()
    base = lax.axis_index("tp") * VLOC
    ids = jnp.broadcast_to(tok[...], (BM, SEQ)) - base
    row = lax.broadcasted_iota(jnp.int32, (BM, SEQ), 0)
    grad = gx[...].reshape(SEQ, DIM)

    def copy(i):
        slot = lax.rem(i, NB)
        return pltpu.make_async_copy(buf.at[slot], out.at[pl.ds(pl.multiple_of(i * BM, BM), BM)], sem.at[slot])

    def step(i, carry):
        @pl.when(i >= NB)
        def _():
            copy(i).wait()
        hot = jnp.where(ids == row + i * BM, 1.0, 0.0).astype(BF)
        buf[lax.rem(i, NB)] = nn(hot, grad)
        copy(i).start()
        return carry
    steps = VLOC // BM
    lax.fori_loop(0, steps, step, 0)
    for k in range(steps - NB, steps):
        copy(k).wait()
    for e in extra:
        e.wait()


def sds(shape, dtype=BF):
    return jax.ShapeDtypeStruct(shape, dtype)


FULL = (2, 2, 32, DIM)
MINE = (2, 32, DIM)


def dma(*shape):
    return pltpu.SemaphoreType.DMA(shape)


def device_fn(tokens, positions, emb, gain_a, gain_m, wq, wk, wv, wo, wg, wu, wd, gh):
    inv_freq = (ROPE_THETA ** (-np.arange(HD // 2, dtype=np.float32) * np.float32(2.0 / HD))).astype(np.float32)
    freq = jnp.asarray(np.tile(inv_freq, 4)[None, :])
    ga, gm = gain_a.reshape(1, DIM), gain_m.reshape(1, DIM)
    flat = lambda w: jnp.transpose(w, (1, 2, 0)).reshape(-1, DIM)
    wqt, wkt, wvt = flat(wq), flat(wk), flat(wv)
    wo2 = wo.reshape(QC, DIM)
    gh2 = gh.reshape(32, DIM)

    n1, x0, qkv, cs, heads, h1, n2, act, ggate, gup, gfull, gn2, wqkv_v, wo_v, wd_v = pl.pallas_call(
        front_kernel,
        out_shape=(on(FULL), on(MINE), on((SEQ, QKV)), on((2, SEQ, 128), F32), on((SEQ, QC)), on(MINE),
                   on(FULL), on((SEQ, FLOC)), on((SEQ, FLOC)), on((SEQ, FLOC)), on(FULL), on(MINE),
                   on((QKV, DIM)), on((QC, DIM)), on((FLOC, DIM))),
        in_specs=hb(14),
        out_specs=tuple(vm(15)),
        scratch_shapes=[
            pltpu.VMEM((1, SEQ), jnp.int32), pltpu.VMEM((1, SEQ), jnp.int32), pltpu.VMEM((1, SEQ), F32),
            pltpu.VMEM((1, DIM), F32), pltpu.VMEM((1, DIM), F32),
            pltpu.VMEM((VLOC, DIM), BF), pltpu.VMEM((DIM, FLOC), BF), pltpu.VMEM((DIM, FLOC), BF),
            pltpu.VMEM((FLOC, DIM), BF), pltpu.VMEM((DIM, QKV), BF),
            pltpu.VMEM((SEQ, VLOC), BF), pltpu.VMEM((SEQ, FLOC), BF),
            pltpu.VMEM(FULL, BF), pltpu.VMEM(MINE, BF), pltpu.VMEM(MINE, BF), pltpu.VMEM(MINE, BF),
            pltpu.VMEM(FULL, BF), pltpu.VMEM(MINE, BF), pltpu.VMEM(MINE, BF), pltpu.VMEM(MINE, BF),
            pltpu.VMEM(FULL, BF), pltpu.VMEM(MINE, BF),
            dma(6), dma(NC), dma(7), dma(3, NC), dma(3, NC), dma(2, NC), dma(2, NC), dma(5), dma(5)],
        compiler_params=pltpu.CompilerParams(collective_id=0, has_side_effects=True, vmem_limit_bytes=42 * 2 ** 20),
    )(tokens, positions, freq, ga, gm, gh2, emb, wqt, wkt, wvt, wo2, wd, wg, wu)

    swap = [(i, i ^ 2) for i in range(4)]
    gn2_got = lax.ppermute(gn2, 'tp', swap)
    gfull2 = gfull.reshape(SEQ, DIM)
    n2f = n2.reshape(SEQ, DIM)
    (g_gate, g_up), token = outer((n2f, ggate, gup), ((0, 1, 0, 0, 0, DIM), (0, 2, 0, 1, 0, UP_FIRST)), (DIM, DIM))

    gh1, gqkv, give, keep, gain_mp = pl.pallas_call(
        middle_kernel,
        out_shape=(on(FULL), on((SEQ, QKV)), on((3, 32, DIM)), on((32, DIM)), on((1, DIM), F32)),
        in_specs=vm(12),
        out_specs=tuple(vm(5)),
        scratch_shapes=[
            pltpu.VMEM((SEQ, QC), BF),
            pltpu.VMEM(FULL, BF), pltpu.VMEM(MINE, BF), pltpu.VMEM(MINE, BF), pltpu.VMEM(FULL, BF), pltpu.VMEM(MINE, BF),
            dma(2, NC), dma(2, NC), dma(1), dma(1)],
        compiler_params=pltpu.CompilerParams(collective_id=1, has_side_effects=True, vmem_limit_bytes=8 * 2 ** 20),
    )(gn2, gn2_got, act, h1, gfull, gm, qkv, cs, wqkv_v, wo_v, wd_v, token)

    got = lax.ppermute(give, 'tp', swap)
    (g_up, g_down, g_out, g_q, g_k, g_v), token2 = outer(
        (n2f, gup, act, gfull2, heads, gh1.reshape(SEQ, DIM), gqkv, n1.reshape(SEQ, DIM)),
        ((0, 1, UP_FIRST, 0, UP_FIRST, DIM - UP_FIRST), (2, 3, 0, 1, 0, FLOC), (4, 5, 0, 2, 0, QC),
         (6, 7, 0, 3, 0, QC), (6, 7, QC, 4, 0, KC), (6, 7, QC + KC, 5, 0, KC)),
        (DIM, FLOC, QC, QC, KC, KC), ((g_up, 0),))

    gx, gains, hid = pl.pallas_call(
        back_kernel,
        out_shape=(on(FULL), on((2, DIM), F32), on((32, DIM))),
        in_specs=vm(9),
        out_specs=tuple(vm(3)),
        scratch_shapes=[pltpu.VMEM((2, 8, DIM), F32), dma(2), dma(2)],
        compiler_params=pltpu.CompilerParams(collective_id=2, has_side_effects=True, vmem_limit_bytes=8 * 2 ** 20),
    )(give, got, keep, h1, x0, gh1, ga, gain_mp, token2)

    g_emb, gain_1, gain_2, hidden = pl.pallas_call(
        emb_kernel,
        out_shape=(sds((VLOC, DIM), F32), sds((1, DIM), F32), sds((1, DIM), F32), sds((32, DIM))),
        in_specs=vm(4),
        out_specs=tuple(hb(4)),
        scratch_shapes=[pltpu.VMEM((NB, BM, DIM), F32), dma(NB), dma(3)],
        compiler_params=pltpu.CompilerParams(vmem_limit_bytes=24 * 2 ** 20),
    )(tokens, gx, gains, hid)

    back3 = lambda g: jnp.transpose(g.reshape(-1, HD, DIM), (2, 0, 1))
    return (hidden.reshape(1, 32, DIM), g_emb, back3(g_q), back3(g_k), back3(g_v), g_out.reshape(HLOC, HD, DIM),
            g_gate, g_up, g_down, gain_1.reshape(DIM), gain_2.reshape(DIM))


def solution(mesh):
    in_specs = (P('dp', None), P('dp', None), P('tp', None), P(None), P(None),
                P(None, 'tp', None), P(None, 'tp', None), P(None, 'tp', None), P('tp', None, None),
                P(None, 'tp'), P(None, 'tp'), P('tp', None), P('dp', 'tp', None))
    out_specs = (P('dp', 'tp', None), P(('dp', 'tp'), None),
                 P('dp', 'tp', None), P('dp', 'tp', None), P('dp', 'tp', None), P(('dp', 'tp'), None, None),
                 P('dp', 'tp'), P('dp', 'tp'), P(('dp', 'tp'), None), P('dp'), P('dp'))
    return jax.shard_map(device_fn, mesh=mesh, in_specs=in_specs, out_specs=out_specs, check_vma=False)
```

```python
import functools

import jax
import jax.numpy as jnp
import numpy as np
from jax import lax
from jax.experimental import pallas as pl
from jax.experimental.pallas import tpu as pltpu
from jax.sharding import PartitionSpec as P

ROPE_THETA = 1000000.0
RMS_EPS = 1e-5
MESH = pl.DeviceIdType.MESH
BF = jnp.bfloat16
F32 = jnp.float32

SEQ = 128
DIM = 2048
VLOC = 2048
FLOC = 2048
HLOC = 8
KVLOC = 2
HD = 64
QC = HLOC * HD
KC = KVLOC * HD
QKV = QC + 2 * KC
GROUP = HLOC // KVLOC
SCALE = HD ** -0.5
NC = 4
W = DIM // NC
NE = 8
WE = DIM // NE
AHEAD = 3
VMEM = pltpu.VMEM
HBM = pltpu.HBM


def nn(a, b):
    return lax.dot_general(a, b, (((1,), (0,)), ((), ())), preferred_element_type=F32)


def nt(a, b):
    return lax.dot_general(a, b, (((1,), (1,)), ((), ())), preferred_element_type=F32)


def tn(a, b):
    return lax.dot_general(a, b, (((0,), (0,)), ((), ())), preferred_element_type=F32)


def place():
    tp = lax.axis_index("tp")
    x = tp // 2
    c = tp - 2 * x
    return x, c, 2 * x + (1 - c), 2 * (1 - x) + c


def greet(*peers):
    sem = pltpu.get_barrier_semaphore()
    for peer in peers:
        pl.semaphore_signal(sem, inc=1, device_id={"tp": peer}, device_id_type=MESH)
    pl.semaphore_wait(sem, len(peers))


def remote(src, dst, send, recv, peer):
    return pltpu.make_async_remote_copy(
        src_ref=src, dst_ref=dst, send_sem=send, recv_sem=recv, device_id={"tp": peer}, device_id_type=MESH)


def cols(j, width=W):
    return pl.ds(pl.multiple_of(j * width, width), width)


class PairSum:
    def __init__(self, part, got, own, sems, c, partner, n=NC):
        self.part, self.got, self.own, self.c, self.partner = part, got, own, c, partner
        self.send, self.recv = sems
        self.n, self.width = n, DIM // n

    def copy(self, j):
        return remote(self.part.at[:, 1 - self.c, :, cols(j, self.width)], self.got.at[:, :, cols(j, self.width)],
                      self.send.at[j], self.recv.at[j], self.partner)

    def put(self, j, value):
        self.part[:, :, :, cols(j, self.width)] = value.astype(BF).reshape(2, 2, 32, self.width)
        self.copy(j).start()

    def take(self, j):
        self.copy(j).wait_recv()
        total = self.part[:, self.c, :, cols(j, self.width)].astype(F32) + self.got[:, :, cols(j, self.width)].astype(F32)
        self.own[0:2, :, cols(j, self.width)] = total.astype(BF)

    def send_all(self, chunk):
        def body(j, carry):
            self.put(j, chunk(j))
            return carry
        lax.fori_loop(0, self.n, body, 0)

    def run(self, chunk, then=lambda j: None, lag=None):
        lag = lag or self.n

        def finish(j):
            self.take(j)
            then(j)

        def body(j, carry):
            self.put(j, chunk(j))
            if lag < self.n:
                @pl.when(j >= lag)
                def _():
                    finish(j - lag)
            return carry
        lax.fori_loop(0, self.n, body, 0)
        for j in range(self.n - lag, self.n):
            finish(j)

    def drain(self):
        for j in range(self.n):
            self.copy(j).wait_send()


def rows16(fn):
    for b in range(2):
        for r in range(0, 32, 16):
            fn(b, slice(r, r + 16))


def norm_rows(x, gain):
    inv = lax.rsqrt(jnp.mean(x * x, axis=-1, keepdims=True) + RMS_EPS)
    return (x * inv * gain).astype(BF)


def norm_back(grad, x, gain):
    inv = lax.rsqrt(jnp.mean(x * x, axis=-1, keepdims=True) + RMS_EPS)
    normed = x * inv
    scaled = grad * gain
    back = inv * (scaled - normed * jnp.mean(scaled * normed, axis=-1, keepdims=True))
    return back, jnp.sum(grad * normed, axis=0, keepdims=True)


def spread(row):
    return jnp.transpose(jnp.broadcast_to(row, (SEQ, SEQ)))


def rope_pair(values, cos_tab, sin_tab):
    lane = lax.broadcasted_iota(jnp.int32, (SEQ, 128), 1)
    low = (lane % HD) < HD // 2
    other = jnp.where(low, pltpu.roll(values, 128 - HD // 2, 1), pltpu.roll(values, HD // 2, 1))
    return values * cos_tab + other * jnp.where(low, -sin_tab, sin_tab)


def stack(ref, g):
    return jnp.concatenate([ref[:, h * HD:(h + 1) * HD] for h in range(g * GROUP, (g + 1) * GROUP)], axis=0)


def unstack(ref, g, value, fix=lambda pair: pair):
    for i in range(0, GROUP, 2):
        lo = (g * GROUP + i) * HD
        pair = jnp.concatenate([value[i * SEQ:(i + 1) * SEQ], value[(i + 1) * SEQ:(i + 2) * SEQ]], axis=1)
        ref[:, lo:lo + 128] = fix(pair).astype(BF)


def probs_of(q, k):
    scores = nt(q, k) * SCALE
    shape = (GROUP * SEQ, SEQ)
    row = lax.broadcasted_iota(jnp.int32, shape, 0) % SEQ
    scores = jnp.where(row >= lax.broadcasted_iota(jnp.int32, shape, 1), scores, -1e30)
    e = jnp.exp(scores - jnp.max(scores, axis=-1, keepdims=True))
    return e / jnp.sum(e, axis=-1, keepdims=True)


def front_kernel(tok, pos, freq, gain_a, gain_m, gh, emb, wq, wk, wv, wo, wd, wg, wu,
                 n1_o, x0_o, qkv_o, cs_o, heads_o, h1_o, n2_o, act_o, ggate_o, gup_o, gfull_o, gn2_o,
                 wqkv_v, wo_v, wd_v,
                 tok_v, pos_v, freq_v, ga_v, gm_v, emb_v, wg_v, wu_v, wut_v, wqkvt_v, hot_v, gact_v,
                 p0, g0, s0, r0, p1, g1, s1, r1, p2, g2,
                 in_sem, emb_sem, w_sem, ps, pr, xs, xr, hs, hr):
    x, c, partner, cross = place()
    tp = 2 * x + c

    def fetch_emb(j):
        return pltpu.make_async_copy(emb.at[:, cols(j, WE)], emb_v.at[:, cols(j, WE)], emb_sem.at[j])

    get_q = pltpu.make_async_copy(wq, wqkv_v.at[pl.ds(0, QC)], w_sem.at[0])
    get_k = pltpu.make_async_copy(wk, wqkv_v.at[pl.ds(QC, KC)], w_sem.at[1])
    get_v = pltpu.make_async_copy(wv, wqkv_v.at[pl.ds(QC + KC, KC)], w_sem.at[2])
    get_out = pltpu.make_async_copy(wo, wo_v, w_sem.at[3])
    get_down = pltpu.make_async_copy(wd, wd_v, w_sem.at[4])
    get_gate = pltpu.make_async_copy(wg, wg_v, w_sem.at[5])
    get_up = pltpu.make_async_copy(wu, wu_v, w_sem.at[6])
    get_small = [pltpu.make_async_copy(src, dst, in_sem.at[i]) for i, (src, dst) in enumerate(
        ((tok, tok_v), (pos, pos_v), (freq, freq_v), (gain_a, ga_v), (gain_m, gm_v), (gh, gfull_o.at[x, c])))]
    get_small[0].start()
    for j in range(AHEAD):
        fetch_emb(j).start()
    for g in get_small[1:]:
        g.start()
    get_small[0].wait()
    ids = spread(tok_v[...].astype(F32))
    base = (tp * VLOC).astype(F32)
    lane = lax.broadcasted_iota(jnp.int32, (SEQ, 128), 1).astype(F32)
    for v in range(VLOC // 128):
        hot_v[:, v * 128:(v + 1) * 128] = jnp.where(ids == lane + (base + float(v * 128)), 1.0, 0.0).astype(BF)

    greet(partner, cross)

    def cross_copy(k, src, dst, j):
        cj = cols(j, WE if k == 0 else W)
        return remote(src.at[:, :, cj], dst.at[:, :, cj], xs.at[k, j], xr.at[k, j], cross)

    sum0 = PairSum(p0, g0, s0, (ps.at[0], pr.at[0]), c, partner, NE)

    def lookup(j):
        fetch_emb(j).wait()

        @pl.when(j + AHEAD < NE)
        def _():
            fetch_emb(j + AHEAD).start()

        @pl.when(j == NE - AHEAD)
        def _():
            for g in (get_q, get_k, get_v):
                g.start()
        return nn(hot_v[...], emb_v[:, cols(j, WE)])

    sum0.run(lookup, lambda j: cross_copy(0, s0, r0, j).start(), 1)
    for g in (get_out, get_down, get_gate, get_up):
        g.start()
    for g in get_small[1:]:
        g.wait()
    mine = gfull_o.at[x, c]
    to_cross = remote(mine, mine, hs.at[0], hr.at[0], cross)
    to_partner = remote(mine, mine, hs.at[1], hr.at[1], partner)
    to_cross.start()
    to_partner.start()
    angle = spread(pos_v[...].astype(F32)) * freq_v[...]
    cs_o[0] = jnp.cos(angle)
    cs_o[1] = jnp.sin(angle)

    for g in (get_q, get_k, get_v):
        g.wait()

    def turn_qkv(j, carry):
        rj = pl.ds(pl.multiple_of(j * 256, 256), 256)
        wqkvt_v[:, rj] = jnp.transpose(wqkv_v[rj, :])
        return carry
    lax.fori_loop(0, QKV // 256, turn_qkv, 0)

    for j in range(NE):
        cross_copy(0, s0, r0, j).wait_recv()

    def first(b, r):
        xv = s0[b, r].astype(F32) + r0[b, r].astype(F32)
        x0_o[b, r] = xv.astype(BF)
        n1_o[b, c, r] = norm_rows(xv, ga_v[...])
    rows16(first)
    share1 = remote(n1_o.at[:, c], n1_o.at[:, c], hs.at[2], hr.at[2], partner)
    share1.start()
    share1.wait_recv()

    n1 = n1_o[...].reshape(SEQ, DIM)
    cos_tab, sin_tab = cs_o[0], cs_o[1]

    for v in range(QKV // 256):
        lin = nn(n1, wqkvt_v[:, v * 256:(v + 1) * 256])
        for h in range(2):
            lo = v * 256 + h * 128
            piece = lin[:, h * 128:(h + 1) * 128]
            if lo < QC + KC:
                piece = rope_pair(piece, cos_tab, sin_tab)
            qkv_o[:, lo:lo + 128] = piece.astype(BF)
    for g in range(KVLOC):
        k = qkv_o[:, QC + g * HD:QC + (g + 1) * HD]
        v = qkv_o[:, QC + KC + g * HD:QC + KC + (g + 1) * HD]
        unstack(heads_o, g, nn(probs_of(stack(qkv_o, g), k).astype(BF), v).astype(BF))
    to_cross.wait_recv()
    onward = remote(gfull_o.at[1 - x, c], gfull_o.at[1 - x, c], hs.at[3], hr.at[3], partner)
    onward.start()
    get_out.wait()

    sum1 = PairSum(p1, g1, s1, (ps.at[1], pr.at[1]), c, partner)
    sum1.run(lambda j: nn(heads_o[...], wo_v[:, cols(j)]), lambda j: cross_copy(1, s1, r1, j).start())

    to_partner.wait_recv()
    onward.wait_recv()
    get_down.wait()
    get_gate.wait()
    gfull = gfull_o[...].reshape(SEQ, DIM)
    wgt_v = emb_v

    def grad_act(j, carry):
        gact_v[:, cols(j)] = nt(gfull, wd_v[cols(j), :]).astype(BF)
        wgt_v[:, cols(j)] = jnp.transpose(wg_v[cols(j), :])
        return carry
    lax.fori_loop(0, NC, grad_act, 0)
    get_up.wait()

    def turn_up(j, carry):
        wut_v[:, cols(j)] = jnp.transpose(wu_v[cols(j), :])
        return carry
    lax.fori_loop(0, NC, turn_up, 0)

    for j in range(NC):
        cross_copy(1, s1, r1, j).wait_recv()

    def second(b, r):
        total = s1[b, r].astype(F32) + r1[b, r].astype(F32)
        h1 = (x0_o[b, r].astype(F32) + total).astype(BF)
        h1_o[b, r] = h1
        n2_o[b, c, r] = norm_rows(h1.astype(F32), gm_v[...])
    rows16(second)
    share2 = remote(n2_o.at[:, c], n2_o.at[:, c], hs.at[4], hr.at[4], partner)
    share2.start()
    share2.wait_recv()
    n2 = n2_o[...].reshape(SEQ, DIM)

    def mlp(j, carry):
        cj = pl.ds(pl.multiple_of(j * 256, 256), 256)
        gate = nn(n2, wg_v[:, cj])
        up = nn(n2, wu_v[:, cj])
        sig = jax.nn.sigmoid(gate)
        gate_act = gate * sig
        act_o[:, cj] = (gate_act * up).astype(BF)
        grad = gact_v[:, cj].astype(F32)
        gup_o[:, cj] = (grad * gate_act).astype(BF)
        ggate_o[:, cj] = (grad * up * sig * (1.0 + gate * (1.0 - sig))).astype(BF)
        return carry
    lax.fori_loop(0, FLOC // 256, mlp, 0)

    sum2 = PairSum(p2, g2, gn2_o, (ps.at[2], pr.at[2]), c, partner)
    sum2.run(lambda j: nn(ggate_o[...], wgt_v[:, cols(j)]) + nn(gup_o[...], wut_v[:, cols(j)]))

    for s in (sum0, sum1, sum2):
        s.drain()
    for j in range(NE):
        cross_copy(0, s0, r0, j).wait_send()
    for j in range(NC):
        cross_copy(1, s1, r1, j).wait_send()
    for copy in (to_cross, to_partner, share1, onward, share2):
        copy.wait_send()


def middle_kernel(gn2_own, gn2_got, act, h1, gfull, gain_m, qkv, cs, wqkv, wo, wd, token,
                  gh1_o, gqkv_o, give_o, keep_o, gain_o,
                  gheads_v, p0, g0, s0, p1, g1, ps, pr, hs, hr):
    x, c, partner, cross = place()
    greet(partner)
    gains = []

    def first(b, r):
        grad = (gn2_own[b, r].astype(F32) + gn2_got[b, r].astype(F32)).astype(BF).astype(F32)
        back, part = norm_back(grad, h1[b, r].astype(F32), gain_m[...])
        gh1_o[b, c, r] = (gfull[b, c, r].astype(F32) + back).astype(BF)
        gains.append(part)
    rows16(first)
    share = remote(gh1_o.at[:, c], gh1_o.at[:, c], hs.at[0], hr.at[0], partner)
    share.start()
    gain_o[...] = gains[0] + gains[1] + gains[2] + gains[3]
    sum0 = PairSum(p0, g0, s0, (ps.at[0], pr.at[0]), c, partner)
    sum0.send_all(lambda j: nn(act[...], wd[:, cols(j)]))
    share.wait_recv()

    gh1 = gh1_o[...].reshape(SEQ, DIM)
    for v in range(QC // 256):
        gheads_v[:, v * 256:(v + 1) * 256] = nt(gh1, wo[v * 256:(v + 1) * 256, :]).astype(BF)

    cos_tab, sin_tab = cs[0], -cs[1]
    turn_back = lambda pair: rope_pair(pair.astype(F32), cos_tab, sin_tab)
    gks, gvs = [], []
    for g in range(KVLOC):
        k = qkv[:, QC + g * HD:QC + (g + 1) * HD]
        v = qkv[:, QC + KC + g * HD:QC + KC + (g + 1) * HD]
        q, gh = stack(qkv, g), stack(gheads_v, g)
        probs = probs_of(q, k)
        gp = nt(gh, v).astype(BF).astype(F32)
        gvs.append(tn(probs.astype(BF), gh).astype(BF))
        gs = (probs * (gp - jnp.sum(gp * probs, axis=-1, keepdims=True)) * SCALE).astype(BF)
        gks.append(tn(gs, q).astype(BF).astype(F32))
        unstack(gqkv_o, g, nn(gs, k).astype(BF), turn_back)
    gqkv_o[:, QC:QC + KC] = rope_pair(jnp.concatenate(gks, axis=1), cos_tab, sin_tab).astype(BF)
    gqkv_o[:, QC + KC:] = jnp.concatenate(gvs, axis=1)

    sum1 = PairSum(p1, g1, give_o, (ps.at[1], pr.at[1]), c, partner)
    sum1.send_all(lambda j: nn(gqkv_o[...], wqkv[:, cols(j)]))
    for j in range(NC):
        sum0.take(j)
    give_o[2] = s0[1 - x]
    keep_o[...] = s0[x]
    for j in range(NC):
        sum1.take(j)
    sum0.drain()
    sum1.drain()
    share.wait_send()


def back_kernel(give, got, keep, h1, x0, gh1, gain_a, gain_mp, token, gx_o, gain_o, hid_o, gbuf, hs, hr):
    x, c, partner, cross = place()
    greet(partner)
    gains = []

    def first(b, r):
        grad = (give[b, r].astype(F32) + got[b, r].astype(F32)).astype(BF).astype(F32)
        back, part = norm_back(grad, x0[b, r].astype(F32), gain_a[...])
        gx_o[b, c, r] = (gh1[b, c, r].astype(F32) + back).astype(BF)
        gains.append(part)
    rows16(first)
    share = remote(gx_o.at[:, c], gx_o.at[:, c], hs.at[0], hr.at[0], partner)
    share.start()
    gbuf[c, 0:1] = gains[0] + gains[1] + gains[2] + gains[3]
    gbuf[c, 1:2] = gain_mp[...]
    share_gain = remote(gbuf.at[c], gbuf.at[c], hs.at[1], hr.at[1], partner)
    share_gain.start()
    hid_o[...] = (h1[x].astype(F32) + (keep[...].astype(F32) + got[2].astype(F32))).astype(BF)
    share_gain.wait_recv()
    gain_o[...] = gbuf[0, 0:2] + gbuf[1, 0:2]
    share.wait_recv()
    share.wait_send()
    share_gain.wait_send()


def vm(n):
    return [pl.BlockSpec(memory_space=VMEM)] * n


def hb(n):
    return [pl.BlockSpec(memory_space=HBM)] * n


def on(shape, dtype=BF):
    return pltpu.VMEM(shape, dtype)


NB = 4
UP_FIRST = 768
BM = 256


def outer_kernel(spec, n_in, n_held, *refs):
    n_out = 1 + max(o for _, _, _, o, _, _ in spec)
    ins, outs = refs[:n_in], refs[n_in + n_held:n_in + n_held + n_out]
    token, buf, sem = refs[n_in + n_held + n_out:]
    token[...] = jnp.zeros_like(token)
    done = 0
    flying = {}
    for l, r, off, o, row, rows in spec:
        lhs, rhs, out = ins[l], ins[r], outs[o]
        bm = min(BM, rows)
        steps = rows // bm

        def copy(i, out=out, done=done, bm=bm, row=row):
            slot = lax.rem(i + done, NB)
            where = pl.ds(pl.multiple_of(row + i * bm, bm), bm)
            return pltpu.make_async_copy(buf.at[slot, pl.ds(0, bm)], out.at[where], sem.at[slot])

        def compute(i, lhs=lhs, rhs=rhs, off=off, done=done, bm=bm):
            a = lhs[:, pl.ds(pl.multiple_of(off + i * bm, 128), bm)]
            buf[lax.rem(i + done, NB), 0:bm] = tn(a, rhs[...])

        free = [(done + i) % NB for i in range(min(NB, steps))]
        uniform = steps >= NB and all(flying.get(k, bm) == bm for k in range(NB)) and (not flying or len(flying) == NB)
        if uniform:
            def step(i, carry, copy=copy, compute=compute, waiting=bool(flying)):
                if waiting:
                    copy(i).wait()
                else:
                    @pl.when(i >= NB)
                    def _():
                        copy(i).wait()
                compute(i)
                copy(i).start()
                return carry
            lax.fori_loop(0, steps, step, 0)
            flying = {k: bm for k in range(NB)}
        else:
            for i in range(steps):
                slot = (done + i) % NB
                if slot in flying:
                    size = flying[slot]
                    pltpu.make_async_copy(buf.at[slot, pl.ds(0, size)], outs[0].at[pl.ds(0, size)], sem.at[slot]).wait()
                compute(i)
                copy(i).start()
                flying[slot] = bm
        done += steps
    for slot, size in flying.items():
        pltpu.make_async_copy(buf.at[slot, pl.ds(0, size)], outs[0].at[pl.ds(0, size)], sem.at[slot]).wait()


def outer(ins, spec, rows, held=()):
    total = sum(n for *_, n in spec)
    *outs, token = pl.pallas_call(
        functools.partial(outer_kernel, spec, len(ins), len(held)),
        out_shape=tuple(jax.ShapeDtypeStruct((m, DIM), F32) for m in rows) + (on((8, 128), F32),),
        in_specs=vm(len(ins)) + hb(len(held)),
        out_specs=tuple(hb(len(rows)) + vm(1)),
        scratch_shapes=[pltpu.VMEM((NB, BM, DIM), F32), pltpu.SemaphoreType.DMA((NB,))],
        input_output_aliases={len(ins) + i: o for i, (_, o) in enumerate(held)},
        cost_estimate=pl.CostEstimate(flops=2 * total * DIM * SEQ, bytes_accessed=4 * total * DIM, transcendentals=0),
        compiler_params=pltpu.CompilerParams(vmem_limit_bytes=16 * 2 ** 20),
    )(*ins, *[h for h, _ in held])
    return outs, token


def emb_kernel(tok, gx, gains, hid, out, ga_o, gm_o, hid_o, buf, sem, out_sem):
    extra = (
        pltpu.make_async_copy(gains.at[pl.ds(0, 1)], ga_o, out_sem.at[0]),
        pltpu.make_async_copy(gains.at[pl.ds(1, 1)], gm_o, out_sem.at[1]),
        pltpu.make_async_copy(hid, hid_o, out_sem.at[2]),
    )
    for e in extra:
        e.start()
    base = lax.axis_index("tp") * VLOC
    ids = jnp.broadcast_to(tok[...], (BM, SEQ)) - base
    row = lax.broadcasted_iota(jnp.int32, (BM, SEQ), 0)
    grad = gx[...].reshape(SEQ, DIM)

    def copy(i):
        slot = lax.rem(i, NB)
        return pltpu.make_async_copy(buf.at[slot], out.at[pl.ds(pl.multiple_of(i * BM, BM), BM)], sem.at[slot])

    def step(i, carry):
        @pl.when(i >= NB)
        def _():
            copy(i).wait()
        hot = jnp.where(ids == row + i * BM, 1.0, 0.0).astype(BF)
        buf[lax.rem(i, NB)] = nn(hot, grad)
        copy(i).start()
        return carry
    steps = VLOC // BM
    lax.fori_loop(0, steps, step, 0)
    for k in range(steps - NB, steps):
        copy(k).wait()
    for e in extra:
        e.wait()


def sds(shape, dtype=BF):
    return jax.ShapeDtypeStruct(shape, dtype)


FULL = (2, 2, 32, DIM)
MINE = (2, 32, DIM)


def dma(*shape):
    return pltpu.SemaphoreType.DMA(shape)


def device_fn(tokens, positions, emb, gain_a, gain_m, wq, wk, wv, wo, wg, wu, wd, gh):
    inv_freq = (ROPE_THETA ** (-np.arange(HD // 2, dtype=np.float32) * np.float32(2.0 / HD))).astype(np.float32)
    freq = jnp.asarray(np.tile(inv_freq, 4)[None, :])
    ga, gm = gain_a.reshape(1, DIM), gain_m.reshape(1, DIM)
    flat = lambda w: jnp.transpose(w, (1, 2, 0)).reshape(-1, DIM)
    wqt, wkt, wvt = flat(wq), flat(wk), flat(wv)
    wo2 = wo.reshape(QC, DIM)
    gh2 = gh.reshape(32, DIM)

    n1, x0, qkv, cs, heads, h1, n2, act, ggate, gup, gfull, gn2, wqkv_v, wo_v, wd_v = pl.pallas_call(
        front_kernel,
        out_shape=(on(FULL), on(MINE), on((SEQ, QKV)), on((2, SEQ, 128), F32), on((SEQ, QC)), on(MINE),
                   on(FULL), on((SEQ, FLOC)), on((SEQ, FLOC)), on((SEQ, FLOC)), on(FULL), on(MINE),
                   on((QKV, DIM)), on((QC, DIM)), on((FLOC, DIM))),
        in_specs=hb(14),
        out_specs=tuple(vm(15)),
        scratch_shapes=[
            pltpu.VMEM((1, SEQ), jnp.int32), pltpu.VMEM((1, SEQ), jnp.int32), pltpu.VMEM((1, SEQ), F32),
            pltpu.VMEM((1, DIM), F32), pltpu.VMEM((1, DIM), F32),
            pltpu.VMEM((VLOC, DIM), BF), pltpu.VMEM((DIM, FLOC), BF), pltpu.VMEM((DIM, FLOC), BF),
            pltpu.VMEM((FLOC, DIM), BF), pltpu.VMEM((DIM, QKV), BF),
            pltpu.VMEM((SEQ, VLOC), BF), pltpu.VMEM((SEQ, FLOC), BF),
            pltpu.VMEM(FULL, BF), pltpu.VMEM(MINE, BF), pltpu.VMEM(MINE, BF), pltpu.VMEM(MINE, BF),
            pltpu.VMEM(FULL, BF), pltpu.VMEM(MINE, BF), pltpu.VMEM(MINE, BF), pltpu.VMEM(MINE, BF),
            pltpu.VMEM(FULL, BF), pltpu.VMEM(MINE, BF),
            dma(6), dma(NE), dma(7), dma(3, NE), dma(3, NE), dma(2, NE), dma(2, NE), dma(5), dma(5)],
        compiler_params=pltpu.CompilerParams(collective_id=0, has_side_effects=True, vmem_limit_bytes=42 * 2 ** 20),
    )(tokens, positions, freq, ga, gm, gh2, emb, wqt, wkt, wvt, wo2, wd, wg, wu)

    swap = [(i, i ^ 2) for i in range(4)]
    gn2_got = lax.ppermute(gn2, 'tp', swap)
    gfull2 = gfull.reshape(SEQ, DIM)
    n2f = n2.reshape(SEQ, DIM)
    (g_gate, g_up), token = outer((n2f, ggate, gup), ((0, 1, 0, 0, 0, DIM), (0, 2, 0, 1, 0, UP_FIRST)), (DIM, DIM))

    gh1, gqkv, give, keep, gain_mp = pl.pallas_call(
        middle_kernel,
        out_shape=(on(FULL), on((SEQ, QKV)), on((3, 32, DIM)), on((32, DIM)), on((1, DIM), F32)),
        in_specs=vm(12),
        out_specs=tuple(vm(5)),
        scratch_shapes=[
            pltpu.VMEM((SEQ, QC), BF),
            pltpu.VMEM(FULL, BF), pltpu.VMEM(MINE, BF), pltpu.VMEM(MINE, BF), pltpu.VMEM(FULL, BF), pltpu.VMEM(MINE, BF),
            dma(2, NC), dma(2, NC), dma(1), dma(1)],
        compiler_params=pltpu.CompilerParams(collective_id=1, has_side_effects=True, vmem_limit_bytes=8 * 2 ** 20),
    )(gn2, gn2_got, act, h1, gfull, gm, qkv, cs, wqkv_v, wo_v, wd_v, token)

    got = lax.ppermute(give, 'tp', swap)
    (g_up, g_down, g_out, g_q, g_k, g_v), token2 = outer(
        (n2f, gup, act, gfull2, heads, gh1.reshape(SEQ, DIM), gqkv, n1.reshape(SEQ, DIM)),
        ((0, 1, UP_FIRST, 0, UP_FIRST, DIM - UP_FIRST), (2, 3, 0, 1, 0, FLOC), (4, 5, 0, 2, 0, QC),
         (6, 7, 0, 3, 0, QC), (6, 7, QC, 4, 0, KC), (6, 7, QC + KC, 5, 0, KC)),
        (DIM, FLOC, QC, QC, KC, KC), ((g_up, 0),))

    gx, gains, hid = pl.pallas_call(
        back_kernel,
        out_shape=(on(FULL), on((2, DIM), F32), on((32, DIM))),
        in_specs=vm(9),
        out_specs=tuple(vm(3)),
        scratch_shapes=[pltpu.VMEM((2, 8, DIM), F32), dma(2), dma(2)],
        compiler_params=pltpu.CompilerParams(collective_id=2, has_side_effects=True, vmem_limit_bytes=8 * 2 ** 20),
    )(give, got, keep, h1, x0, gh1, ga, gain_mp, token2)

    g_emb, gain_1, gain_2, hidden = pl.pallas_call(
        emb_kernel,
        out_shape=(sds((VLOC, DIM), F32), sds((1, DIM), F32), sds((1, DIM), F32), sds((32, DIM))),
        in_specs=vm(4),
        out_specs=tuple(hb(4)),
        scratch_shapes=[pltpu.VMEM((NB, BM, DIM), F32), dma(NB), dma(3)],
        compiler_params=pltpu.CompilerParams(vmem_limit_bytes=24 * 2 ** 20),
    )(tokens, gx, gains, hid)

    back3 = lambda g: jnp.transpose(g.reshape(-1, HD, DIM), (2, 0, 1))
    return (hidden.reshape(1, 32, DIM), g_emb, back3(g_q), back3(g_k), back3(g_v), g_out.reshape(HLOC, HD, DIM),
            g_gate, g_up, g_down, gain_1.reshape(DIM), gain_2.reshape(DIM))


def solution(mesh):
    in_specs = (P('dp', None), P('dp', None), P('tp', None), P(None), P(None),
                P(None, 'tp', None), P(None, 'tp', None), P(None, 'tp', None), P('tp', None, None),
                P(None, 'tp'), P(None, 'tp'), P('tp', None), P('dp', 'tp', None))
    out_specs = (P('dp', 'tp', None), P(('dp', 'tp'), None),
                 P('dp', 'tp', None), P('dp', 'tp', None), P('dp', 'tp', None), P(('dp', 'tp'), None, None),
                 P('dp', 'tp'), P('dp', 'tp'), P(('dp', 'tp'), None), P('dp'), P('dp'))
    return jax.shard_map(device_fn, mesh=mesh, in_specs=in_specs, out_specs=out_specs, check_vma=False)
```

```python
import functools

import jax
import jax.numpy as jnp
import numpy as np
from jax import lax
from jax.experimental import pallas as pl
from jax.experimental.pallas import tpu as pltpu
from jax.sharding import PartitionSpec as P

ROPE_THETA = 1000000.0
RMS_EPS = 1e-5
MESH = pl.DeviceIdType.MESH
BF = jnp.bfloat16
F32 = jnp.float32

SEQ = 128
DIM = 2048
VLOC = 2048
FLOC = 2048
HLOC = 8
KVLOC = 2
HD = 64
QC = HLOC * HD
KC = KVLOC * HD
QKV = QC + 2 * KC
GROUP = HLOC // KVLOC
SCALE = HD ** -0.5
NC = 4
W = DIM // NC
NE = 8
WE = DIM // NE
AHEAD = 6
NB2 = 2
WB = DIM // NB2
LAG = 2
VMEM = pltpu.VMEM
HBM = pltpu.HBM


def nn(a, b):
    return lax.dot_general(a, b, (((1,), (0,)), ((), ())), preferred_element_type=F32)


def nt(a, b):
    return lax.dot_general(a, b, (((1,), (1,)), ((), ())), preferred_element_type=F32)


def tn(a, b):
    return lax.dot_general(a, b, (((0,), (0,)), ((), ())), preferred_element_type=F32)


def place():
    tp = lax.axis_index("tp")
    x = tp // 2
    c = tp - 2 * x
    return x, c, 2 * x + (1 - c), 2 * (1 - x) + c


def greet(*peers):
    sem = pltpu.get_barrier_semaphore()
    for peer in peers:
        pl.semaphore_signal(sem, inc=1, device_id={"tp": peer}, device_id_type=MESH)
    return lambda: pl.semaphore_wait(sem, len(peers))


def remote(src, dst, send, recv, peer):
    return pltpu.make_async_remote_copy(
        src_ref=src, dst_ref=dst, send_sem=send, recv_sem=recv, device_id={"tp": peer}, device_id_type=MESH)


def cols(j, width=W):
    return pl.ds(pl.multiple_of(j * width, width), width)


class PairSum:
    def __init__(self, part, got, own, sems, c, partner, n=NC):
        self.part, self.got, self.own, self.c, self.partner = part, got, own, c, partner
        self.send, self.recv = sems
        self.n, self.width = n, DIM // n

    def copy(self, j):
        return remote(self.part.at[:, 1 - self.c, :, cols(j, self.width)], self.got.at[:, :, cols(j, self.width)],
                      self.send.at[j], self.recv.at[j], self.partner)

    def put(self, j, value):
        self.part[:, :, :, cols(j, self.width)] = value.astype(BF).reshape(2, 2, 32, self.width)
        self.copy(j).start()

    def take(self, j):
        self.copy(j).wait_recv()
        total = self.part[:, self.c, :, cols(j, self.width)].astype(F32) + self.got[:, :, cols(j, self.width)].astype(F32)
        self.own[0:2, :, cols(j, self.width)] = total.astype(BF)

    def send_all(self, chunk):
        def body(j, carry):
            self.put(j, chunk(j))
            return carry
        lax.fori_loop(0, self.n, body, 0)

    def run(self, chunk, then=lambda j: None, lag=None):
        lag = lag or self.n

        def finish(j):
            self.take(j)
            then(j)

        def body(j, carry):
            self.put(j, chunk(j))
            if lag < self.n:
                @pl.when(j >= lag)
                def _():
                    finish(j - lag)
            return carry
        lax.fori_loop(0, self.n, body, 0)
        for j in range(self.n - lag, self.n):
            finish(j)

    def drain(self):
        for j in range(self.n):
            self.copy(j).wait_send()


def rows16(fn):
    for b in range(2):
        for r in range(0, 32, 16):
            fn(b, slice(r, r + 16))


def norm_rows(x, gain):
    inv = lax.rsqrt(jnp.mean(x * x, axis=-1, keepdims=True) + RMS_EPS)
    return (x * inv * gain).astype(BF)


def norm_back(grad, x, gain):
    inv = lax.rsqrt(jnp.mean(x * x, axis=-1, keepdims=True) + RMS_EPS)
    normed = x * inv
    scaled = grad * gain
    back = inv * (scaled - normed * jnp.mean(scaled * normed, axis=-1, keepdims=True))
    return back, jnp.sum(grad * normed, axis=0, keepdims=True)


def spread(row):
    return jnp.transpose(jnp.broadcast_to(row, (SEQ, SEQ)))


def rope_pair(values, cos_tab, sin_tab):
    lane = lax.broadcasted_iota(jnp.int32, (SEQ, 128), 1)
    low = (lane % HD) < HD // 2
    other = jnp.where(low, pltpu.roll(values, 128 - HD // 2, 1), pltpu.roll(values, HD // 2, 1))
    return values * cos_tab + other * jnp.where(low, -sin_tab, sin_tab)


def stack(ref, g):
    return jnp.concatenate([ref[:, h * HD:(h + 1) * HD] for h in range(g * GROUP, (g + 1) * GROUP)], axis=0)


def unstack(ref, g, value, fix=lambda pair: pair):
    for i in range(0, GROUP, 2):
        lo = (g * GROUP + i) * HD
        pair = jnp.concatenate([value[i * SEQ:(i + 1) * SEQ], value[(i + 1) * SEQ:(i + 2) * SEQ]], axis=1)
        ref[:, lo:lo + 128] = fix(pair).astype(BF)


def probs_of(q, k):
    scores = nt(q, k) * SCALE
    shape = (GROUP * SEQ, SEQ)
    row = lax.broadcasted_iota(jnp.int32, shape, 0) % SEQ
    scores = jnp.where(row >= lax.broadcasted_iota(jnp.int32, shape, 1), scores, -1e30)
    e = jnp.exp(scores - jnp.max(scores, axis=-1, keepdims=True))
    return e / jnp.sum(e, axis=-1, keepdims=True)


def front_kernel(tok, pos, freq, gain_a, gain_m, gh, emb, wq, wk, wv, wo, wd, wg, wu,
                 n1_o, x0_o, qkv_o, cs_o, heads_o, h1_o, n2_o, act_o, ggate_o, gup_o, gfull_o, gn2_o,
                 wqkv_v, wo_v, wd_v,
                 tok_v, pos_v, freq_v, ga_v, gm_v, emb_v, wg_v, wu_v, wut_v, hot_v, gact_v,
                 p0, g0, s0, r0, p1, g1, s1, r1, p2, g2,
                 in_sem, emb_sem, w_sem, ps, pr, xs, xr, hs, hr):
    x, c, partner, cross = place()
    tp = 2 * x + c

    def fetch_emb(j):
        return pltpu.make_async_copy(emb.at[:, cols(j, WE)], emb_v.at[:, cols(j, WE)], emb_sem.at[j])

    get_q = pltpu.make_async_copy(wq, wqkv_v.at[pl.ds(0, QC)], w_sem.at[0])
    get_k = pltpu.make_async_copy(wk, wqkv_v.at[pl.ds(QC, KC)], w_sem.at[1])
    get_v = pltpu.make_async_copy(wv, wqkv_v.at[pl.ds(QC + KC, KC)], w_sem.at[2])
    get_out = pltpu.make_async_copy(wo, wo_v, w_sem.at[3])
    get_down = pltpu.make_async_copy(wd, wd_v, w_sem.at[4])
    get_gate = pltpu.make_async_copy(wg, wg_v, w_sem.at[5])
    get_up = pltpu.make_async_copy(wu, wu_v, w_sem.at[6])
    get_small = [pltpu.make_async_copy(src, dst, in_sem.at[i]) for i, (src, dst) in enumerate(
        ((tok, tok_v), (pos, pos_v), (freq, freq_v), (gain_a, ga_v), (gain_m, gm_v), (gh, gfull_o.at[x, c])))]
    get_small[0].start()
    for j in range(AHEAD):
        fetch_emb(j).start()
    for g in get_small[1:]:
        g.start()
    met = greet(partner, cross)
    get_small[0].wait()
    ids = spread(tok_v[...].astype(F32))
    base = (tp * VLOC).astype(F32)
    lane = lax.broadcasted_iota(jnp.int32, (SEQ, 128), 1).astype(F32)
    for v in range(VLOC // 128):
        hot_v[:, v * 128:(v + 1) * 128] = jnp.where(ids == lane + (base + float(v * 128)), 1.0, 0.0).astype(BF)

    met()

    def cross_copy(k, src, dst, j):
        cj = cols(j, WE if k == 0 else W)
        return remote(src.at[:, :, cj], dst.at[:, :, cj], xs.at[k, j], xr.at[k, j], cross)

    sum0 = PairSum(p0, g0, s0, (ps.at[0], pr.at[0]), c, partner, NE)

    def lookup(j):
        fetch_emb(j).wait()

        @pl.when(j + AHEAD < NE)
        def _():
            fetch_emb(j + AHEAD).start()

        @pl.when(j == NE - AHEAD)
        def _():
            for g in (get_q, get_k, get_v):
                g.start()
        return nn(hot_v[...], emb_v[:, cols(j, WE)])

    sum0.run(lookup, lambda j: cross_copy(0, s0, r0, j).start(), LAG)
    for g in (get_out, get_up, get_down, get_gate):
        g.start()
    for g in get_small[1:]:
        g.wait()
    mine = gfull_o.at[x, c]
    to_cross = remote(mine, mine, hs.at[0], hr.at[0], cross)
    to_partner = remote(mine, mine, hs.at[1], hr.at[1], partner)
    to_partner.start()
    angle = spread(pos_v[...].astype(F32)) * freq_v[...]
    cs_o[0] = jnp.cos(angle)
    cs_o[1] = jnp.sin(angle)

    wqkvt_v = wut_v
    for g in (get_q, get_k, get_v):
        g.wait()

    def turn_qkv(j, carry):
        rj = pl.ds(pl.multiple_of(j * 256, 256), 256)
        wqkvt_v[:, rj] = jnp.transpose(wqkv_v[rj, :])
        return carry
    lax.fori_loop(0, QKV // 256, turn_qkv, 0)

    for j in range(NE):
        cross_copy(0, s0, r0, j).wait_recv()

    to_cross.start()

    def first(b, r):
        xv = s0[b, r].astype(F32) + r0[b, r].astype(F32)
        x0_o[b, r] = xv.astype(BF)
        n1_o[b, c, r] = norm_rows(xv, ga_v[...])
    rows16(first)
    share1 = remote(n1_o.at[:, c], n1_o.at[:, c], hs.at[2], hr.at[2], partner)
    share1.start()
    share1.wait_recv()

    n1 = n1_o[...].reshape(SEQ, DIM)
    cos_tab, sin_tab = cs_o[0], cs_o[1]

    for v in range(QKV // 256):
        lin = nn(n1, wqkvt_v[:, v * 256:(v + 1) * 256])
        for h in range(2):
            lo = v * 256 + h * 128
            piece = lin[:, h * 128:(h + 1) * 128]
            if lo < QC + KC:
                piece = rope_pair(piece, cos_tab, sin_tab)
            qkv_o[:, lo:lo + 128] = piece.astype(BF)
    for g in range(KVLOC):
        k = qkv_o[:, QC + g * HD:QC + (g + 1) * HD]
        v = qkv_o[:, QC + KC + g * HD:QC + KC + (g + 1) * HD]
        unstack(heads_o, g, nn(probs_of(stack(qkv_o, g), k).astype(BF), v).astype(BF))
    get_out.wait()

    sum1 = PairSum(p1, g1, s1, (ps.at[1], pr.at[1]), c, partner)
    sum1.run(lambda j: nn(heads_o[...], wo_v[:, cols(j)]), lambda j: cross_copy(1, s1, r1, j).start())

    to_cross.wait_recv()
    onward = remote(gfull_o.at[1 - x, c], gfull_o.at[1 - x, c], hs.at[3], hr.at[3], partner)
    onward.start()
    get_up.wait()

    def turn_up(j, carry):
        wut_v[:, cols(j)] = jnp.transpose(wu_v[cols(j), :])
        return carry
    lax.fori_loop(0, NC, turn_up, 0)

    to_partner.wait_recv()
    onward.wait_recv()
    get_down.wait()
    get_gate.wait()
    gfull = gfull_o[...].reshape(SEQ, DIM)
    wgt_v = emb_v

    def grad_act(j, carry):
        gact_v[:, cols(j)] = nt(gfull, wd_v[cols(j), :]).astype(BF)
        wgt_v[:, cols(j)] = jnp.transpose(wg_v[cols(j), :])
        return carry
    lax.fori_loop(0, NC, grad_act, 0)

    for j in range(NC):
        cross_copy(1, s1, r1, j).wait_recv()

    def second(b, r):
        total = s1[b, r].astype(F32) + r1[b, r].astype(F32)
        h1 = (x0_o[b, r].astype(F32) + total).astype(BF)
        h1_o[b, r] = h1
        n2_o[b, c, r] = norm_rows(h1.astype(F32), gm_v[...])
    rows16(second)
    share2 = remote(n2_o.at[:, c], n2_o.at[:, c], hs.at[4], hr.at[4], partner)
    share2.start()
    share2.wait_recv()
    n2 = n2_o[...].reshape(SEQ, DIM)

    def mlp(j, carry):
        cj = cols(j, WB)
        gate = nn(n2, wg_v[:, cj])
        up = nn(n2, wu_v[:, cj])
        sig = jax.nn.sigmoid(gate)
        gate_act = gate * sig
        act_o[:, cj] = (gate_act * up).astype(BF)
        grad = gact_v[:, cj].astype(F32)
        gup_o[:, cj] = (grad * gate_act).astype(BF)
        ggate_o[:, cj] = (grad * up * sig * (1.0 + gate * (1.0 - sig))).astype(BF)
        return carry
    lax.fori_loop(0, FLOC // WB, mlp, 0)

    sum2 = PairSum(p2, g2, gn2_o, (ps.at[2], pr.at[2]), c, partner, NB2)
    sum2.run(lambda j: nn(ggate_o[...], wgt_v[:, cols(j, WB)]) + nn(gup_o[...], wut_v[:, cols(j, WB)]))

    for s in (sum0, sum1, sum2):
        s.drain()
    for j in range(NE):
        cross_copy(0, s0, r0, j).wait_send()
    for j in range(NC):
        cross_copy(1, s1, r1, j).wait_send()
    for copy in (to_cross, to_partner, share1, onward, share2):
        copy.wait_send()


def middle_kernel(gn2_own, gn2_got, act, h1, gfull, gain_m, qkv, cs, wqkv, wo, wd, token,
                  gh1_o, gqkv_o, give_o, keep_o, gain_o,
                  gheads_v, p0, g0, s0, p1, g1, ps, pr, hs, hr):
    x, c, partner, cross = place()
    met = greet(partner)
    gains = []

    def first(b, r):
        grad = (gn2_own[b, r].astype(F32) + gn2_got[b, r].astype(F32)).astype(BF).astype(F32)
        back, part = norm_back(grad, h1[b, r].astype(F32), gain_m[...])
        gh1_o[b, c, r] = (gfull[b, c, r].astype(F32) + back).astype(BF)
        gains.append(part)
    rows16(first)
    met()
    share = remote(gh1_o.at[:, c], gh1_o.at[:, c], hs.at[0], hr.at[0], partner)
    share.start()
    gain_o[...] = gains[0] + gains[1] + gains[2] + gains[3]
    sum0 = PairSum(p0, g0, s0, (ps.at[0], pr.at[0]), c, partner, NB2)
    sum0.send_all(lambda j: nn(act[...], wd[:, cols(j, WB)]))
    share.wait_recv()

    gh1 = gh1_o[...].reshape(SEQ, DIM)
    for v in range(QC // 256):
        gheads_v[:, v * 256:(v + 1) * 256] = nt(gh1, wo[v * 256:(v + 1) * 256, :]).astype(BF)

    cos_tab, sin_tab = cs[0], -cs[1]
    turn_back = lambda pair: rope_pair(pair.astype(F32), cos_tab, sin_tab)
    gks, gvs = [], []
    for g in range(KVLOC):
        k = qkv[:, QC + g * HD:QC + (g + 1) * HD]
        v = qkv[:, QC + KC + g * HD:QC + KC + (g + 1) * HD]
        q, gh = stack(qkv, g), stack(gheads_v, g)
        probs = probs_of(q, k)
        gp = nt(gh, v).astype(BF).astype(F32)
        gvs.append(tn(probs.astype(BF), gh).astype(BF))
        gs = (probs * (gp - jnp.sum(gp * probs, axis=-1, keepdims=True)) * SCALE).astype(BF)
        gks.append(tn(gs, q).astype(BF).astype(F32))
        unstack(gqkv_o, g, nn(gs, k).astype(BF), turn_back)
    gqkv_o[:, QC:QC + KC] = rope_pair(jnp.concatenate(gks, axis=1), cos_tab, sin_tab).astype(BF)
    gqkv_o[:, QC + KC:] = jnp.concatenate(gvs, axis=1)

    sum1 = PairSum(p1, g1, give_o, (ps.at[1], pr.at[1]), c, partner, NB2)
    sum1.send_all(lambda j: nn(gqkv_o[...], wqkv[:, cols(j, WB)]))
    for j in range(NB2):
        sum0.take(j)
    give_o[2] = s0[1 - x]
    keep_o[...] = s0[x]
    for j in range(NB2):
        sum1.take(j)
    sum0.drain()
    sum1.drain()
    share.wait_send()


def back_kernel(give, got, keep, h1, x0, gh1, gain_a, gain_mp, token, gx_o, gain_o, hid_o, gbuf, hs, hr):
    x, c, partner, cross = place()
    met = greet(partner)
    gains = []

    def first(b, r):
        grad = (give[b, r].astype(F32) + got[b, r].astype(F32)).astype(BF).astype(F32)
        back, part = norm_back(grad, x0[b, r].astype(F32), gain_a[...])
        gx_o[b, c, r] = (gh1[b, c, r].astype(F32) + back).astype(BF)
        gains.append(part)
    rows16(first)
    met()
    share = remote(gx_o.at[:, c], gx_o.at[:, c], hs.at[0], hr.at[0], partner)
    share.start()
    gbuf[c, 0:1] = gains[0] + gains[1] + gains[2] + gains[3]
    gbuf[c, 1:2] = gain_mp[...]
    share_gain = remote(gbuf.at[c], gbuf.at[c], hs.at[1], hr.at[1], partner)
    share_gain.start()
    hid_o[...] = (h1[x].astype(F32) + (keep[...].astype(F32) + got[2].astype(F32))).astype(BF)
    share_gain.wait_recv()
    gain_o[...] = gbuf[0, 0:2] + gbuf[1, 0:2]
    share.wait_recv()
    share.wait_send()
    share_gain.wait_send()


def vm(n):
    return [pl.BlockSpec(memory_space=VMEM)] * n


def hb(n):
    return [pl.BlockSpec(memory_space=HBM)] * n


def on(shape, dtype=BF):
    return pltpu.VMEM(shape, dtype)


NB = 4
UP_FIRST = 768
BM = 256


def outer_kernel(spec, n_in, n_held, *refs):
    n_out = 1 + max(o for _, _, _, o, _, _ in spec)
    ins, outs = refs[:n_in], refs[n_in + n_held:n_in + n_held + n_out]
    token, buf, sem = refs[n_in + n_held + n_out:]
    token[...] = jnp.zeros_like(token)
    done = 0
    flying = {}
    for l, r, off, o, row, rows in spec:
        lhs, rhs, out = ins[l], ins[r], outs[o]
        bm = min(BM, rows)
        steps = rows // bm

        def copy(i, out=out, done=done, bm=bm, row=row):
            slot = lax.rem(i + done, NB)
            where = pl.ds(pl.multiple_of(row + i * bm, bm), bm)
            return pltpu.make_async_copy(buf.at[slot, pl.ds(0, bm)], out.at[where], sem.at[slot])

        def compute(i, lhs=lhs, rhs=rhs, off=off, done=done, bm=bm):
            a = lhs[:, pl.ds(pl.multiple_of(off + i * bm, 128), bm)]
            buf[lax.rem(i + done, NB), 0:bm] = tn(a, rhs[...])

        free = [(done + i) % NB for i in range(min(NB, steps))]
        uniform = steps >= NB and all(flying.get(k, bm) == bm for k in range(NB)) and (not flying or len(flying) == NB)
        if uniform:
            def step(i, carry, copy=copy, compute=compute, waiting=bool(flying)):
                if waiting:
                    copy(i).wait()
                else:
                    @pl.when(i >= NB)
                    def _():
                        copy(i).wait()
                compute(i)
                copy(i).start()
                return carry
            lax.fori_loop(0, steps, step, 0)
            flying = {k: bm for k in range(NB)}
        else:
            for i in range(steps):
                slot = (done + i) % NB
                if slot in flying:
                    size = flying[slot]
                    pltpu.make_async_copy(buf.at[slot, pl.ds(0, size)], outs[0].at[pl.ds(0, size)], sem.at[slot]).wait()
                compute(i)
                copy(i).start()
                flying[slot] = bm
        done += steps
    for slot, size in flying.items():
        pltpu.make_async_copy(buf.at[slot, pl.ds(0, size)], outs[0].at[pl.ds(0, size)], sem.at[slot]).wait()


def outer(ins, spec, rows, held=()):
    total = sum(n for *_, n in spec)
    *outs, token = pl.pallas_call(
        functools.partial(outer_kernel, spec, len(ins), len(held)),
        out_shape=tuple(jax.ShapeDtypeStruct((m, DIM), F32) for m in rows) + (on((8, 128), F32),),
        in_specs=vm(len(ins)) + hb(len(held)),
        out_specs=tuple(hb(len(rows)) + vm(1)),
        scratch_shapes=[pltpu.VMEM((NB, BM, DIM), F32), pltpu.SemaphoreType.DMA((NB,))],
        input_output_aliases={len(ins) + i: o for i, (_, o) in enumerate(held)},
        cost_estimate=pl.CostEstimate(flops=2 * total * DIM * SEQ, bytes_accessed=4 * total * DIM, transcendentals=0),
        compiler_params=pltpu.CompilerParams(vmem_limit_bytes=16 * 2 ** 20),
    )(*ins, *[h for h, _ in held])
    return outs, token


def emb_kernel(tok, gx, gains, hid, out, ga_o, gm_o, hid_o, buf, sem, out_sem):
    extra = (
        pltpu.make_async_copy(gains.at[pl.ds(0, 1)], ga_o, out_sem.at[0]),
        pltpu.make_async_copy(gains.at[pl.ds(1, 1)], gm_o, out_sem.at[1]),
        pltpu.make_async_copy(hid, hid_o, out_sem.at[2]),
    )
    for e in extra:
        e.start()
    base = lax.axis_index("tp") * VLOC
    ids = jnp.broadcast_to(tok[...], (BM, SEQ)) - base
    row = lax.broadcasted_iota(jnp.int32, (BM, SEQ), 0)
    grad = gx[...].reshape(SEQ, DIM)

    def copy(i):
        slot = lax.rem(i, NB)
        return pltpu.make_async_copy(buf.at[slot], out.at[pl.ds(pl.multiple_of(i * BM, BM), BM)], sem.at[slot])

    def step(i, carry):
        @pl.when(i >= NB)
        def _():
            copy(i).wait()
        hot = jnp.where(ids == row + i * BM, 1.0, 0.0).astype(BF)
        buf[lax.rem(i, NB)] = nn(hot, grad)
        copy(i).start()
        return carry
    steps = VLOC // BM
    lax.fori_loop(0, steps, step, 0)
    for k in range(steps - NB, steps):
        copy(k).wait()
    for e in extra:
        e.wait()


def sds(shape, dtype=BF):
    return jax.ShapeDtypeStruct(shape, dtype)


FULL = (2, 2, 32, DIM)
MINE = (2, 32, DIM)


def dma(*shape):
    return pltpu.SemaphoreType.DMA(shape)


def device_fn(tokens, positions, emb, gain_a, gain_m, wq, wk, wv, wo, wg, wu, wd, gh):
    inv_freq = (ROPE_THETA ** (-np.arange(HD // 2, dtype=np.float32) * np.float32(2.0 / HD))).astype(np.float32)
    freq = jnp.asarray(np.tile(inv_freq, 4)[None, :])
    ga, gm = gain_a.reshape(1, DIM), gain_m.reshape(1, DIM)
    flat = lambda w: jnp.transpose(w, (1, 2, 0)).reshape(-1, DIM)
    wqt, wkt, wvt = flat(wq), flat(wk), flat(wv)
    wo2 = wo.reshape(QC, DIM)
    gh2 = gh.reshape(32, DIM)

    n1, x0, qkv, cs, heads, h1, n2, act, ggate, gup, gfull, gn2, wqkv_v, wo_v, wd_v = pl.pallas_call(
        front_kernel,
        out_shape=(on(FULL), on(MINE), on((SEQ, QKV)), on((2, SEQ, 128), F32), on((SEQ, QC)), on(MINE),
                   on(FULL), on((SEQ, FLOC)), on((SEQ, FLOC)), on((SEQ, FLOC)), on(FULL), on(MINE),
                   on((QKV, DIM)), on((QC, DIM)), on((FLOC, DIM))),
        in_specs=hb(14),
        out_specs=tuple(vm(15)),
        scratch_shapes=[
            pltpu.VMEM((1, SEQ), jnp.int32), pltpu.VMEM((1, SEQ), jnp.int32), pltpu.VMEM((1, SEQ), F32),
            pltpu.VMEM((1, DIM), F32), pltpu.VMEM((1, DIM), F32),
            pltpu.VMEM((VLOC, DIM), BF), pltpu.VMEM((DIM, FLOC), BF), pltpu.VMEM((DIM, FLOC), BF),
            pltpu.VMEM((FLOC, DIM), BF),
            pltpu.VMEM((SEQ, VLOC), BF), pltpu.VMEM((SEQ, FLOC), BF),
            pltpu.VMEM(FULL, BF), pltpu.VMEM(MINE, BF), pltpu.VMEM(MINE, BF), pltpu.VMEM(MINE, BF),
            pltpu.VMEM(FULL, BF), pltpu.VMEM(MINE, BF), pltpu.VMEM(MINE, BF), pltpu.VMEM(MINE, BF),
            pltpu.VMEM(FULL, BF), pltpu.VMEM(MINE, BF),
            dma(6), dma(NE), dma(7), dma(3, NE), dma(3, NE), dma(2, NE), dma(2, NE), dma(5), dma(5)],
        compiler_params=pltpu.CompilerParams(collective_id=0, has_side_effects=True, vmem_limit_bytes=44 * 2 ** 20),
    )(tokens, positions, freq, ga, gm, gh2, emb, wqt, wkt, wvt, wo2, wd, wg, wu)

    swap = [(i, i ^ 2) for i in range(4)]
    gn2_got = lax.ppermute(gn2, 'tp', swap)
    gfull2 = gfull.reshape(SEQ, DIM)
    n2f = n2.reshape(SEQ, DIM)
    (g_gate, g_up), token = outer((n2f, ggate, gup), ((0, 1, 0, 0, 0, DIM), (0, 2, 0, 1, 0, UP_FIRST)), (DIM, DIM))

    gh1, gqkv, give, keep, gain_mp = pl.pallas_call(
        middle_kernel,
        out_shape=(on(FULL), on((SEQ, QKV)), on((3, 32, DIM)), on((32, DIM)), on((1, DIM), F32)),
        in_specs=vm(12),
        out_specs=tuple(vm(5)),
        scratch_shapes=[
            pltpu.VMEM((SEQ, QC), BF),
            pltpu.VMEM(FULL, BF), pltpu.VMEM(MINE, BF), pltpu.VMEM(MINE, BF), pltpu.VMEM(FULL, BF), pltpu.VMEM(MINE, BF),
            dma(2, NC), dma(2, NC), dma(1), dma(1)],
        compiler_params=pltpu.CompilerParams(collective_id=1, has_side_effects=True, vmem_limit_bytes=8 * 2 ** 20),
    )(gn2, gn2_got, act, h1, gfull, gm, qkv, cs, wqkv_v, wo_v, wd_v, token)

    got = lax.ppermute(give, 'tp', swap)
    (g_up, g_down, g_out, g_q, g_k, g_v), token2 = outer(
        (n2f, gup, act, gfull2, heads, gh1.reshape(SEQ, DIM), gqkv, n1.reshape(SEQ, DIM)),
        ((0, 1, UP_FIRST, 0, UP_FIRST, DIM - UP_FIRST), (2, 3, 0, 1, 0, FLOC), (4, 5, 0, 2, 0, QC),
         (6, 7, 0, 3, 0, QC), (6, 7, QC, 4, 0, KC), (6, 7, QC + KC, 5, 0, KC)),
        (DIM, FLOC, QC, QC, KC, KC), ((g_up, 0),))

    gx, gains, hid = pl.pallas_call(
        back_kernel,
        out_shape=(on(FULL), on((2, DIM), F32), on((32, DIM))),
        in_specs=vm(9),
        out_specs=tuple(vm(3)),
        scratch_shapes=[pltpu.VMEM((2, 8, DIM), F32), dma(2), dma(2)],
        compiler_params=pltpu.CompilerParams(collective_id=2, has_side_effects=True, vmem_limit_bytes=8 * 2 ** 20),
    )(give, got, keep, h1, x0, gh1, ga, gain_mp, token2)

    g_emb, gain_1, gain_2, hidden = pl.pallas_call(
        emb_kernel,
        out_shape=(sds((VLOC, DIM), F32), sds((1, DIM), F32), sds((1, DIM), F32), sds((32, DIM))),
        in_specs=vm(4),
        out_specs=tuple(hb(4)),
        scratch_shapes=[pltpu.VMEM((NB, BM, DIM), F32), dma(NB), dma(3)],
        compiler_params=pltpu.CompilerParams(vmem_limit_bytes=24 * 2 ** 20),
    )(tokens, gx, gains, hid)

    back3 = lambda g: jnp.transpose(g.reshape(-1, HD, DIM), (2, 0, 1))
    return (hidden.reshape(1, 32, DIM), g_emb, back3(g_q), back3(g_k), back3(g_v), g_out.reshape(HLOC, HD, DIM),
            g_gate, g_up, g_down, gain_1.reshape(DIM), gain_2.reshape(DIM))


def solution(mesh):
    in_specs = (P('dp', None), P('dp', None), P('tp', None), P(None), P(None),
                P(None, 'tp', None), P(None, 'tp', None), P(None, 'tp', None), P('tp', None, None),
                P(None, 'tp'), P(None, 'tp'), P('tp', None), P('dp', 'tp', None))
    out_specs = (P('dp', 'tp', None), P(('dp', 'tp'), None),
                 P('dp', 'tp', None), P('dp', 'tp', None), P('dp', 'tp', None), P(('dp', 'tp'), None, None),
                 P('dp', 'tp'), P('dp', 'tp'), P(('dp', 'tp'), None), P('dp'), P('dp'))
    return jax.shard_map(device_fn, mesh=mesh, in_specs=in_specs, out_specs=out_specs, check_vma=False)
```

```python
import functools

import jax
import jax.numpy as jnp
import numpy as np
from jax import lax
from jax.experimental import pallas as pl
from jax.experimental.pallas import tpu as pltpu
from jax.sharding import PartitionSpec as P

ROPE_THETA = 1000000.0
RMS_EPS = 1e-5
MESH = pl.DeviceIdType.MESH
BF = jnp.bfloat16
F32 = jnp.float32

SEQ = 128
DIM = 2048
VLOC = 2048
FLOC = 2048
HLOC = 8
KVLOC = 2
HD = 64
QC = HLOC * HD
KC = KVLOC * HD
QKV = QC + 2 * KC
GROUP = HLOC // KVLOC
SCALE = HD ** -0.5
NC = 4
W = DIM // NC
NE = 8
WE = DIM // NE
AHEAD = 6
NB2 = 2
WB = DIM // NB2
LAG = 2
VMEM = pltpu.VMEM
HBM = pltpu.HBM


def nn(a, b):
    return lax.dot_general(a, b, (((1,), (0,)), ((), ())), preferred_element_type=F32)


def nt(a, b):
    return lax.dot_general(a, b, (((1,), (1,)), ((), ())), preferred_element_type=F32)


def tn(a, b):
    return lax.dot_general(a, b, (((0,), (0,)), ((), ())), preferred_element_type=F32)


def place():
    tp = lax.axis_index("tp")
    x = tp // 2
    c = tp - 2 * x
    return x, c, 2 * x + (1 - c), 2 * (1 - x) + c


def greet(*peers):
    sem = pltpu.get_barrier_semaphore()
    for peer in peers:
        pl.semaphore_signal(sem, inc=1, device_id={"tp": peer}, device_id_type=MESH)
    return lambda: pl.semaphore_wait(sem, len(peers))


def remote(src, dst, send, recv, peer):
    return pltpu.make_async_remote_copy(
        src_ref=src, dst_ref=dst, send_sem=send, recv_sem=recv, device_id={"tp": peer}, device_id_type=MESH)


def cols(j, width=W):
    return pl.ds(pl.multiple_of(j * width, width), width)


class PairSum:
    def __init__(self, part, got, own, sems, c, partner, n=NC):
        self.part, self.got, self.own, self.c, self.partner = part, got, own, c, partner
        self.send, self.recv = sems
        self.n, self.width = n, DIM // n

    def copy(self, j):
        return remote(self.part.at[:, 1 - self.c, :, cols(j, self.width)], self.got.at[:, :, cols(j, self.width)],
                      self.send.at[j], self.recv.at[j], self.partner)

    def put(self, j, value):
        self.part[:, :, :, cols(j, self.width)] = value.astype(BF).reshape(2, 2, 32, self.width)
        self.copy(j).start()

    def take(self, j):
        self.copy(j).wait_recv()
        total = self.part[:, self.c, :, cols(j, self.width)].astype(F32) + self.got[:, :, cols(j, self.width)].astype(F32)
        self.own[0:2, :, cols(j, self.width)] = total.astype(BF)

    def send_all(self, chunk):
        def body(j, carry):
            self.put(j, chunk(j))
            return carry
        lax.fori_loop(0, self.n, body, 0)

    def run(self, chunk, then=lambda j: None, lag=None):
        lag = lag or self.n

        def finish(j):
            self.take(j)
            then(j)

        def body(j, carry):
            self.put(j, chunk(j))
            if lag < self.n:
                @pl.when(j >= lag)
                def _():
                    finish(j - lag)
            return carry
        lax.fori_loop(0, self.n, body, 0)
        for j in range(self.n - lag, self.n):
            finish(j)

    def drain(self):
        for j in range(self.n):
            self.copy(j).wait_send()


def rows16(fn):
    for b in range(2):
        for r in range(0, 32, 16):
            fn(b, slice(r, r + 16))


def norm_rows(x, gain):
    inv = lax.rsqrt(jnp.mean(x * x, axis=-1, keepdims=True) + RMS_EPS)
    return (x * inv * gain).astype(BF)


def norm_back(grad, x, gain):
    inv = lax.rsqrt(jnp.mean(x * x, axis=-1, keepdims=True) + RMS_EPS)
    normed = x * inv
    scaled = grad * gain
    back = inv * (scaled - normed * jnp.mean(scaled * normed, axis=-1, keepdims=True))
    return back, jnp.sum(grad * normed, axis=0, keepdims=True)


def spread(row):
    return jnp.transpose(jnp.broadcast_to(row, (SEQ, SEQ)))


def rope_pair(values, cos_tab, sin_tab):
    lane = lax.broadcasted_iota(jnp.int32, (SEQ, 128), 1)
    low = (lane % HD) < HD // 2
    other = jnp.where(low, pltpu.roll(values, 128 - HD // 2, 1), pltpu.roll(values, HD // 2, 1))
    return values * cos_tab + other * jnp.where(low, -sin_tab, sin_tab)


def stack(ref, g):
    return jnp.concatenate([ref[:, h * HD:(h + 1) * HD] for h in range(g * GROUP, (g + 1) * GROUP)], axis=0)


def unstack(ref, g, value, fix=lambda pair: pair):
    for i in range(0, GROUP, 2):
        lo = (g * GROUP + i) * HD
        pair = jnp.concatenate([value[i * SEQ:(i + 1) * SEQ], value[(i + 1) * SEQ:(i + 2) * SEQ]], axis=1)
        ref[:, lo:lo + 128] = fix(pair).astype(BF)


def probs_of(q, k):
    scores = nt(q, k) * SCALE
    shape = (GROUP * SEQ, SEQ)
    row = lax.broadcasted_iota(jnp.int32, shape, 0) % SEQ
    scores = jnp.where(row >= lax.broadcasted_iota(jnp.int32, shape, 1), scores, -1e30)
    e = jnp.exp(scores - jnp.max(scores, axis=-1, keepdims=True))
    return e / jnp.sum(e, axis=-1, keepdims=True)


def front_kernel(tok, pos, freq, gain_a, gain_m, gh, emb, wq, wk, wv, wo, wd, wg, wu,
                 n1_o, x0_o, qkv_o, cs_o, heads_o, h1_o, n2_o, act_o, ggate_o, gup_o, gfull_o, gn2_o,
                 wqkv_v, wo_v, wd_v,
                 tok_v, pos_v, freq_v, ga_v, gm_v, emb_v, wg_v, wu_v, wut_v, hot_v, gact_v,
                 p0, g0, s0, r0, p1, g1, s1, r1, p2, g2,
                 in_sem, emb_sem, w_sem, ps, pr, xs, xr, hs, hr):
    x, c, partner, cross = place()
    tp = 2 * x + c

    def fetch_emb(j):
        return pltpu.make_async_copy(emb.at[:, cols(j, WE)], emb_v.at[:, cols(j, WE)], emb_sem.at[j])

    get_q = pltpu.make_async_copy(wq, wqkv_v.at[pl.ds(0, QC)], w_sem.at[0])
    get_k = pltpu.make_async_copy(wk, wqkv_v.at[pl.ds(QC, KC)], w_sem.at[1])
    get_v = pltpu.make_async_copy(wv, wqkv_v.at[pl.ds(QC + KC, KC)], w_sem.at[2])
    get_out = pltpu.make_async_copy(wo, wo_v, w_sem.at[3])
    get_down = pltpu.make_async_copy(wd, wd_v, w_sem.at[4])
    get_gate = pltpu.make_async_copy(wg, wg_v, w_sem.at[5])
    get_up = pltpu.make_async_copy(wu, wu_v, w_sem.at[6])
    get_small = [pltpu.make_async_copy(src, dst, in_sem.at[i]) for i, (src, dst) in enumerate(
        ((tok, tok_v), (pos, pos_v), (freq, freq_v), (gain_a, ga_v), (gain_m, gm_v), (gh, gfull_o.at[x, c])))]
    get_small[0].start()
    for j in range(AHEAD):
        fetch_emb(j).start()
    for g in get_small[1:]:
        g.start()
    met = greet(partner, cross)
    get_small[0].wait()
    ids = spread(tok_v[...].astype(F32))
    base = (tp * VLOC).astype(F32)
    lane = lax.broadcasted_iota(jnp.int32, (SEQ, 128), 1).astype(F32)
    for v in range(VLOC // 128):
        hot_v[:, v * 128:(v + 1) * 128] = jnp.where(ids == lane + (base + float(v * 128)), 1.0, 0.0).astype(BF)

    met()

    def cross_copy(k, src, dst, j):
        cj = cols(j, WE if k == 0 else W)
        return remote(src.at[:, :, cj], dst.at[:, :, cj], xs.at[k, j], xr.at[k, j], cross)

    sum0 = PairSum(p0, g0, s0, (ps.at[0], pr.at[0]), c, partner, NE)

    def lookup(j):
        fetch_emb(j).wait()

        @pl.when(j + AHEAD < NE)
        def _():
            fetch_emb(j + AHEAD).start()

        @pl.when(j == NE - AHEAD)
        def _():
            for g in (get_q, get_k, get_v):
                g.start()
        return nn(hot_v[...], emb_v[:, cols(j, WE)])

    sum0.run(lookup, lambda j: cross_copy(0, s0, r0, j).start(), LAG)
    for g in (get_out, get_up, get_down, get_gate):
        g.start()
    for g in get_small[1:]:
        g.wait()
    mine = gfull_o.at[x, c]
    to_cross = remote(mine, mine, hs.at[0], hr.at[0], cross)
    to_partner = remote(mine, mine, hs.at[1], hr.at[1], partner)
    to_partner.start()
    angle = spread(pos_v[...].astype(F32)) * freq_v[...]
    cs_o[0] = jnp.cos(angle)
    cs_o[1] = jnp.sin(angle)

    wqkvt_v = wut_v
    for g in (get_q, get_k, get_v):
        g.wait()

    def turn_qkv(j, carry):
        rj = pl.ds(pl.multiple_of(j * 256, 256), 256)
        wqkvt_v[:, rj] = jnp.transpose(wqkv_v[rj, :])
        return carry
    lax.fori_loop(0, QKV // 256, turn_qkv, 0)

    for j in range(NE):
        cross_copy(0, s0, r0, j).wait_recv()

    to_cross.start()

    def first(b, r):
        xv = s0[b, r].astype(F32) + r0[b, r].astype(F32)
        x0_o[b, r] = xv.astype(BF)
        n1_o[b, c, r] = norm_rows(xv, ga_v[...])
    rows16(first)
    share1 = remote(n1_o.at[:, c], n1_o.at[:, c], hs.at[2], hr.at[2], partner)
    share1.start()
    share1.wait_recv()

    n1 = n1_o[...].reshape(SEQ, DIM)
    cos_tab, sin_tab = cs_o[0], cs_o[1]

    for v in range(QKV // 256):
        lin = nn(n1, wqkvt_v[:, v * 256:(v + 1) * 256])
        for h in range(2):
            lo = v * 256 + h * 128
            piece = lin[:, h * 128:(h + 1) * 128]
            if lo < QC + KC:
                piece = rope_pair(piece, cos_tab, sin_tab)
            qkv_o[:, lo:lo + 128] = piece.astype(BF)
    for g in range(KVLOC):
        k = qkv_o[:, QC + g * HD:QC + (g + 1) * HD]
        v = qkv_o[:, QC + KC + g * HD:QC + KC + (g + 1) * HD]
        unstack(heads_o, g, nn(probs_of(stack(qkv_o, g), k).astype(BF), v).astype(BF))
    get_out.wait()

    sum1 = PairSum(p1, g1, s1, (ps.at[1], pr.at[1]), c, partner)
    sum1.run(lambda j: nn(heads_o[...], wo_v[:, cols(j)]), lambda j: cross_copy(1, s1, r1, j).start())

    to_cross.wait_recv()
    onward = remote(gfull_o.at[1 - x, c], gfull_o.at[1 - x, c], hs.at[3], hr.at[3], partner)
    onward.start()
    get_up.wait()

    def turn_up(j, carry):
        wut_v[:, cols(j)] = jnp.transpose(wu_v[cols(j), :])
        return carry
    lax.fori_loop(0, NC, turn_up, 0)

    to_partner.wait_recv()
    onward.wait_recv()
    get_down.wait()
    get_gate.wait()
    gfull = gfull_o[...].reshape(SEQ, DIM)
    wgt_v = emb_v

    def grad_act(j, carry):
        gact_v[:, cols(j)] = nt(gfull, wd_v[cols(j), :]).astype(BF)
        wgt_v[:, cols(j)] = jnp.transpose(wg_v[cols(j), :])
        return carry
    lax.fori_loop(0, NC, grad_act, 0)

    for j in range(NC):
        cross_copy(1, s1, r1, j).wait_recv()

    def second(b, r):
        total = s1[b, r].astype(F32) + r1[b, r].astype(F32)
        h1 = (x0_o[b, r].astype(F32) + total).astype(BF)
        h1_o[b, r] = h1
        n2_o[b, c, r] = norm_rows(h1.astype(F32), gm_v[...])
    rows16(second)
    share2 = remote(n2_o.at[:, c], n2_o.at[:, c], hs.at[4], hr.at[4], partner)
    share2.start()
    share2.wait_recv()
    n2 = n2_o[...].reshape(SEQ, DIM)

    def mlp(j, carry):
        cj = cols(j, WB)
        gate = nn(n2, wg_v[:, cj])
        up = nn(n2, wu_v[:, cj])
        sig = jax.nn.sigmoid(gate)
        gate_act = gate * sig
        act_o[:, cj] = (gate_act * up).astype(BF)
        grad = gact_v[:, cj].astype(F32)
        gup_o[:, cj] = (grad * gate_act).astype(BF)
        ggate_o[:, cj] = (grad * up * sig * (1.0 + gate * (1.0 - sig))).astype(BF)
        return carry
    lax.fori_loop(0, FLOC // WB, mlp, 0)

    sum2 = PairSum(p2, g2, gn2_o, (ps.at[2], pr.at[2]), c, partner, NB2)
    sum2.run(lambda j: nn(ggate_o[...], wgt_v[:, cols(j, WB)]) + nn(gup_o[...], wut_v[:, cols(j, WB)]))

    for s in (sum0, sum1, sum2):
        s.drain()
    for j in range(NE):
        cross_copy(0, s0, r0, j).wait_send()
    for j in range(NC):
        cross_copy(1, s1, r1, j).wait_send()
    for copy in (to_cross, to_partner, share1, onward, share2):
        copy.wait_send()


def middle_kernel(gn2_own, gn2_got, part, h1, gfull, gain_m, qkv, cs, wqkv, wo, token,
                  gh1_o, gqkv_o, give_o, keep_o, gain_o,
                  gheads_v, probs_v, g0, s0, p1, g1, ps, pr, hs, hr):
    x, c, partner, cross = place()
    met = greet(partner)
    gains = []

    def first(b, r):
        grad = (gn2_own[b, r].astype(F32) + gn2_got[b, r].astype(F32)).astype(BF).astype(F32)
        back, part = norm_back(grad, h1[b, r].astype(F32), gain_m[...])
        gh1_o[b, c, r] = (gfull[b, c, r].astype(F32) + back).astype(BF)
        gains.append(part)
    rows16(first)
    met()
    share = remote(gh1_o.at[:, c], gh1_o.at[:, c], hs.at[0], hr.at[0], partner)
    share.start()
    gain_o[...] = gains[0] + gains[1] + gains[2] + gains[3]
    sum0 = PairSum(part, g0, s0, (ps.at[0], pr.at[0]), c, partner, 1)
    sum0.copy(0).start()
    for g in range(KVLOC):
        probs_v[g] = probs_of(stack(qkv, g), qkv[:, QC + g * HD:QC + (g + 1) * HD])
    share.wait_recv()

    gh1 = gh1_o[...].reshape(SEQ, DIM)
    for v in range(QC // 256):
        gheads_v[:, v * 256:(v + 1) * 256] = nt(gh1, wo[v * 256:(v + 1) * 256, :]).astype(BF)

    cos_tab, sin_tab = cs[0], -cs[1]
    turn_back = lambda pair: rope_pair(pair.astype(F32), cos_tab, sin_tab)
    gks, gvs = [], []
    for g in range(KVLOC):
        k = qkv[:, QC + g * HD:QC + (g + 1) * HD]
        v = qkv[:, QC + KC + g * HD:QC + KC + (g + 1) * HD]
        q, gh = stack(qkv, g), stack(gheads_v, g)
        probs = probs_v[g]
        gp = nt(gh, v).astype(BF).astype(F32)
        gvs.append(tn(probs.astype(BF), gh).astype(BF))
        gs = (probs * (gp - jnp.sum(gp * probs, axis=-1, keepdims=True)) * SCALE).astype(BF)
        gks.append(tn(gs, q).astype(BF).astype(F32))
        unstack(gqkv_o, g, nn(gs, k).astype(BF), turn_back)
    gqkv_o[:, QC:QC + KC] = rope_pair(jnp.concatenate(gks, axis=1), cos_tab, sin_tab).astype(BF)
    gqkv_o[:, QC + KC:] = jnp.concatenate(gvs, axis=1)

    sum1 = PairSum(p1, g1, give_o, (ps.at[1], pr.at[1]), c, partner, NB2)
    sum1.send_all(lambda j: nn(gqkv_o[...], wqkv[:, cols(j, WB)]))
    sum0.take(0)
    give_o[2] = s0[1 - x]
    keep_o[...] = s0[x]
    for j in range(NB2):
        sum1.take(j)
    sum0.drain()
    sum1.drain()
    share.wait_send()


def back_kernel(give, got, keep, h1, x0, gh1, gain_a, gain_mp, token, gx_o, gain_o, hid_o, gbuf, hs, hr):
    x, c, partner, cross = place()
    met = greet(partner)
    gains = []

    def first(b, r):
        grad = (give[b, r].astype(F32) + got[b, r].astype(F32)).astype(BF).astype(F32)
        back, part = norm_back(grad, x0[b, r].astype(F32), gain_a[...])
        gx_o[b, c, r] = (gh1[b, c, r].astype(F32) + back).astype(BF)
        gains.append(part)
    rows16(first)
    met()
    share = remote(gx_o.at[:, c], gx_o.at[:, c], hs.at[0], hr.at[0], partner)
    share.start()
    gbuf[c, 0:1] = gains[0] + gains[1] + gains[2] + gains[3]
    gbuf[c, 1:2] = gain_mp[...]
    share_gain = remote(gbuf.at[c], gbuf.at[c], hs.at[1], hr.at[1], partner)
    share_gain.start()
    hid_o[...] = (h1[x].astype(F32) + (keep[...].astype(F32) + got[2].astype(F32))).astype(BF)
    share_gain.wait_recv()
    gain_o[...] = gbuf[0, 0:2] + gbuf[1, 0:2]
    share.wait_recv()
    share.wait_send()
    share_gain.wait_send()


def vm(n):
    return [pl.BlockSpec(memory_space=VMEM)] * n


def hb(n):
    return [pl.BlockSpec(memory_space=HBM)] * n


def on(shape, dtype=BF):
    return pltpu.VMEM(shape, dtype)


NB = 3
BM = 512
UP_FIRST = 512
EB = 256
ENB = 4


def outer_kernel(spec, n_in, n_held, side, *refs):
    n_out = 1 + max(o for _, _, _, o, _, _ in spec)
    ins, outs = refs[:n_in], refs[n_in + n_held:n_in + n_held + n_out]
    *part, token, buf, sem = refs[n_in + n_held + n_out:]
    token[...] = jnp.zeros_like(token)
    done = 0
    flying = {}
    for l, r, off, o, row, rows in spec:
        lhs, rhs, out = ins[l], ins[r], outs[o]
        bm = min(BM, rows)
        steps = rows // bm

        def copy(i, out=out, done=done, bm=bm, row=row):
            slot = lax.rem(i + done, NB)
            where = pl.ds(pl.multiple_of(row + i * bm, bm), bm)
            return pltpu.make_async_copy(buf.at[slot, pl.ds(0, bm)], out.at[where], sem.at[slot])

        def compute(i, lhs=lhs, rhs=rhs, off=off, done=done, bm=bm):
            a = lhs[:, pl.ds(pl.multiple_of(off + i * bm, 128), bm)]
            buf[lax.rem(i + done, NB), 0:bm] = tn(a, rhs[...])

        free = [(done + i) % NB for i in range(min(NB, steps))]
        uniform = steps >= NB and all(flying.get(k, bm) == bm for k in range(NB)) and (not flying or len(flying) == NB)
        if uniform:
            def step(i, carry, copy=copy, compute=compute, waiting=bool(flying)):
                if waiting:
                    copy(i).wait()
                else:
                    @pl.when(i >= NB)
                    def _():
                        copy(i).wait()
                compute(i)
                copy(i).start()
                return carry
            lax.fori_loop(0, steps, step, 0)
            flying = {k: bm for k in range(NB)}
        else:
            for i in range(steps):
                slot = (done + i) % NB
                if slot in flying:
                    size = flying[slot]
                    pltpu.make_async_copy(buf.at[slot, pl.ds(0, size)], outs[0].at[pl.ds(0, size)], sem.at[slot]).wait()
                compute(i)
                copy(i).start()
                flying[slot] = bm
        done += steps
        if side and done == steps:
            for j in range(NB2):
                lo, hi = j * WB, (j + 1) * WB
                out = nn(ins[side[0]][...], ins[side[1]][:, lo:hi])
                part[0][:, :, :, lo:hi] = out.astype(BF).reshape(2, 2, 32, WB)
    for slot, size in flying.items():
        pltpu.make_async_copy(buf.at[slot, pl.ds(0, size)], outs[0].at[pl.ds(0, size)], sem.at[slot]).wait()


def outer(ins, spec, rows, held=(), side=()):
    total = sum(n for *_, n in spec)
    extra = (on(FULL),) if side else ()
    return pl.pallas_call(
        functools.partial(outer_kernel, spec, len(ins), len(held), side),
        out_shape=tuple(jax.ShapeDtypeStruct((m, DIM), F32) for m in rows) + extra + (on((8, 128), F32),),
        in_specs=vm(len(ins)) + hb(len(held)),
        out_specs=tuple(hb(len(rows)) + vm(1 + len(extra))),
        scratch_shapes=[pltpu.VMEM((NB, BM, DIM), F32), pltpu.SemaphoreType.DMA((NB,))],
        input_output_aliases={len(ins) + i: o for i, (_, o) in enumerate(held)},
        cost_estimate=pl.CostEstimate(flops=2 * total * DIM * SEQ, bytes_accessed=4 * total * DIM, transcendentals=0),
        compiler_params=pltpu.CompilerParams(vmem_limit_bytes=24 * 2 ** 20),
    )(*ins, *[h for h, _ in held])


def emb_kernel(tok, gx, gains, hid, out, ga_o, gm_o, hid_o, buf, sem, out_sem):
    extra = (
        pltpu.make_async_copy(gains.at[pl.ds(0, 1)], ga_o, out_sem.at[0]),
        pltpu.make_async_copy(gains.at[pl.ds(1, 1)], gm_o, out_sem.at[1]),
        pltpu.make_async_copy(hid, hid_o, out_sem.at[2]),
    )
    for e in extra:
        e.start()
    base = lax.axis_index("tp") * VLOC
    ids = jnp.broadcast_to(tok[...], (EB, SEQ)) - base
    row = lax.broadcasted_iota(jnp.int32, (EB, SEQ), 0)
    grad = gx[...].reshape(SEQ, DIM)

    def copy(i):
        slot = lax.rem(i, ENB)
        return pltpu.make_async_copy(buf.at[slot], out.at[pl.ds(pl.multiple_of(i * EB, EB), EB)], sem.at[slot])

    def step(i, carry):
        @pl.when(i >= ENB)
        def _():
            copy(i).wait()
        hot = jnp.where(ids == row + i * EB, 1.0, 0.0).astype(BF)
        buf[lax.rem(i, ENB)] = nn(hot, grad)
        copy(i).start()
        return carry
    steps = VLOC // EB
    lax.fori_loop(0, steps, step, 0)
    for k in range(steps - ENB, steps):
        copy(k).wait()
    for e in extra:
        e.wait()


def sds(shape, dtype=BF):
    return jax.ShapeDtypeStruct(shape, dtype)


FULL = (2, 2, 32, DIM)
MINE = (2, 32, DIM)


def dma(*shape):
    return pltpu.SemaphoreType.DMA(shape)


def device_fn(tokens, positions, emb, gain_a, gain_m, wq, wk, wv, wo, wg, wu, wd, gh):
    inv_freq = (ROPE_THETA ** (-np.arange(HD // 2, dtype=np.float32) * np.float32(2.0 / HD))).astype(np.float32)
    freq = jnp.asarray(np.tile(inv_freq, 4)[None, :])
    ga, gm = gain_a.reshape(1, DIM), gain_m.reshape(1, DIM)
    flat = lambda w: jnp.transpose(w, (1, 2, 0)).reshape(-1, DIM)
    wqt, wkt, wvt = flat(wq), flat(wk), flat(wv)
    wo2 = wo.reshape(QC, DIM)
    gh2 = gh.reshape(32, DIM)

    n1, x0, qkv, cs, heads, h1, n2, act, ggate, gup, gfull, gn2, wqkv_v, wo_v, wd_v = pl.pallas_call(
        front_kernel,
        out_shape=(on(FULL), on(MINE), on((SEQ, QKV)), on((2, SEQ, 128), F32), on((SEQ, QC)), on(MINE),
                   on(FULL), on((SEQ, FLOC)), on((SEQ, FLOC)), on((SEQ, FLOC)), on(FULL), on(MINE),
                   on((QKV, DIM)), on((QC, DIM)), on((FLOC, DIM))),
        in_specs=hb(14),
        out_specs=tuple(vm(15)),
        scratch_shapes=[
            pltpu.VMEM((1, SEQ), jnp.int32), pltpu.VMEM((1, SEQ), jnp.int32), pltpu.VMEM((1, SEQ), F32),
            pltpu.VMEM((1, DIM), F32), pltpu.VMEM((1, DIM), F32),
            pltpu.VMEM((VLOC, DIM), BF), pltpu.VMEM((DIM, FLOC), BF), pltpu.VMEM((DIM, FLOC), BF),
            pltpu.VMEM((FLOC, DIM), BF),
            pltpu.VMEM((SEQ, VLOC), BF), pltpu.VMEM((SEQ, FLOC), BF),
            pltpu.VMEM(FULL, BF), pltpu.VMEM(MINE, BF), pltpu.VMEM(MINE, BF), pltpu.VMEM(MINE, BF),
            pltpu.VMEM(FULL, BF), pltpu.VMEM(MINE, BF), pltpu.VMEM(MINE, BF), pltpu.VMEM(MINE, BF),
            pltpu.VMEM(FULL, BF), pltpu.VMEM(MINE, BF),
            dma(6), dma(NE), dma(7), dma(3, NE), dma(3, NE), dma(2, NE), dma(2, NE), dma(5), dma(5)],
        compiler_params=pltpu.CompilerParams(collective_id=0, has_side_effects=True, vmem_limit_bytes=44 * 2 ** 20),
    )(tokens, positions, freq, ga, gm, gh2, emb, wqt, wkt, wvt, wo2, wd, wg, wu)

    swap = [(i, i ^ 2) for i in range(4)]
    gn2_got = lax.ppermute(gn2, 'tp', swap)
    gfull2 = gfull.reshape(SEQ, DIM)
    n2f = n2.reshape(SEQ, DIM)
    g_gate, g_up, part, token = outer(
        (n2f, ggate, gup, act, wd_v), ((0, 1, 0, 0, 0, DIM), (0, 2, 0, 1, 0, UP_FIRST)), (DIM, DIM), side=(3, 4))

    gh1, gqkv, give, keep, gain_mp = pl.pallas_call(
        middle_kernel,
        out_shape=(on(FULL), on((SEQ, QKV)), on((3, 32, DIM)), on((32, DIM)), on((1, DIM), F32)),
        in_specs=vm(11),
        out_specs=tuple(vm(5)),
        scratch_shapes=[
            pltpu.VMEM((SEQ, QC), BF), pltpu.VMEM((KVLOC, GROUP * SEQ, SEQ), F32),
            pltpu.VMEM(MINE, BF), pltpu.VMEM(MINE, BF), pltpu.VMEM(FULL, BF), pltpu.VMEM(MINE, BF),
            dma(2, NC), dma(2, NC), dma(1), dma(1)],
        compiler_params=pltpu.CompilerParams(collective_id=1, has_side_effects=True, vmem_limit_bytes=8 * 2 ** 20),
    )(gn2, gn2_got, part, h1, gfull, gm, qkv, cs, wqkv_v, wo_v, token)

    got = lax.ppermute(give, 'tp', swap)
    g_up, g_down, g_out, g_q, g_k, g_v, token2 = outer(
        (n2f, gup, act, gfull2, heads, gh1.reshape(SEQ, DIM), gqkv, n1.reshape(SEQ, DIM)),
        ((0, 1, UP_FIRST, 0, UP_FIRST, DIM - UP_FIRST), (2, 3, 0, 1, 0, FLOC), (4, 5, 0, 2, 0, QC),
         (6, 7, 0, 3, 0, QC), (6, 7, QC, 4, 0, KC), (6, 7, QC + KC, 5, 0, KC)),
        (DIM, FLOC, QC, QC, KC, KC), ((g_up, 0),))

    gx, gains, hid = pl.pallas_call(
        back_kernel,
        out_shape=(on(FULL), on((2, DIM), F32), on((32, DIM))),
        in_specs=vm(9),
        out_specs=tuple(vm(3)),
        scratch_shapes=[pltpu.VMEM((2, 8, DIM), F32), dma(2), dma(2)],
        compiler_params=pltpu.CompilerParams(collective_id=2, has_side_effects=True, vmem_limit_bytes=8 * 2 ** 20),
    )(give, got, keep, h1, x0, gh1, ga, gain_mp, token2)

    g_emb, gain_1, gain_2, hidden = pl.pallas_call(
        emb_kernel,
        out_shape=(sds((VLOC, DIM), F32), sds((1, DIM), F32), sds((1, DIM), F32), sds((32, DIM))),
        in_specs=vm(4),
        out_specs=tuple(hb(4)),
        scratch_shapes=[pltpu.VMEM((ENB, EB, DIM), F32), dma(ENB), dma(3)],
        compiler_params=pltpu.CompilerParams(vmem_limit_bytes=24 * 2 ** 20),
    )(tokens, gx, gains, hid)

    back3 = lambda g: jnp.transpose(g.reshape(-1, HD, DIM), (2, 0, 1))
    return (hidden.reshape(1, 32, DIM), g_emb, back3(g_q), back3(g_k), back3(g_v), g_out.reshape(HLOC, HD, DIM),
            g_gate, g_up, g_down, gain_1.reshape(DIM), gain_2.reshape(DIM))


def solution(mesh):
    in_specs = (P('dp', None), P('dp', None), P('tp', None), P(None), P(None),
                P(None, 'tp', None), P(None, 'tp', None), P(None, 'tp', None), P('tp', None, None),
                P(None, 'tp'), P(None, 'tp'), P('tp', None), P('dp', 'tp', None))
    out_specs = (P('dp', 'tp', None), P(('dp', 'tp'), None),
                 P('dp', 'tp', None), P('dp', 'tp', None), P('dp', 'tp', None), P(('dp', 'tp'), None, None),
                 P('dp', 'tp'), P('dp', 'tp'), P(('dp', 'tp'), None), P('dp'), P('dp'))
    return jax.shard_map(device_fn, mesh=mesh, in_specs=in_specs, out_specs=out_specs, check_vma=False)
```

```python
import functools

import jax
import jax.numpy as jnp
import numpy as np
from jax import lax
from jax.experimental import pallas as pl
from jax.experimental.pallas import tpu as pltpu
from jax.sharding import PartitionSpec as P

ROPE_THETA = 1000000.0
RMS_EPS = 1e-5
MESH = pl.DeviceIdType.MESH
BF = jnp.bfloat16
F32 = jnp.float32

SEQ = 128
DIM = 2048
VLOC = 2048
FLOC = 2048
HLOC = 8
KVLOC = 2
HD = 64
QC = HLOC * HD
KC = KVLOC * HD
QKV = QC + 2 * KC
GROUP = HLOC // KVLOC
SCALE = HD ** -0.5
NC = 4
W = DIM // NC
NE = 8
WE = DIM // NE
AHEAD = 6
NB2 = 2
WB = DIM // NB2
LAG = 2
VMEM = pltpu.VMEM
HBM = pltpu.HBM


def nn(a, b):
    return lax.dot_general(a, b, (((1,), (0,)), ((), ())), preferred_element_type=F32)


def nt(a, b):
    return lax.dot_general(a, b, (((1,), (1,)), ((), ())), preferred_element_type=F32)


def tn(a, b):
    return lax.dot_general(a, b, (((0,), (0,)), ((), ())), preferred_element_type=F32)


def place():
    tp = lax.axis_index("tp")
    x = tp // 2
    c = tp - 2 * x
    return x, c, 2 * x + (1 - c), 2 * (1 - x) + c


def greet(*peers):
    sem = pltpu.get_barrier_semaphore()
    for peer in peers:
        pl.semaphore_signal(sem, inc=1, device_id={"tp": peer}, device_id_type=MESH)
    return lambda: pl.semaphore_wait(sem, len(peers))


def remote(src, dst, send, recv, peer):
    return pltpu.make_async_remote_copy(
        src_ref=src, dst_ref=dst, send_sem=send, recv_sem=recv, device_id={"tp": peer}, device_id_type=MESH)


def cols(j, width=W):
    return pl.ds(pl.multiple_of(j * width, width), width)


def dma(*shape):
    return pltpu.SemaphoreType.DMA(shape)


class PairSum:
    def __init__(self, part, got, own, sems, c, partner, n=NC, base=0):
        self.part, self.got, self.own, self.c, self.partner = part, got, own, c, partner
        self.send, self.recv = sems
        self.n, self.width, self.base = n, DIM // n, base

    def copy(self, j):
        return remote(self.part.at[:, 1 - self.c, :, cols(j, self.width)], self.got.at[:, :, cols(j, self.width)],
                      self.send.at[self.base + j], self.recv.at[self.base + j], self.partner)

    def put(self, j, value):
        self.part[:, :, :, cols(j, self.width)] = value.astype(BF).reshape(2, 2, 32, self.width)
        self.copy(j).start()

    def take(self, j):
        self.copy(j).wait_recv()
        total = self.part[:, self.c, :, cols(j, self.width)].astype(F32) + self.got[:, :, cols(j, self.width)].astype(F32)
        self.own[0:2, :, cols(j, self.width)] = total.astype(BF)

    def send_all(self, chunk):
        def body(j, carry):
            self.put(j, chunk(j))
            return carry
        lax.fori_loop(0, self.n, body, 0)

    def run(self, chunk, then=lambda j: None, lag=None):
        lag = lag or self.n

        def finish(j):
            self.take(j)
            then(j)

        def body(j, carry):
            self.put(j, chunk(j))
            if lag < self.n:
                @pl.when(j >= lag)
                def _():
                    finish(j - lag)
            return carry
        lax.fori_loop(0, self.n, body, 0)
        for j in range(self.n - lag, self.n):
            finish(j)

    def drain(self):
        for j in range(self.n):
            self.copy(j).wait_send()


def rows16(fn):
    for b in range(2):
        for r in range(0, 32, 16):
            fn(b, slice(r, r + 16))


def norm_rows(x, gain):
    inv = lax.rsqrt(jnp.mean(x * x, axis=-1, keepdims=True) + RMS_EPS)
    return (x * inv * gain).astype(BF)


def norm_back(grad, x, gain):
    inv = lax.rsqrt(jnp.mean(x * x, axis=-1, keepdims=True) + RMS_EPS)
    normed = x * inv
    scaled = grad * gain
    back = inv * (scaled - normed * jnp.mean(scaled * normed, axis=-1, keepdims=True))
    return back, jnp.sum(grad * normed, axis=0, keepdims=True)


def spread(row):
    return jnp.transpose(jnp.broadcast_to(row, (SEQ, SEQ)))


def rope_pair(values, cos_tab, sin_tab):
    lane = lax.broadcasted_iota(jnp.int32, (SEQ, 128), 1)
    low = (lane % HD) < HD // 2
    other = jnp.where(low, pltpu.roll(values, 128 - HD // 2, 1), pltpu.roll(values, HD // 2, 1))
    return values * cos_tab + other * jnp.where(low, -sin_tab, sin_tab)


def stack(ref, g):
    return jnp.concatenate([ref[:, h * HD:(h + 1) * HD] for h in range(g * GROUP, (g + 1) * GROUP)], axis=0)


def unstack(ref, g, value, fix=lambda pair: pair):
    for i in range(0, GROUP, 2):
        lo = (g * GROUP + i) * HD
        pair = jnp.concatenate([value[i * SEQ:(i + 1) * SEQ], value[(i + 1) * SEQ:(i + 2) * SEQ]], axis=1)
        ref[:, lo:lo + 128] = fix(pair).astype(BF)


def probs_of(q, k):
    scores = nt(q, k) * SCALE
    shape = (GROUP * SEQ, SEQ)
    row = lax.broadcasted_iota(jnp.int32, shape, 0) % SEQ
    scores = jnp.where(row >= lax.broadcasted_iota(jnp.int32, shape, 1), scores, -1e30)
    e = jnp.exp(scores - jnp.max(scores, axis=-1, keepdims=True))
    return e / jnp.sum(e, axis=-1, keepdims=True)


def front_kernel(tok, pos, freq, gain_a, gain_m, gh, emb, wq, wk, wv, wo, wd, wg, wu,
                 n1_o, x0_o, qkv_o, cs_o, heads_o, h1_o, n2_o, act_o, ggate_o, gup_o, gfull_o, gn2_o,
                 wqkv_v, wo_v, wd_v,
                 tok_v, pos_v, freq_v, ga_v, gm_v, emb_v, wg_v, wu_v, wut_v, hot_v, gact_v,
                 p0, g0, s0, r0, p1, g1, s1, r1, p2, g2,
                 in_sem, emb_sem, w_sem, ps, pr, xs, xr, hs, hr):
    x, c, partner, cross = place()
    tp = 2 * x + c

    def fetch_emb(j):
        return pltpu.make_async_copy(emb.at[:, cols(j, WE)], emb_v.at[:, cols(j, WE)], emb_sem.at[j])

    get_q = pltpu.make_async_copy(wq, wqkv_v.at[pl.ds(0, QC)], w_sem.at[0])
    get_k = pltpu.make_async_copy(wk, wqkv_v.at[pl.ds(QC, KC)], w_sem.at[1])
    get_v = pltpu.make_async_copy(wv, wqkv_v.at[pl.ds(QC + KC, KC)], w_sem.at[2])
    get_out = pltpu.make_async_copy(wo, wo_v, w_sem.at[3])
    get_down = pltpu.make_async_copy(wd, wd_v, w_sem.at[4])
    get_gate = pltpu.make_async_copy(wg, wg_v, w_sem.at[5])
    get_up = pltpu.make_async_copy(wu, wu_v, w_sem.at[6])
    get_small = [pltpu.make_async_copy(src, dst, in_sem.at[i]) for i, (src, dst) in enumerate(
        ((tok, tok_v), (pos, pos_v), (freq, freq_v), (gain_a, ga_v), (gain_m, gm_v), (gh, gfull_o.at[x, c])))]
    get_small[0].start()
    for j in range(AHEAD):
        fetch_emb(j).start()
    for g in get_small[1:]:
        g.start()
    met = greet(partner, cross)
    get_small[0].wait()
    ids = spread(tok_v[...].astype(F32))
    base = (tp * VLOC).astype(F32)
    lane = lax.broadcasted_iota(jnp.int32, (SEQ, 128), 1).astype(F32)
    for v in range(VLOC // 128):
        hot_v[:, v * 128:(v + 1) * 128] = jnp.where(ids == lane + (base + float(v * 128)), 1.0, 0.0).astype(BF)

    met()

    def cross_copy(k, src, dst, j):
        cj = cols(j, WE if k == 0 else W)
        return remote(src.at[:, :, cj], dst.at[:, :, cj], xs.at[k * NE + j], xr.at[k * NE + j], cross)

    sum0 = PairSum(p0, g0, s0, (ps, pr), c, partner, NE)

    def lookup(j):
        fetch_emb(j).wait()

        @pl.when(j + AHEAD < NE)
        def _():
            fetch_emb(j + AHEAD).start()

        @pl.when(j == NE - AHEAD)
        def _():
            for g in (get_q, get_k, get_v):
                g.start()
        return nn(hot_v[...], emb_v[:, cols(j, WE)])

    sum0.run(lookup, lambda j: cross_copy(0, s0, r0, j).start(), LAG)
    for g in (get_out, get_up, get_down, get_gate):
        g.start()
    for g in get_small[1:]:
        g.wait()
    mine = gfull_o.at[x, c]
    to_cross = remote(mine, mine, hs.at[0], hr.at[0], cross)
    to_partner = remote(mine, mine, hs.at[1], hr.at[1], partner)
    to_partner.start()
    angle = spread(pos_v[...].astype(F32)) * freq_v[...]
    cs_o[0] = jnp.cos(angle)
    cs_o[1] = jnp.sin(angle)

    wqkvt_v = wut_v
    for g in (get_q, get_k, get_v):
        g.wait()

    def turn_qkv(j, carry):
        rj = pl.ds(pl.multiple_of(j * 256, 256), 256)
        wqkvt_v[:, rj] = jnp.transpose(wqkv_v[rj, :])
        return carry
    lax.fori_loop(0, QKV // 256, turn_qkv, 0)

    for j in range(NE):
        cross_copy(0, s0, r0, j).wait_recv()

    to_cross.start()

    def first(b, r):
        xv = s0[b, r].astype(F32) + r0[b, r].astype(F32)
        x0_o[b, r] = xv.astype(BF)
        n1_o[b, c, r] = norm_rows(xv, ga_v[...])
    rows16(first)
    share1 = remote(n1_o.at[:, c], n1_o.at[:, c], hs.at[2], hr.at[2], partner)
    share1.start()
    share1.wait_recv()

    n1 = n1_o[...].reshape(SEQ, DIM)
    cos_tab, sin_tab = cs_o[0], cs_o[1]

    lin = nn(n1, wqkvt_v[:, 0:QKV])
    for lo in range(0, QKV, 128):
        piece = lin[:, lo:lo + 128]
        if lo < QC + KC:
            piece = rope_pair(piece, cos_tab, sin_tab)
        qkv_o[:, lo:lo + 128] = piece.astype(BF)
    for g in range(KVLOC):
        k = qkv_o[:, QC + g * HD:QC + (g + 1) * HD]
        v = qkv_o[:, QC + KC + g * HD:QC + KC + (g + 1) * HD]
        unstack(heads_o, g, nn(probs_of(stack(qkv_o, g), k).astype(BF), v).astype(BF))
    get_out.wait()

    sum1 = PairSum(p1, g1, s1, (ps, pr), c, partner, NC, NE)
    sum1.run(lambda j: nn(heads_o[...], wo_v[:, cols(j)]), lambda j: cross_copy(1, s1, r1, j).start())

    to_cross.wait_recv()
    onward = remote(gfull_o.at[1 - x, c], gfull_o.at[1 - x, c], hs.at[3], hr.at[3], partner)
    onward.start()
    get_up.wait()

    def turn_up(j, carry):
        wut_v[:, cols(j)] = jnp.transpose(wu_v[cols(j), :])
        return carry
    lax.fori_loop(0, NC, turn_up, 0)

    to_partner.wait_recv()
    onward.wait_recv()
    get_down.wait()
    get_gate.wait()
    gfull = gfull_o[...].reshape(SEQ, DIM)
    wgt_v = emb_v

    def grad_act(j, carry):
        gact_v[:, cols(j)] = nt(gfull, wd_v[cols(j), :]).astype(BF)
        wgt_v[:, cols(j)] = jnp.transpose(wg_v[cols(j), :])
        return carry
    lax.fori_loop(0, NC, grad_act, 0)

    for j in range(NC):
        cross_copy(1, s1, r1, j).wait_recv()

    def second(b, r):
        total = s1[b, r].astype(F32) + r1[b, r].astype(F32)
        h1 = (x0_o[b, r].astype(F32) + total).astype(BF)
        h1_o[b, r] = h1
        n2_o[b, c, r] = norm_rows(h1.astype(F32), gm_v[...])
    rows16(second)
    share2 = remote(n2_o.at[:, c], n2_o.at[:, c], hs.at[4], hr.at[4], partner)
    share2.start()
    share2.wait_recv()
    n2 = n2_o[...].reshape(SEQ, DIM)

    def mlp(j, carry):
        cj = cols(j, WB)
        gate = nn(n2, wg_v[:, cj])
        up = nn(n2, wu_v[:, cj])
        sig = jax.nn.sigmoid(gate)
        gate_act = gate * sig
        act_o[:, cj] = (gate_act * up).astype(BF)
        grad = gact_v[:, cj].astype(F32)
        gup_o[:, cj] = (grad * gate_act).astype(BF)
        ggate_o[:, cj] = (grad * up * sig * (1.0 + gate * (1.0 - sig))).astype(BF)
        return carry
    lax.fori_loop(0, FLOC // WB, mlp, 0)

    sum2 = PairSum(p2, g2, gn2_o, (ps, pr), c, partner, NB2, NE + NC)
    sum2.run(lambda j: nn(ggate_o[...], wgt_v[:, cols(j, WB)]) + nn(gup_o[...], wut_v[:, cols(j, WB)]))

    for s in (sum0, sum1, sum2):
        s.drain()
    for j in range(NE):
        cross_copy(0, s0, r0, j).wait_send()
    for j in range(NC):
        cross_copy(1, s1, r1, j).wait_send()
    for copy in (to_cross, to_partner, share1, onward, share2):
        copy.wait_send()


def middle_kernel(gn2_own, gn2_got, part, h1, gfull, gain_m, qkv, cs, wqkv, wo, token,
                  gh1_o, gqkv_o, give_o, keep_o, gain_o,
                  gheads_v, probs_v, g0, s0, p1, g1, ps, pr, hs, hr):
    x, c, partner, cross = place()
    met = greet(partner)
    gains = []

    def first(b, r):
        grad = (gn2_own[b, r].astype(F32) + gn2_got[b, r].astype(F32)).astype(BF).astype(F32)
        back, part = norm_back(grad, h1[b, r].astype(F32), gain_m[...])
        gh1_o[b, c, r] = (gfull[b, c, r].astype(F32) + back).astype(BF)
        gains.append(part)
    rows16(first)
    met()
    share = remote(gh1_o.at[:, c], gh1_o.at[:, c], hs.at[0], hr.at[0], partner)
    share.start()
    gain_o[...] = gains[0] + gains[1] + gains[2] + gains[3]
    sum0 = PairSum(part, g0, s0, (ps, pr), c, partner, 1)
    sum0.copy(0).start()
    for g in range(KVLOC):
        probs_v[g] = probs_of(stack(qkv, g), qkv[:, QC + g * HD:QC + (g + 1) * HD])
    share.wait_recv()

    gh1 = gh1_o[...].reshape(SEQ, DIM)
    gheads_v[...] = nt(gh1, wo[...]).astype(BF)

    cos_tab, sin_tab = cs[0], -cs[1]
    turn_back = lambda pair: rope_pair(pair.astype(F32), cos_tab, sin_tab)
    gks, gvs = [], []
    for g in range(KVLOC):
        k = qkv[:, QC + g * HD:QC + (g + 1) * HD]
        v = qkv[:, QC + KC + g * HD:QC + KC + (g + 1) * HD]
        q, gh = stack(qkv, g), stack(gheads_v, g)
        probs = probs_v[g]
        gp = nt(gh, v).astype(BF).astype(F32)
        gvs.append(tn(probs.astype(BF), gh).astype(BF))
        gs = (probs * (gp - jnp.sum(gp * probs, axis=-1, keepdims=True)) * SCALE).astype(BF)
        gks.append(tn(gs, q).astype(BF).astype(F32))
        unstack(gqkv_o, g, nn(gs, k).astype(BF), turn_back)
    gqkv_o[:, QC:QC + KC] = rope_pair(jnp.concatenate(gks, axis=1), cos_tab, sin_tab).astype(BF)
    gqkv_o[:, QC + KC:] = jnp.concatenate(gvs, axis=1)

    sum1 = PairSum(p1, g1, give_o, (ps, pr), c, partner, NB2, 1)
    sum1.send_all(lambda j: nn(gqkv_o[...], wqkv[:, cols(j, WB)]))
    sum0.take(0)
    give_o[2] = s0[1 - x]
    keep_o[...] = s0[x]
    for j in range(NB2):
        sum1.take(j)
    sum0.drain()
    sum1.drain()
    share.wait_send()


def back_kernel(give, got, keep, h1, x0, gh1, gain_a, gain_mp, token, gx_o, gain_o, hid_o, gbuf, hs, hr):
    x, c, partner, cross = place()
    met = greet(partner)
    gains = []

    def first(b, r):
        grad = (give[b, r].astype(F32) + got[b, r].astype(F32)).astype(BF).astype(F32)
        back, part = norm_back(grad, x0[b, r].astype(F32), gain_a[...])
        gx_o[b, c, r] = (gh1[b, c, r].astype(F32) + back).astype(BF)
        gains.append(part)
    rows16(first)
    met()
    share = remote(gx_o.at[:, c], gx_o.at[:, c], hs.at[0], hr.at[0], partner)
    share.start()
    gbuf[c, 0:1] = gains[0] + gains[1] + gains[2] + gains[3]
    gbuf[c, 1:2] = gain_mp[...]
    share_gain = remote(gbuf.at[c], gbuf.at[c], hs.at[1], hr.at[1], partner)
    share_gain.start()
    hid_o[...] = (h1[x].astype(F32) + (keep[...].astype(F32) + got[2].astype(F32))).astype(BF)
    share_gain.wait_recv()
    gain_o[...] = gbuf[0, 0:2] + gbuf[1, 0:2]
    share.wait_recv()
    share.wait_send()
    share_gain.wait_send()


def vm(n):
    return [pl.BlockSpec(memory_space=VMEM)] * n


def hb(n):
    return [pl.BlockSpec(memory_space=HBM)] * n


def on(shape, dtype=BF):
    return pltpu.VMEM(shape, dtype)


NB = 5
BM = 256
UP_FIRST = 768
RAMP = ((0, 64), (64, 64), (128, 128))
EB = 256
ENB = 4


def outer_kernel(spec, n_in, n_held, side, *refs):
    n_out = 1 + max(o for _, _, _, o, _, _ in spec)
    ins, outs = refs[:n_in], refs[n_in + n_held:n_in + n_held + n_out]
    *part, token, buf, sem, ramp, ramp_sem = refs[n_in + n_held + n_out:]
    token[...] = jnp.zeros_like(token)
    done = 0
    flying = {}
    small = []
    for l, r, off, o, row, rows in spec:
        lhs, rhs, out = ins[l], ins[r], outs[o]
        if not small:
            for i, (lo, size) in enumerate(RAMP):
                ramp[lo:lo + size] = tn(lhs[:, off + lo:off + lo + size], rhs[...])
                small.append(pltpu.make_async_copy(
                    ramp.at[pl.ds(lo, size)], out.at[pl.ds(row + lo, size)], ramp_sem.at[i]))
                small[-1].start()
            off, row, rows = off + BM, row + BM, rows - BM
        bm = min(BM, rows)
        steps = rows // bm

        def copy(i, out=out, done=done, bm=bm, row=row):
            slot = lax.rem(i + done, NB)
            where = pl.ds(pl.multiple_of(row + i * bm, bm), bm)
            return pltpu.make_async_copy(buf.at[slot, pl.ds(0, bm)], out.at[where], sem.at[slot])

        def compute(i, lhs=lhs, rhs=rhs, off=off, done=done, bm=bm):
            a = lhs[:, pl.ds(pl.multiple_of(off + i * bm, 128), bm)]
            buf[lax.rem(i + done, NB), 0:bm] = tn(a, rhs[...])

        free = [(done + i) % NB for i in range(min(NB, steps))]
        uniform = steps >= NB and all(flying.get(k, bm) == bm for k in range(NB)) and (not flying or len(flying) == NB)
        if uniform:
            def step(i, carry, copy=copy, compute=compute, waiting=bool(flying)):
                if waiting:
                    copy(i).wait()
                else:
                    @pl.when(i >= NB)
                    def _():
                        copy(i).wait()
                compute(i)
                copy(i).start()
                return carry
            lax.fori_loop(0, steps, step, 0)
            flying = {k: bm for k in range(NB)}
        else:
            for i in range(steps):
                slot = (done + i) % NB
                if slot in flying:
                    size = flying[slot]
                    pltpu.make_async_copy(buf.at[slot, pl.ds(0, size)], outs[0].at[pl.ds(0, size)], sem.at[slot]).wait()
                compute(i)
                copy(i).start()
                flying[slot] = bm
        done += steps
        if side and done == steps:
            for j in range(NB2):
                lo, hi = j * WB, (j + 1) * WB
                out = nn(ins[side[0]][...], ins[side[1]][:, lo:hi])
                part[0][:, :, :, lo:hi] = out.astype(BF).reshape(2, 2, 32, WB)
    for copy in small:
        copy.wait()
    for slot, size in flying.items():
        pltpu.make_async_copy(buf.at[slot, pl.ds(0, size)], outs[0].at[pl.ds(0, size)], sem.at[slot]).wait()


def outer(ins, spec, rows, held=(), side=()):
    total = sum(n for *_, n in spec)
    extra = (on(FULL),) if side else ()
    return pl.pallas_call(
        functools.partial(outer_kernel, spec, len(ins), len(held), side),
        out_shape=tuple(jax.ShapeDtypeStruct((m, DIM), F32) for m in rows) + extra + (on((8, 128), F32),),
        in_specs=vm(len(ins)) + hb(len(held)),
        out_specs=tuple(hb(len(rows)) + vm(1 + len(extra))),
        scratch_shapes=[pltpu.VMEM((NB, BM, DIM), F32), dma(NB), pltpu.VMEM((BM, DIM), F32), dma(len(RAMP))],
        input_output_aliases={len(ins) + i: o for i, (_, o) in enumerate(held)},
        cost_estimate=pl.CostEstimate(flops=2 * total * DIM * SEQ, bytes_accessed=4 * total * DIM, transcendentals=0),
        compiler_params=pltpu.CompilerParams(vmem_limit_bytes=24 * 2 ** 20),
    )(*ins, *[h for h, _ in held])


def emb_kernel(tok, gx, gains, hid, out, ga_o, gm_o, hid_o, buf, sem, out_sem, ramp, ramp_sem):
    base = lax.axis_index("tp") * VLOC
    ids = jnp.broadcast_to(tok[...], (EB, SEQ)) - base
    row = lax.broadcasted_iota(jnp.int32, (EB, SEQ), 0)
    grad = gx[...].reshape(SEQ, DIM)

    small = []
    for i, (lo, size) in enumerate(RAMP):
        hot = jnp.where(ids[:size] == row[:size] + lo, 1.0, 0.0).astype(BF)
        ramp[lo:lo + size] = nn(hot, grad)
        small.append(pltpu.make_async_copy(ramp.at[pl.ds(lo, size)], out.at[pl.ds(lo, size)], ramp_sem.at[i]))
        small[-1].start()
    extra = (
        pltpu.make_async_copy(gains.at[pl.ds(0, 1)], ga_o, out_sem.at[0]),
        pltpu.make_async_copy(gains.at[pl.ds(1, 1)], gm_o, out_sem.at[1]),
        pltpu.make_async_copy(hid, hid_o, out_sem.at[2]),
    )
    for e in extra:
        e.start()

    def copy(i):
        slot = lax.rem(i - 1, ENB)
        return pltpu.make_async_copy(buf.at[slot], out.at[pl.ds(pl.multiple_of(i * EB, EB), EB)], sem.at[slot])

    def step(i, carry):
        @pl.when(i >= ENB + 1)
        def _():
            copy(i).wait()
        hot = jnp.where(ids == row + i * EB, 1.0, 0.0).astype(BF)
        buf[lax.rem(i - 1, ENB)] = nn(hot, grad)
        copy(i).start()
        return carry
    steps = VLOC // EB
    lax.fori_loop(1, steps, step, 0)
    for k in range(steps - ENB, steps):
        copy(k).wait()
    for e in (*small, *extra):
        e.wait()


def sds(shape, dtype=BF):
    return jax.ShapeDtypeStruct(shape, dtype)


FULL = (2, 2, 32, DIM)
MINE = (2, 32, DIM)


def device_fn(tokens, positions, emb, gain_a, gain_m, wq, wk, wv, wo, wg, wu, wd, gh):
    inv_freq = (ROPE_THETA ** (-np.arange(HD // 2, dtype=np.float32) * np.float32(2.0 / HD))).astype(np.float32)
    freq = jnp.asarray(np.tile(inv_freq, 4)[None, :])
    ga, gm = gain_a.reshape(1, DIM), gain_m.reshape(1, DIM)
    flat = lambda w: jnp.transpose(w, (1, 2, 0)).reshape(-1, DIM)
    wqt, wkt, wvt = flat(wq), flat(wk), flat(wv)
    wo2 = wo.reshape(QC, DIM)
    gh2 = gh.reshape(32, DIM)

    n1, x0, qkv, cs, heads, h1, n2, act, ggate, gup, gfull, gn2, wqkv_v, wo_v, wd_v = pl.pallas_call(
        front_kernel,
        out_shape=(on(FULL), on(MINE), on((SEQ, QKV)), on((2, SEQ, 128), F32), on((SEQ, QC)), on(MINE),
                   on(FULL), on((SEQ, FLOC)), on((SEQ, FLOC)), on((SEQ, FLOC)), on(FULL), on(MINE),
                   on((QKV, DIM)), on((QC, DIM)), on((FLOC, DIM))),
        in_specs=hb(14),
        out_specs=tuple(vm(15)),
        scratch_shapes=[
            pltpu.VMEM((1, SEQ), jnp.int32), pltpu.VMEM((1, SEQ), jnp.int32), pltpu.VMEM((1, SEQ), F32),
            pltpu.VMEM((1, DIM), F32), pltpu.VMEM((1, DIM), F32),
            pltpu.VMEM((VLOC, DIM), BF), pltpu.VMEM((DIM, FLOC), BF), pltpu.VMEM((DIM, FLOC), BF),
            pltpu.VMEM((FLOC, DIM), BF),
            pltpu.VMEM((SEQ, VLOC), BF), pltpu.VMEM((SEQ, FLOC), BF),
            pltpu.VMEM(FULL, BF), pltpu.VMEM(MINE, BF), pltpu.VMEM(MINE, BF), pltpu.VMEM(MINE, BF),
            pltpu.VMEM(FULL, BF), pltpu.VMEM(MINE, BF), pltpu.VMEM(MINE, BF), pltpu.VMEM(MINE, BF),
            pltpu.VMEM(FULL, BF), pltpu.VMEM(MINE, BF),
            dma(6), dma(NE), dma(7), dma(NE + NC + NB2), dma(NE + NC + NB2), dma(NE + NC), dma(NE + NC), dma(5), dma(5)],
        compiler_params=pltpu.CompilerParams(collective_id=0, has_side_effects=True, vmem_limit_bytes=44 * 2 ** 20),
    )(tokens, positions, freq, ga, gm, gh2, emb, wqt, wkt, wvt, wo2, wd, wg, wu)

    swap = [(i, i ^ 2) for i in range(4)]
    gn2_got = lax.ppermute(gn2, 'tp', swap)
    gfull2 = gfull.reshape(SEQ, DIM)
    n2f = n2.reshape(SEQ, DIM)
    g_gate, g_up, part, token = outer(
        (n2f, ggate, gup, act, wd_v), ((0, 1, 0, 0, 0, DIM), (0, 2, 0, 1, 0, UP_FIRST)), (DIM, DIM), side=(3, 4))

    gh1, gqkv, give, keep, gain_mp = pl.pallas_call(
        middle_kernel,
        out_shape=(on(FULL), on((SEQ, QKV)), on((3, 32, DIM)), on((32, DIM)), on((1, DIM), F32)),
        in_specs=vm(11),
        out_specs=tuple(vm(5)),
        scratch_shapes=[
            pltpu.VMEM((SEQ, QC), BF), pltpu.VMEM((KVLOC, GROUP * SEQ, SEQ), F32),
            pltpu.VMEM(MINE, BF), pltpu.VMEM(MINE, BF), pltpu.VMEM(FULL, BF), pltpu.VMEM(MINE, BF),
            dma(1 + NB2), dma(1 + NB2), dma(1), dma(1)],
        compiler_params=pltpu.CompilerParams(collective_id=1, has_side_effects=True, vmem_limit_bytes=8 * 2 ** 20),
    )(gn2, gn2_got, part, h1, gfull, gm, qkv, cs, wqkv_v, wo_v, token)

    got = lax.ppermute(give, 'tp', swap)
    g_up, g_down, g_out, g_q, g_k, g_v, token2 = outer(
        (n2f, gup, act, gfull2, heads, gh1.reshape(SEQ, DIM), gqkv, n1.reshape(SEQ, DIM)),
        ((0, 1, UP_FIRST, 0, UP_FIRST, DIM - UP_FIRST), (2, 3, 0, 1, 0, FLOC), (4, 5, 0, 2, 0, QC),
         (6, 7, 0, 3, 0, QC), (6, 7, QC, 4, 0, KC), (6, 7, QC + KC, 5, 0, KC)),
        (DIM, FLOC, QC, QC, KC, KC), ((g_up, 0),))

    gx, gains, hid = pl.pallas_call(
        back_kernel,
        out_shape=(on(FULL), on((2, DIM), F32), on((32, DIM))),
        in_specs=vm(9),
        out_specs=tuple(vm(3)),
        scratch_shapes=[pltpu.VMEM((2, 8, DIM), F32), dma(2), dma(2)],
        compiler_params=pltpu.CompilerParams(collective_id=2, has_side_effects=True, vmem_limit_bytes=8 * 2 ** 20),
    )(give, got, keep, h1, x0, gh1, ga, gain_mp, token2)

    g_emb, gain_1, gain_2, hidden = pl.pallas_call(
        emb_kernel,
        out_shape=(sds((VLOC, DIM), F32), sds((1, DIM), F32), sds((1, DIM), F32), sds((32, DIM))),
        in_specs=vm(4),
        out_specs=tuple(hb(4)),
        scratch_shapes=[pltpu.VMEM((ENB, EB, DIM), F32), dma(ENB), dma(3), pltpu.VMEM((EB, DIM), F32), dma(len(RAMP))],
        compiler_params=pltpu.CompilerParams(vmem_limit_bytes=24 * 2 ** 20),
    )(tokens, gx, gains, hid)

    back3 = lambda g: jnp.transpose(g.reshape(-1, HD, DIM), (2, 0, 1))
    return (hidden.reshape(1, 32, DIM), g_emb, back3(g_q), back3(g_k), back3(g_v), g_out.reshape(HLOC, HD, DIM),
            g_gate, g_up, g_down, gain_1.reshape(DIM), gain_2.reshape(DIM))


def solution(mesh):
    in_specs = (P('dp', None), P('dp', None), P('tp', None), P(None), P(None),
                P(None, 'tp', None), P(None, 'tp', None), P(None, 'tp', None), P('tp', None, None),
                P(None, 'tp'), P(None, 'tp'), P('tp', None), P('dp', 'tp', None))
    out_specs = (P('dp', 'tp', None), P(('dp', 'tp'), None),
                 P('dp', 'tp', None), P('dp', 'tp', None), P('dp', 'tp', None), P(('dp', 'tp'), None, None),
                 P('dp', 'tp'), P('dp', 'tp'), P(('dp', 'tp'), None), P('dp'), P('dp'))
    return jax.shard_map(device_fn, mesh=mesh, in_specs=in_specs, out_specs=out_specs, check_vma=False)
```

```python
import functools

import jax
import jax.numpy as jnp
import numpy as np
from jax import lax
from jax.experimental import pallas as pl
from jax.experimental.pallas import tpu as pltpu
from jax.sharding import PartitionSpec as P

ROPE_THETA = 1000000.0
RMS_EPS = 1e-5
MESH = pl.DeviceIdType.MESH
BF = jnp.bfloat16
F32 = jnp.float32

SEQ = 128
DIM = 2048
VLOC = 2048
FLOC = 2048
HLOC = 8
KVLOC = 2
HD = 64
QC = HLOC * HD
KC = KVLOC * HD
QKV = QC + 2 * KC
GROUP = HLOC // KVLOC
SCALE = HD ** -0.5
NC = 4
W = DIM // NC
NE = 8
WE = DIM // NE
AHEAD = 4
NB2 = 2
WB = DIM // NB2
LAG = 1
VMEM = pltpu.VMEM
HBM = pltpu.HBM


def nn(a, b):
    return lax.dot_general(a, b, (((1,), (0,)), ((), ())), preferred_element_type=F32)


def nt(a, b):
    return lax.dot_general(a, b, (((1,), (1,)), ((), ())), preferred_element_type=F32)


def tn(a, b):
    return lax.dot_general(a, b, (((0,), (0,)), ((), ())), preferred_element_type=F32)


def place():
    tp = lax.axis_index("tp")
    x = tp // 2
    c = tp - 2 * x
    return x, c, 2 * x + (1 - c), 2 * (1 - x) + c


def greet(*peers):
    sem = pltpu.get_barrier_semaphore()
    for peer in peers:
        pl.semaphore_signal(sem, inc=1, device_id={"tp": peer}, device_id_type=MESH)
    return lambda: pl.semaphore_wait(sem, len(peers))


def remote(src, dst, send, recv, peer):
    return pltpu.make_async_remote_copy(
        src_ref=src, dst_ref=dst, send_sem=send, recv_sem=recv, device_id={"tp": peer}, device_id_type=MESH)


def cols(j, width=W):
    return pl.ds(pl.multiple_of(j * width, width), width)


def dma(*shape):
    return pltpu.SemaphoreType.DMA(shape)


class PairSum:
    def __init__(self, part, got, own, sems, c, partner, n=NC, base=0):
        self.part, self.got, self.own, self.c, self.partner = part, got, own, c, partner
        self.send, self.recv = sems
        self.n, self.width, self.base = n, DIM // n, base

    def copy(self, j):
        return remote(self.part.at[:, 1 - self.c, :, cols(j, self.width)], self.got.at[:, :, cols(j, self.width)],
                      self.send.at[self.base + j], self.recv.at[self.base + j], self.partner)

    def put(self, j, value):
        self.part[:, :, :, cols(j, self.width)] = value.astype(BF).reshape(2, 2, 32, self.width)
        self.copy(j).start()

    def take(self, j):
        self.copy(j).wait_recv()
        total = self.part[:, self.c, :, cols(j, self.width)].astype(F32) + self.got[:, :, cols(j, self.width)].astype(F32)
        self.own[0:2, :, cols(j, self.width)] = total.astype(BF)

    def send_all(self, chunk):
        def body(j, carry):
            self.put(j, chunk(j))
            return carry
        lax.fori_loop(0, self.n, body, 0)

    def run(self, chunk, then=lambda j: None, lag=None):
        lag = lag or self.n

        def finish(j):
            self.take(j)
            then(j)

        def body(j, carry):
            self.put(j, chunk(j))
            if lag < self.n:
                @pl.when(j >= lag)
                def _():
                    finish(j - lag)
            return carry
        lax.fori_loop(0, self.n, body, 0)
        for j in range(self.n - lag, self.n):
            finish(j)

    def drain(self):
        for j in range(self.n):
            self.copy(j).wait_send()


def rows16(fn):
    for b in range(2):
        for r in range(0, 32, 16):
            fn(b, slice(r, r + 16))


def norm_rows(x, gain):
    inv = lax.rsqrt(jnp.mean(x * x, axis=-1, keepdims=True) + RMS_EPS)
    return (x * inv * gain).astype(BF)


def norm_back(grad, x, gain):
    inv = lax.rsqrt(jnp.mean(x * x, axis=-1, keepdims=True) + RMS_EPS)
    normed = x * inv
    scaled = grad * gain
    back = inv * (scaled - normed * jnp.mean(scaled * normed, axis=-1, keepdims=True))
    return back, jnp.sum(grad * normed, axis=0, keepdims=True)


def spread(row):
    return jnp.transpose(jnp.broadcast_to(row, (SEQ, SEQ)))


def rope_pair(values, cos_tab, sin_tab):
    lane = lax.broadcasted_iota(jnp.int32, (SEQ, 128), 1)
    low = (lane % HD) < HD // 2
    other = jnp.where(low, pltpu.roll(values, 128 - HD // 2, 1), pltpu.roll(values, HD // 2, 1))
    return values * cos_tab + other * jnp.where(low, -sin_tab, sin_tab)


def stack(ref, g):
    return jnp.concatenate([ref[:, h * HD:(h + 1) * HD] for h in range(g * GROUP, (g + 1) * GROUP)], axis=0)


def unstack(ref, g, value, fix=lambda pair: pair):
    for i in range(0, GROUP, 2):
        lo = (g * GROUP + i) * HD
        pair = jnp.concatenate([value[i * SEQ:(i + 1) * SEQ], value[(i + 1) * SEQ:(i + 2) * SEQ]], axis=1)
        ref[:, lo:lo + 128] = fix(pair).astype(BF)


def probs_of(q, k):
    scores = nt(q, k) * SCALE
    shape = (GROUP * SEQ, SEQ)
    row = lax.broadcasted_iota(jnp.int32, shape, 0) % SEQ
    scores = jnp.where(row >= lax.broadcasted_iota(jnp.int32, shape, 1), scores, -1e30)
    e = jnp.exp(scores - jnp.max(scores, axis=-1, keepdims=True))
    return e / jnp.sum(e, axis=-1, keepdims=True)


def front_kernel(tok, pos, freq, gain_a, gain_m, gh, emb, wq, wk, wv, wo, wd, wg, wu,
                 n1_o, x0_o, qkv_o, cs_o, heads_o, h1_o, n2_o, act_o, ggate_o, gup_o, gfull_o, gn2_o,
                 wqkv_v, wo_v, wd_v,
                 tok_v, pos_v, freq_v, ga_v, gm_v, emb_v, wg_v, wu_v, wut_v, hot_v, gact_v,
                 p0, g0, s0, r0, p1, g1, s1, r1, p2, g2,
                 in_sem, emb_sem, w_sem, ps, pr, xs, xr, hs, hr):
    x, c, partner, cross = place()
    tp = 2 * x + c

    def fetch_emb(j):
        return pltpu.make_async_copy(emb.at[:, cols(j, WE)], emb_v.at[:, cols(j, WE)], emb_sem.at[j])

    get_q = pltpu.make_async_copy(wq, wqkv_v.at[pl.ds(0, QC)], w_sem.at[0])
    get_k = pltpu.make_async_copy(wk, wqkv_v.at[pl.ds(QC, KC)], w_sem.at[1])
    get_v = pltpu.make_async_copy(wv, wqkv_v.at[pl.ds(QC + KC, KC)], w_sem.at[2])
    get_out = pltpu.make_async_copy(wo, wo_v, w_sem.at[3])
    get_down = pltpu.make_async_copy(wd, wd_v, w_sem.at[4])
    get_gate = pltpu.make_async_copy(wg, wg_v, w_sem.at[5])
    get_up = pltpu.make_async_copy(wu, wu_v, w_sem.at[6])
    get_small = [pltpu.make_async_copy(src, dst, in_sem.at[i]) for i, (src, dst) in enumerate(
        ((tok, tok_v), (pos, pos_v), (freq, freq_v), (gain_a, ga_v), (gain_m, gm_v), (gh, gfull_o.at[x, c])))]
    get_small[0].start()
    for j in range(AHEAD):
        fetch_emb(j).start()
    for g in get_small[1:]:
        g.start()
    met = greet(partner, cross)
    get_small[0].wait()
    ids = spread(tok_v[...].astype(F32))
    base = (tp * VLOC).astype(F32)
    lane = lax.broadcasted_iota(jnp.int32, (SEQ, 128), 1).astype(F32)
    for v in range(VLOC // 128):
        hot_v[:, v * 128:(v + 1) * 128] = jnp.where(ids == lane + (base + float(v * 128)), 1.0, 0.0).astype(BF)

    met()

    def cross_copy(k, src, dst, j):
        cj = cols(j, WE if k == 0 else W)
        return remote(src.at[:, :, cj], dst.at[:, :, cj], xs.at[k * NE + j], xr.at[k * NE + j], cross)

    sum0 = PairSum(p0, g0, s0, (ps, pr), c, partner, NE)

    def lookup(j):
        fetch_emb(j).wait()

        @pl.when(j + AHEAD < NE)
        def _():
            fetch_emb(j + AHEAD).start()

        @pl.when(j == NE - AHEAD)
        def _():
            for g in (get_q, get_k, get_v):
                g.start()
        return nn(hot_v[...], emb_v[:, cols(j, WE)])

    sum0.run(lookup, lambda j: cross_copy(0, s0, r0, j).start(), LAG)
    for g in (get_out, get_up, get_down, get_gate):
        g.start()
    for g in get_small[1:]:
        g.wait()
    mine = gfull_o.at[x, c]
    to_cross = remote(mine, mine, hs.at[0], hr.at[0], cross)
    to_partner = remote(mine, mine, hs.at[1], hr.at[1], partner)
    to_partner.start()
    angle = spread(pos_v[...].astype(F32)) * freq_v[...]
    cs_o[0] = jnp.cos(angle)
    cs_o[1] = jnp.sin(angle)

    wqkvt_v = wut_v
    for g in (get_q, get_k, get_v):
        g.wait()

    def turn_qkv(j, carry):
        rj = pl.ds(pl.multiple_of(j * 256, 256), 256)
        wqkvt_v[:, rj] = jnp.transpose(wqkv_v[rj, :])
        return carry
    lax.fori_loop(0, QKV // 256, turn_qkv, 0)

    for j in range(NE):
        cross_copy(0, s0, r0, j).wait_recv()

    to_cross.start()

    def first(b, r):
        xv = s0[b, r].astype(F32) + r0[b, r].astype(F32)
        x0_o[b, r] = xv.astype(BF)
        n1_o[b, c, r] = norm_rows(xv, ga_v[...])
    rows16(first)
    share1 = remote(n1_o.at[:, c], n1_o.at[:, c], hs.at[2], hr.at[2], partner)
    share1.start()
    share1.wait_recv()

    n1 = n1_o[...].reshape(SEQ, DIM)
    cos_tab, sin_tab = cs_o[0], cs_o[1]

    lin = nn(n1, wqkvt_v[:, 0:QKV])
    for lo in range(0, QKV, 128):
        piece = lin[:, lo:lo + 128]
        if lo < QC + KC:
            piece = rope_pair(piece, cos_tab, sin_tab)
        qkv_o[:, lo:lo + 128] = piece.astype(BF)
    for g in range(KVLOC):
        k = qkv_o[:, QC + g * HD:QC + (g + 1) * HD]
        v = qkv_o[:, QC + KC + g * HD:QC + KC + (g + 1) * HD]
        unstack(heads_o, g, nn(probs_of(stack(qkv_o, g), k).astype(BF), v).astype(BF))
    get_out.wait()

    sum1 = PairSum(p1, g1, s1, (ps, pr), c, partner, NC, NE)
    sum1.run(lambda j: nn(heads_o[...], wo_v[:, cols(j)]), lambda j: cross_copy(1, s1, r1, j).start())

    to_cross.wait_recv()
    onward = remote(gfull_o.at[1 - x, c], gfull_o.at[1 - x, c], hs.at[3], hr.at[3], partner)
    onward.start()
    get_up.wait()

    def turn_up(j, carry):
        wut_v[:, cols(j, WB)] = jnp.transpose(wu_v[cols(j, WB), :])
        return carry
    lax.fori_loop(0, NB2, turn_up, 0)

    to_partner.wait_recv()
    onward.wait_recv()
    get_down.wait()
    get_gate.wait()
    gfull = gfull_o[...].reshape(SEQ, DIM)
    wgt_v = emb_v

    def grad_act(j, carry):
        gact_v[:, cols(j, WB)] = nt(gfull, wd_v[cols(j, WB), :]).astype(BF)
        wgt_v[:, cols(j, WB)] = jnp.transpose(wg_v[cols(j, WB), :])
        return carry
    lax.fori_loop(0, NB2, grad_act, 0)

    for j in range(NC):
        cross_copy(1, s1, r1, j).wait_recv()

    def second(b, r):
        total = s1[b, r].astype(F32) + r1[b, r].astype(F32)
        h1 = (x0_o[b, r].astype(F32) + total).astype(BF)
        h1_o[b, r] = h1
        n2_o[b, c, r] = norm_rows(h1.astype(F32), gm_v[...])
    rows16(second)
    share2 = remote(n2_o.at[:, c], n2_o.at[:, c], hs.at[4], hr.at[4], partner)
    share2.start()
    share2.wait_recv()
    n2 = n2_o[...].reshape(SEQ, DIM)

    gate = nn(n2, wg_v[...])
    up = nn(n2, wu_v[...])
    sig = jax.nn.sigmoid(gate)
    gate_act = gate * sig
    act_o[...] = (gate_act * up).astype(BF)
    grad = gact_v[...].astype(F32)
    gup_o[...] = (grad * gate_act).astype(BF)
    ggate_o[...] = (grad * up * sig * (1.0 + gate * (1.0 - sig))).astype(BF)

    sum2 = PairSum(p2, g2, gn2_o, (ps, pr), c, partner, NB2, NE + NC)
    sum2.run(lambda j: nn(ggate_o[...], wgt_v[:, cols(j, WB)]) + nn(gup_o[...], wut_v[:, cols(j, WB)]))

    for s in (sum0, sum1, sum2):
        s.drain()
    for j in range(NE):
        cross_copy(0, s0, r0, j).wait_send()
    for j in range(NC):
        cross_copy(1, s1, r1, j).wait_send()
    for copy in (to_cross, to_partner, share1, onward, share2):
        copy.wait_send()


def middle_kernel(gn2_own, gn2_got, part, h1, gfull, gain_m, qkv, cs, wqkv, wo, token,
                  gh1_o, gqkv_o, give_o, keep_o, gain_o,
                  gheads_v, probs_v, g0, s0, p1, g1, ps, pr, hs, hr):
    x, c, partner, cross = place()
    met = greet(partner)
    gains = []

    def first(b, r):
        grad = (gn2_own[b, r].astype(F32) + gn2_got[b, r].astype(F32)).astype(BF).astype(F32)
        back, part = norm_back(grad, h1[b, r].astype(F32), gain_m[...])
        gh1_o[b, c, r] = (gfull[b, c, r].astype(F32) + back).astype(BF)
        gains.append(part)
    rows16(first)
    met()
    share = remote(gh1_o.at[:, c], gh1_o.at[:, c], hs.at[0], hr.at[0], partner)
    share.start()
    gain_o[...] = gains[0] + gains[1] + gains[2] + gains[3]
    sum0 = PairSum(part, g0, s0, (ps, pr), c, partner, 1)
    sum0.copy(0).start()
    for g in range(KVLOC):
        probs_v[g] = probs_of(stack(qkv, g), qkv[:, QC + g * HD:QC + (g + 1) * HD])
    share.wait_recv()

    gh1 = gh1_o[...].reshape(SEQ, DIM)
    gheads_v[...] = nt(gh1, wo[...]).astype(BF)

    cos_tab, sin_tab = cs[0], -cs[1]
    turn_back = lambda pair: rope_pair(pair.astype(F32), cos_tab, sin_tab)
    gks, gvs = [], []
    for g in range(KVLOC):
        k = qkv[:, QC + g * HD:QC + (g + 1) * HD]
        v = qkv[:, QC + KC + g * HD:QC + KC + (g + 1) * HD]
        q, gh = stack(qkv, g), stack(gheads_v, g)
        probs = probs_v[g]
        gp = nt(gh, v).astype(BF).astype(F32)
        gvs.append(tn(probs.astype(BF), gh).astype(BF))
        gs = (probs * (gp - jnp.sum(gp * probs, axis=-1, keepdims=True)) * SCALE).astype(BF)
        gks.append(tn(gs, q).astype(BF).astype(F32))
        unstack(gqkv_o, g, nn(gs, k).astype(BF), turn_back)
    gqkv_o[:, QC:QC + KC] = rope_pair(jnp.concatenate(gks, axis=1), cos_tab, sin_tab).astype(BF)
    gqkv_o[:, QC + KC:] = jnp.concatenate(gvs, axis=1)

    sum1 = PairSum(p1, g1, give_o, (ps, pr), c, partner, NB2, 1)
    sum1.send_all(lambda j: nn(gqkv_o[...], wqkv[:, cols(j, WB)]))
    sum0.take(0)
    give_o[2] = s0[1 - x]
    keep_o[...] = s0[x]
    for j in range(NB2):
        sum1.take(j)
    sum0.drain()
    sum1.drain()
    share.wait_send()


def back_kernel(give, got, keep, h1, x0, gh1, gain_a, gain_mp, token, gx_o, gain_o, hid_o, gbuf, hs, hr):
    x, c, partner, cross = place()
    met = greet(partner)
    gains = []

    def first(b, r):
        grad = (give[b, r].astype(F32) + got[b, r].astype(F32)).astype(BF).astype(F32)
        back, part = norm_back(grad, x0[b, r].astype(F32), gain_a[...])
        gx_o[b, c, r] = (gh1[b, c, r].astype(F32) + back).astype(BF)
        gains.append(part)
    rows16(first)
    met()
    share = remote(gx_o.at[:, c], gx_o.at[:, c], hs.at[0], hr.at[0], partner)
    share.start()
    gbuf[c, 0:1] = gains[0] + gains[1] + gains[2] + gains[3]
    gbuf[c, 1:2] = gain_mp[...]
    share_gain = remote(gbuf.at[c], gbuf.at[c], hs.at[1], hr.at[1], partner)
    share_gain.start()
    hid_o[...] = (h1[x].astype(F32) + (keep[...].astype(F32) + got[2].astype(F32))).astype(BF)
    share_gain.wait_recv()
    gain_o[...] = gbuf[0, 0:2] + gbuf[1, 0:2]
    share.wait_recv()
    share.wait_send()
    share_gain.wait_send()


def vm(n):
    return [pl.BlockSpec(memory_space=VMEM)] * n


def hb(n):
    return [pl.BlockSpec(memory_space=HBM)] * n


def on(shape, dtype=BF):
    return pltpu.VMEM(shape, dtype)


NB = 5
BM = 256
UP_FIRST = 768
RAMP = ((0, 64), (64, 64), (128, 128))
EB = 256
ENB = 4


def outer_kernel(spec, n_in, n_held, side, *refs):
    n_out = 1 + max(o for _, _, _, o, _, _ in spec)
    ins, outs = refs[:n_in], refs[n_in + n_held:n_in + n_held + n_out]
    *part, token, buf, sem, ramp, ramp_sem = refs[n_in + n_held + n_out:]
    token[...] = jnp.zeros_like(token)
    done = 0
    flying = {}
    small = []
    for l, r, off, o, row, rows in spec:
        lhs, rhs, out = ins[l], ins[r], outs[o]
        if not small:
            for i, (lo, size) in enumerate(RAMP):
                ramp[lo:lo + size] = tn(lhs[:, off + lo:off + lo + size], rhs[...])
                small.append(pltpu.make_async_copy(
                    ramp.at[pl.ds(lo, size)], out.at[pl.ds(row + lo, size)], ramp_sem.at[i]))
                small[-1].start()
            off, row, rows = off + BM, row + BM, rows - BM
        bm = min(BM, rows)
        steps = rows // bm

        def copy(i, out=out, done=done, bm=bm, row=row):
            slot = lax.rem(i + done, NB)
            where = pl.ds(pl.multiple_of(row + i * bm, bm), bm)
            return pltpu.make_async_copy(buf.at[slot, pl.ds(0, bm)], out.at[where], sem.at[slot])

        def compute(i, lhs=lhs, rhs=rhs, off=off, done=done, bm=bm):
            a = lhs[:, pl.ds(pl.multiple_of(off + i * bm, 128), bm)]
            buf[lax.rem(i + done, NB), 0:bm] = tn(a, rhs[...])

        free = [(done + i) % NB for i in range(min(NB, steps))]
        uniform = steps >= NB and all(flying.get(k, bm) == bm for k in range(NB)) and (not flying or len(flying) == NB)
        if uniform:
            def step(i, carry, copy=copy, compute=compute, waiting=bool(flying)):
                if waiting:
                    copy(i).wait()
                else:
                    @pl.when(i >= NB)
                    def _():
                        copy(i).wait()
                compute(i)
                copy(i).start()
                return carry
            lax.fori_loop(0, steps, step, 0)
            flying = {k: bm for k in range(NB)}
        else:
            for i in range(steps):
                slot = (done + i) % NB
                if slot in flying:
                    size = flying[slot]
                    pltpu.make_async_copy(buf.at[slot, pl.ds(0, size)], outs[0].at[pl.ds(0, size)], sem.at[slot]).wait()
                compute(i)
                copy(i).start()
                flying[slot] = bm
        done += steps
        if side and done == steps:
            for j in range(NB2):
                lo, hi = j * WB, (j + 1) * WB
                out = nn(ins[side[0]][...], ins[side[1]][:, lo:hi])
                part[0][:, :, :, lo:hi] = out.astype(BF).reshape(2, 2, 32, WB)
    for copy in small:
        copy.wait()
    for slot, size in flying.items():
        pltpu.make_async_copy(buf.at[slot, pl.ds(0, size)], outs[0].at[pl.ds(0, size)], sem.at[slot]).wait()


def outer(ins, spec, rows, held=(), side=()):
    total = sum(n for *_, n in spec)
    extra = (on(FULL),) if side else ()
    return pl.pallas_call(
        functools.partial(outer_kernel, spec, len(ins), len(held), side),
        out_shape=tuple(jax.ShapeDtypeStruct((m, DIM), F32) for m in rows) + extra + (on((8, 128), F32),),
        in_specs=vm(len(ins)) + hb(len(held)),
        out_specs=tuple(hb(len(rows)) + vm(1 + len(extra))),
        scratch_shapes=[pltpu.VMEM((NB, BM, DIM), F32), dma(NB), pltpu.VMEM((BM, DIM), F32), dma(len(RAMP))],
        input_output_aliases={len(ins) + i: o for i, (_, o) in enumerate(held)},
        cost_estimate=pl.CostEstimate(flops=2 * total * DIM * SEQ, bytes_accessed=4 * total * DIM, transcendentals=0),
        compiler_params=pltpu.CompilerParams(vmem_limit_bytes=24 * 2 ** 20),
    )(*ins, *[h for h, _ in held])


def emb_kernel(tok, gx, gains, hid, out, ga_o, gm_o, hid_o, buf, sem, out_sem, ramp, ramp_sem):
    base = lax.axis_index("tp") * VLOC
    ids = jnp.broadcast_to(tok[...], (EB, SEQ)) - base
    row = lax.broadcasted_iota(jnp.int32, (EB, SEQ), 0)
    grad = gx[...].reshape(SEQ, DIM)

    small = []
    for i, (lo, size) in enumerate(RAMP):
        hot = jnp.where(ids[:size] == row[:size] + lo, 1.0, 0.0).astype(BF)
        ramp[lo:lo + size] = nn(hot, grad)
        small.append(pltpu.make_async_copy(ramp.at[pl.ds(lo, size)], out.at[pl.ds(lo, size)], ramp_sem.at[i]))
        small[-1].start()
    extra = (
        pltpu.make_async_copy(gains.at[pl.ds(0, 1)], ga_o, out_sem.at[0]),
        pltpu.make_async_copy(gains.at[pl.ds(1, 1)], gm_o, out_sem.at[1]),
        pltpu.make_async_copy(hid, hid_o, out_sem.at[2]),
    )
    for e in extra:
        e.start()

    def copy(i):
        slot = lax.rem(i - 1, ENB)
        return pltpu.make_async_copy(buf.at[slot], out.at[pl.ds(pl.multiple_of(i * EB, EB), EB)], sem.at[slot])

    def step(i, carry):
        @pl.when(i >= ENB + 1)
        def _():
            copy(i).wait()
        hot = jnp.where(ids == row + i * EB, 1.0, 0.0).astype(BF)
        buf[lax.rem(i - 1, ENB)] = nn(hot, grad)
        copy(i).start()
        return carry
    steps = VLOC // EB
    lax.fori_loop(1, steps, step, 0)
    for k in range(steps - ENB, steps):
        copy(k).wait()
    for e in (*small, *extra):
        e.wait()


def sds(shape, dtype=BF):
    return jax.ShapeDtypeStruct(shape, dtype)


FULL = (2, 2, 32, DIM)
MINE = (2, 32, DIM)


def device_fn(tokens, positions, emb, gain_a, gain_m, wq, wk, wv, wo, wg, wu, wd, gh):
    inv_freq = (ROPE_THETA ** (-np.arange(HD // 2, dtype=np.float32) * np.float32(2.0 / HD))).astype(np.float32)
    freq = jnp.asarray(np.tile(inv_freq, 4)[None, :])
    ga, gm = gain_a.reshape(1, DIM), gain_m.reshape(1, DIM)
    flat = lambda w: jnp.transpose(w, (1, 2, 0)).reshape(-1, DIM)
    wqt, wkt, wvt = flat(wq), flat(wk), flat(wv)
    wo2 = wo.reshape(QC, DIM)
    gh2 = gh.reshape(32, DIM)

    n1, x0, qkv, cs, heads, h1, n2, act, ggate, gup, gfull, gn2, wqkv_v, wo_v, wd_v = pl.pallas_call(
        front_kernel,
        out_shape=(on(FULL), on(MINE), on((SEQ, QKV)), on((2, SEQ, 128), F32), on((SEQ, QC)), on(MINE),
                   on(FULL), on((SEQ, FLOC)), on((SEQ, FLOC)), on((SEQ, FLOC)), on(FULL), on(MINE),
                   on((QKV, DIM)), on((QC, DIM)), on((FLOC, DIM))),
        in_specs=hb(14),
        out_specs=tuple(vm(15)),
        scratch_shapes=[
            pltpu.VMEM((1, SEQ), jnp.int32), pltpu.VMEM((1, SEQ), jnp.int32), pltpu.VMEM((1, SEQ), F32),
            pltpu.VMEM((1, DIM), F32), pltpu.VMEM((1, DIM), F32),
            pltpu.VMEM((VLOC, DIM), BF), pltpu.VMEM((DIM, FLOC), BF), pltpu.VMEM((DIM, FLOC), BF),
            pltpu.VMEM((FLOC, DIM), BF),
            pltpu.VMEM((SEQ, VLOC), BF), pltpu.VMEM((SEQ, FLOC), BF),
            pltpu.VMEM(FULL, BF), pltpu.VMEM(MINE, BF), pltpu.VMEM(MINE, BF), pltpu.VMEM(MINE, BF),
            pltpu.VMEM(FULL, BF), pltpu.VMEM(MINE, BF), pltpu.VMEM(MINE, BF), pltpu.VMEM(MINE, BF),
            pltpu.VMEM(FULL, BF), pltpu.VMEM(MINE, BF),
            dma(6), dma(NE), dma(7), dma(NE + NC + NB2), dma(NE + NC + NB2), dma(NE + NC), dma(NE + NC), dma(5), dma(5)],
        compiler_params=pltpu.CompilerParams(collective_id=0, has_side_effects=True, vmem_limit_bytes=44 * 2 ** 20),
    )(tokens, positions, freq, ga, gm, gh2, emb, wqt, wkt, wvt, wo2, wd, wg, wu)

    swap = [(i, i ^ 2) for i in range(4)]
    gn2_got = lax.ppermute(gn2, 'tp', swap)
    gfull2 = gfull.reshape(SEQ, DIM)
    n2f = n2.reshape(SEQ, DIM)
    g_gate, g_up, part, token = outer(
        (n2f, ggate, gup, act, wd_v), ((0, 1, 0, 0, 0, DIM), (0, 2, 0, 1, 0, UP_FIRST)), (DIM, DIM), side=(3, 4))

    gh1, gqkv, give, keep, gain_mp = pl.pallas_call(
        middle_kernel,
        out_shape=(on(FULL), on((SEQ, QKV)), on((3, 32, DIM)), on((32, DIM)), on((1, DIM), F32)),
        in_specs=vm(11),
        out_specs=tuple(vm(5)),
        scratch_shapes=[
            pltpu.VMEM((SEQ, QC), BF), pltpu.VMEM((KVLOC, GROUP * SEQ, SEQ), F32),
            pltpu.VMEM(MINE, BF), pltpu.VMEM(MINE, BF), pltpu.VMEM(FULL, BF), pltpu.VMEM(MINE, BF),
            dma(1 + NB2), dma(1 + NB2), dma(1), dma(1)],
        compiler_params=pltpu.CompilerParams(collective_id=1, has_side_effects=True, vmem_limit_bytes=8 * 2 ** 20),
    )(gn2, gn2_got, part, h1, gfull, gm, qkv, cs, wqkv_v, wo_v, token)

    got = lax.ppermute(give, 'tp', swap)
    g_up, g_down, g_out, g_q, g_k, g_v, token2 = outer(
        (n2f, gup, act, gfull2, heads, gh1.reshape(SEQ, DIM), gqkv, n1.reshape(SEQ, DIM)),
        ((0, 1, UP_FIRST, 0, UP_FIRST, DIM - UP_FIRST), (2, 3, 0, 1, 0, FLOC), (4, 5, 0, 2, 0, QC),
         (6, 7, 0, 3, 0, QC), (6, 7, QC, 4, 0, KC), (6, 7, QC + KC, 5, 0, KC)),
        (DIM, FLOC, QC, QC, KC, KC), ((g_up, 0),))

    gx, gains, hid = pl.pallas_call(
        back_kernel,
        out_shape=(on(FULL), on((2, DIM), F32), on((32, DIM))),
        in_specs=vm(9),
        out_specs=tuple(vm(3)),
        scratch_shapes=[pltpu.VMEM((2, 8, DIM), F32), dma(2), dma(2)],
        compiler_params=pltpu.CompilerParams(collective_id=2, has_side_effects=True, vmem_limit_bytes=8 * 2 ** 20),
    )(give, got, keep, h1, x0, gh1, ga, gain_mp, token2)

    g_emb, gain_1, gain_2, hidden = pl.pallas_call(
        emb_kernel,
        out_shape=(sds((VLOC, DIM), F32), sds((1, DIM), F32), sds((1, DIM), F32), sds((32, DIM))),
        in_specs=vm(4),
        out_specs=tuple(hb(4)),
        scratch_shapes=[pltpu.VMEM((ENB, EB, DIM), F32), dma(ENB), dma(3), pltpu.VMEM((EB, DIM), F32), dma(len(RAMP))],
        compiler_params=pltpu.CompilerParams(vmem_limit_bytes=24 * 2 ** 20),
    )(tokens, gx, gains, hid)

    back3 = lambda g: jnp.transpose(g.reshape(-1, HD, DIM), (2, 0, 1))
    return (hidden.reshape(1, 32, DIM), g_emb, back3(g_q), back3(g_k), back3(g_v), g_out.reshape(HLOC, HD, DIM),
            g_gate, g_up, g_down, gain_1.reshape(DIM), gain_2.reshape(DIM))


def solution(mesh):
    in_specs = (P('dp', None), P('dp', None), P('tp', None), P(None), P(None),
                P(None, 'tp', None), P(None, 'tp', None), P(None, 'tp', None), P('tp', None, None),
                P(None, 'tp'), P(None, 'tp'), P('tp', None), P('dp', 'tp', None))
    out_specs = (P('dp', 'tp', None), P(('dp', 'tp'), None),
                 P('dp', 'tp', None), P('dp', 'tp', None), P('dp', 'tp', None), P(('dp', 'tp'), None, None),
                 P('dp', 'tp'), P('dp', 'tp'), P(('dp', 'tp'), None), P('dp'), P('dp'))
    return jax.shard_map(device_fn, mesh=mesh, in_specs=in_specs, out_specs=out_specs, check_vma=False)
```

```python
import functools

import jax
import jax.numpy as jnp
import numpy as np
from jax import lax
from jax.experimental import pallas as pl
from jax.experimental.pallas import tpu as pltpu
from jax.sharding import PartitionSpec as P

ROPE_THETA = 1000000.0
RMS_EPS = 1e-5
MESH = pl.DeviceIdType.MESH
BF = jnp.bfloat16
F32 = jnp.float32

SEQ = 128
DIM = 2048
VLOC = 2048
FLOC = 2048
HLOC = 8
KVLOC = 2
HD = 64
QC = HLOC * HD
KC = KVLOC * HD
QKV = QC + 2 * KC
GROUP = HLOC // KVLOC
SCALE = HD ** -0.5
NC = 4
W = DIM // NC
NE = 8
WE = DIM // NE
AHEAD = 4
NB2 = 2
WB = DIM // NB2
LAG = 1
VMEM = pltpu.VMEM
HBM = pltpu.HBM


def nn(a, b):
    return lax.dot_general(a, b, (((1,), (0,)), ((), ())), preferred_element_type=F32)


def nt(a, b):
    return lax.dot_general(a, b, (((1,), (1,)), ((), ())), preferred_element_type=F32)


def tn(a, b):
    return lax.dot_general(a, b, (((0,), (0,)), ((), ())), preferred_element_type=F32)


def place():
    tp = lax.axis_index("tp")
    x = tp // 2
    c = tp - 2 * x
    return x, c, 2 * x + (1 - c), 2 * (1 - x) + c


def greet(*peers):
    sem = pltpu.get_barrier_semaphore()
    for peer in peers:
        pl.semaphore_signal(sem, inc=1, device_id={"tp": peer}, device_id_type=MESH)
    return lambda: pl.semaphore_wait(sem, len(peers))


def remote(src, dst, send, recv, peer):
    return pltpu.make_async_remote_copy(
        src_ref=src, dst_ref=dst, send_sem=send, recv_sem=recv, device_id={"tp": peer}, device_id_type=MESH)


def cols(j, width=W):
    return pl.ds(pl.multiple_of(j * width, width), width)


def dma(*shape):
    return pltpu.SemaphoreType.DMA(shape)


class PairSum:
    def __init__(self, part, got, own, sems, c, partner, n=NC, base=0):
        self.part, self.got, self.own, self.c, self.partner = part, got, own, c, partner
        self.send, self.recv = sems
        self.n, self.width, self.base = n, DIM // n, base

    def copy(self, j):
        return remote(self.part.at[:, 1 - self.c, :, cols(j, self.width)], self.got.at[:, :, cols(j, self.width)],
                      self.send.at[self.base + j], self.recv.at[self.base + j], self.partner)

    def put(self, j, value):
        self.part[:, :, :, cols(j, self.width)] = value.astype(BF).reshape(2, 2, 32, self.width)
        self.copy(j).start()

    def take(self, j):
        self.copy(j).wait_recv()
        total = self.part[:, self.c, :, cols(j, self.width)].astype(F32) + self.got[:, :, cols(j, self.width)].astype(F32)
        self.own[0:2, :, cols(j, self.width)] = total.astype(BF)

    def send_all(self, chunk):
        def body(j, carry):
            self.put(j, chunk(j))
            return carry
        lax.fori_loop(0, self.n, body, 0)

    def run(self, chunk, then=lambda j: None, lag=None):
        lag = lag or self.n

        def finish(j):
            self.take(j)
            then(j)

        def body(j, carry):
            self.put(j, chunk(j))
            if lag < self.n:
                @pl.when(j >= lag)
                def _():
                    finish(j - lag)
            return carry
        lax.fori_loop(0, self.n, body, 0)
        for j in range(self.n - lag, self.n):
            finish(j)

    def drain(self):
        for j in range(self.n):
            self.copy(j).wait_send()


def rows16(fn):
    for b in range(2):
        for r in range(0, 32, 16):
            fn(b, slice(r, r + 16))


def norm_rows(x, gain):
    inv = lax.rsqrt(jnp.mean(x * x, axis=-1, keepdims=True) + RMS_EPS)
    return (x * inv * gain).astype(BF)


def norm_back(grad, x, gain):
    inv = lax.rsqrt(jnp.mean(x * x, axis=-1, keepdims=True) + RMS_EPS)
    normed = x * inv
    scaled = grad * gain
    back = inv * (scaled - normed * jnp.mean(scaled * normed, axis=-1, keepdims=True))
    return back, jnp.sum(grad * normed, axis=0, keepdims=True)


def spread(row):
    return jnp.transpose(jnp.broadcast_to(row, (SEQ, SEQ)))


def rope_pair(values, cos_tab, sin_tab):
    lane = lax.broadcasted_iota(jnp.int32, (SEQ, 128), 1)
    low = (lane % HD) < HD // 2
    other = jnp.where(low, pltpu.roll(values, 128 - HD // 2, 1), pltpu.roll(values, HD // 2, 1))
    return values * cos_tab + other * jnp.where(low, -sin_tab, sin_tab)


def stack(ref, g):
    return jnp.concatenate([ref[:, h * HD:(h + 1) * HD] for h in range(g * GROUP, (g + 1) * GROUP)], axis=0)


def unstack(ref, g, value, fix=lambda pair: pair):
    for i in range(0, GROUP, 2):
        lo = (g * GROUP + i) * HD
        pair = jnp.concatenate([value[i * SEQ:(i + 1) * SEQ], value[(i + 1) * SEQ:(i + 2) * SEQ]], axis=1)
        ref[:, lo:lo + 128] = fix(pair).astype(BF)


def probs_of(q, k):
    scores = nt(q, k) * SCALE
    shape = (GROUP * SEQ, SEQ)
    row = lax.broadcasted_iota(jnp.int32, shape, 0) % SEQ
    scores = jnp.where(row >= lax.broadcasted_iota(jnp.int32, shape, 1), scores, -1e30)
    e = jnp.exp(scores - jnp.max(scores, axis=-1, keepdims=True))
    return e / jnp.sum(e, axis=-1, keepdims=True)


def front_kernel(tok, pos, freq, gain_a, gain_m, gh, emb, wq, wk, wv, wo, wd, wg, wu,
                 n1_o, x0_o, qkv_o, cs_o, heads_o, h1_o, n2_o, act_o, ggate_o, gup_o, gfull_o, gn2_o,
                 wqkv_v, wo_v, wd_v,
                 tok_v, pos_v, freq_v, ga_v, gm_v, emb_v, wg_v, wu_v, wut_v, hot_v, gact_v,
                 p0, g0, s0, r0, p1, g1, s1, r1, p2, g2,
                 in_sem, emb_sem, w_sem, ps, pr, xs, xr, hs, hr):
    x, c, partner, cross = place()
    tp = 2 * x + c

    def fetch_emb(j):
        return pltpu.make_async_copy(emb.at[:, cols(j, WE)], emb_v.at[:, cols(j, WE)], emb_sem.at[j])

    get_q = pltpu.make_async_copy(wq, wqkv_v.at[pl.ds(0, QC)], w_sem.at[0])
    get_k = pltpu.make_async_copy(wk, wqkv_v.at[pl.ds(QC, KC)], w_sem.at[1])
    get_v = pltpu.make_async_copy(wv, wqkv_v.at[pl.ds(QC + KC, KC)], w_sem.at[2])
    get_out = pltpu.make_async_copy(wo, wo_v, emb_sem.at[0])
    get_down = pltpu.make_async_copy(wd, wd_v, emb_sem.at[1])
    get_gate = pltpu.make_async_copy(wg, wg_v, emb_sem.at[2])
    get_up = pltpu.make_async_copy(wu, wu_v, emb_sem.at[3])
    get_small = [pltpu.make_async_copy(src, dst, in_sem.at[i]) for i, (src, dst) in enumerate(
        ((tok, tok_v), (pos, pos_v), (freq, freq_v), (gain_a, ga_v), (gain_m, gm_v), (gh, gfull_o.at[x, c])))]
    get_small[0].start()
    for j in range(AHEAD):
        fetch_emb(j).start()
    for g in get_small[1:]:
        g.start()
    met = greet(partner, cross)
    get_small[0].wait()
    ids = spread(tok_v[...].astype(F32))
    base = (tp * VLOC).astype(F32)
    lane = lax.broadcasted_iota(jnp.int32, (SEQ, 128), 1).astype(F32)
    for v in range(VLOC // 128):
        hot_v[:, v * 128:(v + 1) * 128] = jnp.where(ids == lane + (base + float(v * 128)), 1.0, 0.0).astype(BF)

    met()

    def cross_copy(k, src, dst, j):
        cj = cols(j, WE if k == 0 else W)
        return remote(src.at[:, :, cj], dst.at[:, :, cj], xs.at[k * NE + j], xr.at[k * NE + j], cross)

    sum0 = PairSum(p0, g0, s0, (ps, pr), c, partner, NE)

    def lookup(j):
        fetch_emb(j).wait()

        @pl.when(j + AHEAD < NE)
        def _():
            fetch_emb(j + AHEAD).start()

        @pl.when(j == NE - AHEAD)
        def _():
            for g in (get_q, get_k, get_v):
                g.start()
        return nn(hot_v[...], emb_v[:, cols(j, WE)])

    sum0.run(lookup, lambda j: cross_copy(0, s0, r0, j).start(), LAG)
    for g in (get_out, get_up, get_down, get_gate):
        g.start()
    for g in get_small[1:]:
        g.wait()
    mine = gfull_o.at[x, c]
    to_cross = remote(mine, mine, hs.at[0], hr.at[0], cross)
    to_partner = remote(mine, mine, hs.at[1], hr.at[1], partner)
    to_partner.start()
    angle = spread(pos_v[...].astype(F32)) * freq_v[...]
    cs_o[0] = jnp.cos(angle)
    cs_o[1] = jnp.sin(angle)

    wqkvt_v = wut_v
    for g in (get_q, get_k, get_v):
        g.wait()

    def turn_qkv(j, carry):
        rj = pl.ds(pl.multiple_of(j * 256, 256), 256)
        wqkvt_v[:, rj] = jnp.transpose(wqkv_v[rj, :])
        return carry
    lax.fori_loop(0, QKV // 256, turn_qkv, 0)

    for j in range(NE):
        cross_copy(0, s0, r0, j).wait_recv()

    to_cross.start()

    def first(b, r):
        xv = s0[b, r].astype(F32) + r0[b, r].astype(F32)
        x0_o[b, r] = xv.astype(BF)
        n1_o[b, c, r] = norm_rows(xv, ga_v[...])
    rows16(first)
    share1 = remote(n1_o.at[:, c], n1_o.at[:, c], hs.at[2], hr.at[2], partner)
    share1.start()
    share1.wait_recv()

    n1 = n1_o[...].reshape(SEQ, DIM)
    cos_tab, sin_tab = cs_o[0], cs_o[1]

    lin = nn(n1, wqkvt_v[:, 0:QKV])
    for lo in range(0, QKV, 128):
        piece = lin[:, lo:lo + 128]
        if lo < QC + KC:
            piece = rope_pair(piece, cos_tab, sin_tab)
        qkv_o[:, lo:lo + 128] = piece.astype(BF)
    for g in range(KVLOC):
        k = qkv_o[:, QC + g * HD:QC + (g + 1) * HD]
        v = qkv_o[:, QC + KC + g * HD:QC + KC + (g + 1) * HD]
        unstack(heads_o, g, nn(probs_of(stack(qkv_o, g), k).astype(BF), v).astype(BF))
    get_out.wait()

    sum0.drain()
    sum1 = PairSum(p1, g1, s1, (ps, pr), c, partner)
    sum1.run(lambda j: nn(heads_o[...], wo_v[:, cols(j)]), lambda j: cross_copy(1, s1, r1, j).start())

    to_cross.wait_recv()
    onward = remote(gfull_o.at[1 - x, c], gfull_o.at[1 - x, c], hs.at[3], hr.at[3], partner)
    onward.start()
    get_up.wait()

    def turn_up(j, carry):
        wut_v[:, cols(j, WB)] = jnp.transpose(wu_v[cols(j, WB), :])
        return carry
    lax.fori_loop(0, NB2, turn_up, 0)

    to_partner.wait_recv()
    onward.wait_recv()
    get_down.wait()
    get_gate.wait()
    gfull = gfull_o[...].reshape(SEQ, DIM)
    wgt_v = emb_v

    def grad_act(j, carry):
        gact_v[:, cols(j, WB)] = nt(gfull, wd_v[cols(j, WB), :]).astype(BF)
        wgt_v[:, cols(j, WB)] = jnp.transpose(wg_v[cols(j, WB), :])
        return carry
    lax.fori_loop(0, NB2, grad_act, 0)

    for j in range(NC):
        cross_copy(1, s1, r1, j).wait_recv()

    def second(b, r):
        total = s1[b, r].astype(F32) + r1[b, r].astype(F32)
        h1 = (x0_o[b, r].astype(F32) + total).astype(BF)
        h1_o[b, r] = h1
        n2_o[b, c, r] = norm_rows(h1.astype(F32), gm_v[...])
    rows16(second)
    share2 = remote(n2_o.at[:, c], n2_o.at[:, c], hs.at[4], hr.at[4], partner)
    share2.start()
    share2.wait_recv()
    n2 = n2_o[...].reshape(SEQ, DIM)

    gate = nn(n2, wg_v[...])
    up = nn(n2, wu_v[...])
    sig = jax.nn.sigmoid(gate)
    gate_act = gate * sig
    act_o[...] = (gate_act * up).astype(BF)
    grad = gact_v[...].astype(F32)
    gup_o[...] = (grad * gate_act).astype(BF)
    ggate_o[...] = (grad * up * sig * (1.0 + gate * (1.0 - sig))).astype(BF)

    sum1.drain()
    sum2 = PairSum(p2, g2, gn2_o, (ps, pr), c, partner, NB2)
    sum2.run(lambda j: nn(ggate_o[...], wgt_v[:, cols(j, WB)]) + nn(gup_o[...], wut_v[:, cols(j, WB)]))

    sum2.drain()
    for j in range(NE):
        cross_copy(0, s0, r0, j).wait_send()
    for j in range(NC):
        cross_copy(1, s1, r1, j).wait_send()
    for copy in (to_cross, to_partner, share1, onward, share2):
        copy.wait_send()


def middle_kernel(gn2_own, gn2_got, part, h1, gfull, gain_m, qkv, cs, wqkv, wo, token,
                  gh1_o, gqkv_o, give_o, keep_o, gain_o,
                  gheads_v, probs_v, g0, s0, p1, g1, ps, pr, hs, hr):
    x, c, partner, cross = place()
    met = greet(partner)
    gains = []

    def first(b, r):
        grad = (gn2_own[b, r].astype(F32) + gn2_got[b, r].astype(F32)).astype(BF).astype(F32)
        back, part = norm_back(grad, h1[b, r].astype(F32), gain_m[...])
        gh1_o[b, c, r] = (gfull[b, c, r].astype(F32) + back).astype(BF)
        gains.append(part)
    rows16(first)
    met()
    share = remote(gh1_o.at[:, c], gh1_o.at[:, c], hs.at[0], hr.at[0], partner)
    share.start()
    gain_o[...] = gains[0] + gains[1] + gains[2] + gains[3]
    sum0 = PairSum(part, g0, s0, (ps, pr), c, partner, 1)
    sum0.copy(0).start()
    for g in range(KVLOC):
        probs_v[g] = probs_of(stack(qkv, g), qkv[:, QC + g * HD:QC + (g + 1) * HD])
    share.wait_recv()

    gh1 = gh1_o[...].reshape(SEQ, DIM)
    gheads_v[...] = nt(gh1, wo[...]).astype(BF)

    cos_tab, sin_tab = cs[0], -cs[1]
    turn_back = lambda pair: rope_pair(pair.astype(F32), cos_tab, sin_tab)
    gks, gvs = [], []
    for g in range(KVLOC):
        k = qkv[:, QC + g * HD:QC + (g + 1) * HD]
        v = qkv[:, QC + KC + g * HD:QC + KC + (g + 1) * HD]
        q, gh = stack(qkv, g), stack(gheads_v, g)
        probs = probs_v[g]
        gp = nt(gh, v).astype(BF).astype(F32)
        gvs.append(tn(probs.astype(BF), gh).astype(BF))
        gs = (probs * (gp - jnp.sum(gp * probs, axis=-1, keepdims=True)) * SCALE).astype(BF)
        gks.append(tn(gs, q).astype(BF).astype(F32))
        unstack(gqkv_o, g, nn(gs, k).astype(BF), turn_back)
    gqkv_o[:, QC:QC + KC] = rope_pair(jnp.concatenate(gks, axis=1), cos_tab, sin_tab).astype(BF)
    gqkv_o[:, QC + KC:] = jnp.concatenate(gvs, axis=1)

    sum1 = PairSum(p1, g1, give_o, (ps, pr), c, partner, NB2, 1)
    sum1.send_all(lambda j: nn(gqkv_o[...], wqkv[:, cols(j, WB)]))
    sum0.take(0)
    give_o[2] = s0[1 - x]
    keep_o[...] = s0[x]
    for j in range(NB2):
        sum1.take(j)
    sum0.drain()
    sum1.drain()
    share.wait_send()


def back_kernel(give, got, keep, h1, x0, gh1, gain_a, gain_mp, token, gx_o, gain_o, hid_o, gbuf, hs, hr):
    x, c, partner, cross = place()
    met = greet(partner)
    gains = []

    def first(b, r):
        grad = (give[b, r].astype(F32) + got[b, r].astype(F32)).astype(BF).astype(F32)
        back, part = norm_back(grad, x0[b, r].astype(F32), gain_a[...])
        gx_o[b, c, r] = (gh1[b, c, r].astype(F32) + back).astype(BF)
        gains.append(part)
    rows16(first)
    met()
    share = remote(gx_o.at[:, c], gx_o.at[:, c], hs.at[0], hr.at[0], partner)
    share.start()
    gbuf[c, 0:1] = gains[0] + gains[1] + gains[2] + gains[3]
    gbuf[c, 1:2] = gain_mp[...]
    share_gain = remote(gbuf.at[c], gbuf.at[c], hs.at[1], hr.at[1], partner)
    share_gain.start()
    hid_o[...] = (h1[x].astype(F32) + (keep[...].astype(F32) + got[2].astype(F32))).astype(BF)
    share_gain.wait_recv()
    gain_o[...] = gbuf[0, 0:2] + gbuf[1, 0:2]
    share.wait_recv()
    share.wait_send()
    share_gain.wait_send()


def vm(n):
    return [pl.BlockSpec(memory_space=VMEM)] * n


def hb(n):
    return [pl.BlockSpec(memory_space=HBM)] * n


def on(shape, dtype=BF):
    return pltpu.VMEM(shape, dtype)


NB = 5
BM = 256
UP_FIRST = 768
RAMP = ((0, 64), (64, 64), (128, 128))
EB = 256
ENB = 4


def outer_kernel(spec, n_in, n_held, side, *refs):
    n_out = 1 + max(o for _, _, _, o, _, _ in spec)
    ins, outs = refs[:n_in], refs[n_in + n_held:n_in + n_held + n_out]
    *part, token, buf, sem, ramp, ramp_sem = refs[n_in + n_held + n_out:]
    token[...] = jnp.zeros_like(token)
    done = 0
    flying = {}
    small = []
    for l, r, off, o, row, rows in spec:
        lhs, rhs, out = ins[l], ins[r], outs[o]
        if not small:
            for i, (lo, size) in enumerate(RAMP):
                ramp[lo:lo + size] = tn(lhs[:, off + lo:off + lo + size], rhs[...])
                small.append(pltpu.make_async_copy(
                    ramp.at[pl.ds(lo, size)], out.at[pl.ds(row + lo, size)], ramp_sem.at[i]))
                small[-1].start()
            off, row, rows = off + BM, row + BM, rows - BM
        bm = min(BM, rows)
        steps = rows // bm

        def copy(i, out=out, done=done, bm=bm, row=row):
            slot = lax.rem(i + done, NB)
            where = pl.ds(pl.multiple_of(row + i * bm, bm), bm)
            return pltpu.make_async_copy(buf.at[slot, pl.ds(0, bm)], out.at[where], sem.at[slot])

        def compute(i, lhs=lhs, rhs=rhs, off=off, done=done, bm=bm):
            a = lhs[:, pl.ds(pl.multiple_of(off + i * bm, 128), bm)]
            buf[lax.rem(i + done, NB), 0:bm] = tn(a, rhs[...])

        free = [(done + i) % NB for i in range(min(NB, steps))]
        uniform = steps >= NB and all(flying.get(k, bm) == bm for k in range(NB)) and (not flying or len(flying) == NB)
        if uniform:
            def step(i, carry, copy=copy, compute=compute, waiting=bool(flying)):
                if waiting:
                    copy(i).wait()
                else:
                    @pl.when(i >= NB)
                    def _():
                        copy(i).wait()
                compute(i)
                copy(i).start()
                return carry
            lax.fori_loop(0, steps, step, 0)
            flying = {k: bm for k in range(NB)}
        else:
            for i in range(steps):
                slot = (done + i) % NB
                if slot in flying:
                    size = flying[slot]
                    pltpu.make_async_copy(buf.at[slot, pl.ds(0, size)], outs[0].at[pl.ds(0, size)], sem.at[slot]).wait()
                compute(i)
                copy(i).start()
                flying[slot] = bm
        done += steps
        if side and done == steps:
            for j in range(NB2):
                lo, hi = j * WB, (j + 1) * WB
                out = nn(ins[side[0]][...], ins[side[1]][:, lo:hi])
                part[0][:, :, :, lo:hi] = out.astype(BF).reshape(2, 2, 32, WB)
    for copy in small:
        copy.wait()
    for slot, size in flying.items():
        pltpu.make_async_copy(buf.at[slot, pl.ds(0, size)], outs[0].at[pl.ds(0, size)], sem.at[slot]).wait()


def outer(ins, spec, rows, held=(), side=()):
    total = sum(n for *_, n in spec)
    extra = (on(FULL),) if side else ()
    return pl.pallas_call(
        functools.partial(outer_kernel, spec, len(ins), len(held), side),
        out_shape=tuple(jax.ShapeDtypeStruct((m, DIM), F32) for m in rows) + extra + (on((8, 128), F32),),
        in_specs=vm(len(ins)) + hb(len(held)),
        out_specs=tuple(hb(len(rows)) + vm(1 + len(extra))),
        scratch_shapes=[pltpu.VMEM((NB, BM, DIM), F32), dma(NB), pltpu.VMEM((BM, DIM), F32), dma(len(RAMP))],
        input_output_aliases={len(ins) + i: o for i, (_, o) in enumerate(held)},
        cost_estimate=pl.CostEstimate(flops=2 * total * DIM * SEQ, bytes_accessed=4 * total * DIM, transcendentals=0),
        compiler_params=pltpu.CompilerParams(vmem_limit_bytes=24 * 2 ** 20),
    )(*ins, *[h for h, _ in held])


def emb_kernel(tok, gx, gains, hid, out, ga_o, gm_o, hid_o, buf, sem, out_sem, ramp, ramp_sem):
    base = lax.axis_index("tp") * VLOC
    ids = jnp.broadcast_to(tok[...], (EB, SEQ)) - base
    row = lax.broadcasted_iota(jnp.int32, (EB, SEQ), 0)
    grad = gx[...].reshape(SEQ, DIM)

    small = []
    for i, (lo, size) in enumerate(RAMP):
        hot = jnp.where(ids[:size] == row[:size] + lo, 1.0, 0.0).astype(BF)
        ramp[lo:lo + size] = nn(hot, grad)
        small.append(pltpu.make_async_copy(ramp.at[pl.ds(lo, size)], out.at[pl.ds(lo, size)], ramp_sem.at[i]))
        small[-1].start()
    extra = (
        pltpu.make_async_copy(gains.at[pl.ds(0, 1)], ga_o, out_sem.at[0]),
        pltpu.make_async_copy(gains.at[pl.ds(1, 1)], gm_o, out_sem.at[1]),
        pltpu.make_async_copy(hid, hid_o, out_sem.at[2]),
    )
    for e in extra:
        e.start()

    def copy(i):
        slot = lax.rem(i - 1, ENB)
        return pltpu.make_async_copy(buf.at[slot], out.at[pl.ds(pl.multiple_of(i * EB, EB), EB)], sem.at[slot])

    def step(i, carry):
        @pl.when(i >= ENB + 1)
        def _():
            copy(i).wait()
        hot = jnp.where(ids == row + i * EB, 1.0, 0.0).astype(BF)
        buf[lax.rem(i - 1, ENB)] = nn(hot, grad)
        copy(i).start()
        return carry
    steps = VLOC // EB
    lax.fori_loop(1, steps, step, 0)
    for k in range(steps - ENB, steps):
        copy(k).wait()
    for e in (*small, *extra):
        e.wait()


def sds(shape, dtype=BF):
    return jax.ShapeDtypeStruct(shape, dtype)


FULL = (2, 2, 32, DIM)
MINE = (2, 32, DIM)


def device_fn(tokens, positions, emb, gain_a, gain_m, wq, wk, wv, wo, wg, wu, wd, gh):
    inv_freq = (ROPE_THETA ** (-np.arange(HD // 2, dtype=np.float32) * np.float32(2.0 / HD))).astype(np.float32)
    freq = jnp.asarray(np.tile(inv_freq, 4)[None, :])
    ga, gm = gain_a.reshape(1, DIM), gain_m.reshape(1, DIM)
    flat = lambda w: jnp.transpose(w, (1, 2, 0)).reshape(-1, DIM)
    wqt, wkt, wvt = flat(wq), flat(wk), flat(wv)
    wo2 = wo.reshape(QC, DIM)
    gh2 = gh.reshape(32, DIM)

    n1, x0, qkv, cs, heads, h1, n2, act, ggate, gup, gfull, gn2, wqkv_v, wo_v, wd_v = pl.pallas_call(
        front_kernel,
        out_shape=(on(FULL), on(MINE), on((SEQ, QKV)), on((2, SEQ, 128), F32), on((SEQ, QC)), on(MINE),
                   on(FULL), on((SEQ, FLOC)), on((SEQ, FLOC)), on((SEQ, FLOC)), on(FULL), on(MINE),
                   on((QKV, DIM)), on((QC, DIM)), on((FLOC, DIM))),
        in_specs=hb(14),
        out_specs=tuple(vm(15)),
        scratch_shapes=[
            pltpu.VMEM((1, SEQ), jnp.int32), pltpu.VMEM((1, SEQ), jnp.int32), pltpu.VMEM((1, SEQ), F32),
            pltpu.VMEM((1, DIM), F32), pltpu.VMEM((1, DIM), F32),
            pltpu.VMEM((VLOC, DIM), BF), pltpu.VMEM((DIM, FLOC), BF), pltpu.VMEM((DIM, FLOC), BF),
            pltpu.VMEM((FLOC, DIM), BF),
            pltpu.VMEM((SEQ, VLOC), BF), pltpu.VMEM((SEQ, FLOC), BF),
            pltpu.VMEM(FULL, BF), pltpu.VMEM(MINE, BF), pltpu.VMEM(MINE, BF), pltpu.VMEM(MINE, BF),
            pltpu.VMEM(FULL, BF), pltpu.VMEM(MINE, BF), pltpu.VMEM(MINE, BF), pltpu.VMEM(MINE, BF),
            pltpu.VMEM(FULL, BF), pltpu.VMEM(MINE, BF),
            dma(6), dma(NE), dma(3), dma(NE), dma(NE), dma(NE + NC), dma(NE + NC), dma(5), dma(5)],
        compiler_params=pltpu.CompilerParams(collective_id=0, has_side_effects=True, vmem_limit_bytes=44 * 2 ** 20),
    )(tokens, positions, freq, ga, gm, gh2, emb, wqt, wkt, wvt, wo2, wd, wg, wu)

    swap = [(i, i ^ 2) for i in range(4)]
    gn2_got = lax.ppermute(gn2, 'tp', swap)
    gfull2 = gfull.reshape(SEQ, DIM)
    n2f = n2.reshape(SEQ, DIM)
    g_gate, g_up, part, token = outer(
        (n2f, ggate, gup, act, wd_v), ((0, 1, 0, 0, 0, DIM), (0, 2, 0, 1, 0, UP_FIRST)), (DIM, DIM), side=(3, 4))

    gh1, gqkv, give, keep, gain_mp = pl.pallas_call(
        middle_kernel,
        out_shape=(on(FULL), on((SEQ, QKV)), on((3, 32, DIM)), on((32, DIM)), on((1, DIM), F32)),
        in_specs=vm(11),
        out_specs=tuple(vm(5)),
        scratch_shapes=[
            pltpu.VMEM((SEQ, QC), BF), pltpu.VMEM((KVLOC, GROUP * SEQ, SEQ), F32),
            pltpu.VMEM(MINE, BF), pltpu.VMEM(MINE, BF), pltpu.VMEM(FULL, BF), pltpu.VMEM(MINE, BF),
            dma(1 + NB2), dma(1 + NB2), dma(1), dma(1)],
        compiler_params=pltpu.CompilerParams(collective_id=1, has_side_effects=True, vmem_limit_bytes=8 * 2 ** 20),
    )(gn2, gn2_got, part, h1, gfull, gm, qkv, cs, wqkv_v, wo_v, token)

    got = lax.ppermute(give, 'tp', swap)
    g_up, g_down, g_out, g_q, g_k, g_v, token2 = outer(
        (n2f, gup, act, gfull2, heads, gh1.reshape(SEQ, DIM), gqkv, n1.reshape(SEQ, DIM)),
        ((0, 1, UP_FIRST, 0, UP_FIRST, DIM - UP_FIRST), (2, 3, 0, 1, 0, FLOC), (4, 5, 0, 2, 0, QC),
         (6, 7, 0, 3, 0, QC), (6, 7, QC, 4, 0, KC), (6, 7, QC + KC, 5, 0, KC)),
        (DIM, FLOC, QC, QC, KC, KC), ((g_up, 0),))

    gx, gains, hid = pl.pallas_call(
        back_kernel,
        out_shape=(on(FULL), on((2, DIM), F32), on((32, DIM))),
        in_specs=vm(9),
        out_specs=tuple(vm(3)),
        scratch_shapes=[pltpu.VMEM((2, 8, DIM), F32), dma(2), dma(2)],
        compiler_params=pltpu.CompilerParams(collective_id=2, has_side_effects=True, vmem_limit_bytes=8 * 2 ** 20),
    )(give, got, keep, h1, x0, gh1, ga, gain_mp, token2)

    g_emb, gain_1, gain_2, hidden = pl.pallas_call(
        emb_kernel,
        out_shape=(sds((VLOC, DIM), F32), sds((1, DIM), F32), sds((1, DIM), F32), sds((32, DIM))),
        in_specs=vm(4),
        out_specs=tuple(hb(4)),
        scratch_shapes=[pltpu.VMEM((ENB, EB, DIM), F32), dma(ENB), dma(3), pltpu.VMEM((EB, DIM), F32), dma(len(RAMP))],
        compiler_params=pltpu.CompilerParams(vmem_limit_bytes=24 * 2 ** 20),
    )(tokens, gx, gains, hid)

    back3 = lambda g: jnp.transpose(g.reshape(-1, HD, DIM), (2, 0, 1))
    return (hidden.reshape(1, 32, DIM), g_emb, back3(g_q), back3(g_k), back3(g_v), g_out.reshape(HLOC, HD, DIM),
            g_gate, g_up, g_down, gain_1.reshape(DIM), gain_2.reshape(DIM))


def solution(mesh):
    in_specs = (P('dp', None), P('dp', None), P('tp', None), P(None), P(None),
                P(None, 'tp', None), P(None, 'tp', None), P(None, 'tp', None), P('tp', None, None),
                P(None, 'tp'), P(None, 'tp'), P('tp', None), P('dp', 'tp', None))
    out_specs = (P('dp', 'tp', None), P(('dp', 'tp'), None),
                 P('dp', 'tp', None), P('dp', 'tp', None), P('dp', 'tp', None), P(('dp', 'tp'), None, None),
                 P('dp', 'tp'), P('dp', 'tp'), P(('dp', 'tp'), None), P('dp'), P('dp'))
    return jax.shard_map(device_fn, mesh=mesh, in_specs=in_specs, out_specs=out_specs, check_vma=False)
```

```python
import functools

import jax
import jax.numpy as jnp
import numpy as np
from jax import lax
from jax.experimental import pallas as pl
from jax.experimental.pallas import tpu as pltpu
from jax.sharding import PartitionSpec as P

ROPE_THETA = 1000000.0
RMS_EPS = 1e-5
MESH = pl.DeviceIdType.MESH
BF = jnp.bfloat16
F32 = jnp.float32

SEQ = 128
DIM = 2048
VLOC = 2048
FLOC = 2048
HLOC = 8
KVLOC = 2
HD = 64
QC = HLOC * HD
KC = KVLOC * HD
QKV = QC + 2 * KC
GROUP = HLOC // KVLOC
SCALE = HD ** -0.5
NC = 4
W = DIM // NC
NE = 8
WE = DIM // NE
AHEAD = 4
NB2 = 2
WB = DIM // NB2
LAG = 1
VMEM = pltpu.VMEM
HBM = pltpu.HBM


def nn(a, b):
    return lax.dot_general(a, b, (((1,), (0,)), ((), ())), preferred_element_type=F32)


def nt(a, b):
    return lax.dot_general(a, b, (((1,), (1,)), ((), ())), preferred_element_type=F32)


def tn(a, b):
    return lax.dot_general(a, b, (((0,), (0,)), ((), ())), preferred_element_type=F32)


def place():
    tp = lax.axis_index("tp")
    x = tp // 2
    c = tp - 2 * x
    return x, c, 2 * x + (1 - c), 2 * (1 - x) + c


def greet(*peers):
    sem = pltpu.get_barrier_semaphore()
    for peer in peers:
        pl.semaphore_signal(sem, inc=1, device_id={"tp": peer}, device_id_type=MESH)
    return lambda: pl.semaphore_wait(sem, len(peers))


def remote(src, dst, send, recv, peer):
    return pltpu.make_async_remote_copy(
        src_ref=src, dst_ref=dst, send_sem=send, recv_sem=recv, device_id={"tp": peer}, device_id_type=MESH)


def cols(j, width=W):
    return pl.ds(pl.multiple_of(j * width, width), width)


def dma(*shape):
    return pltpu.SemaphoreType.DMA(shape)


class PairSum:
    def __init__(self, part, got, own, sems, c, partner, n=NC, base=0):
        self.part, self.got, self.own, self.c, self.partner = part, got, own, c, partner
        self.send, self.recv = sems
        self.n, self.width, self.base = n, DIM // n, base

    def copy(self, j):
        return remote(self.part.at[:, 1 - self.c, :, cols(j, self.width)], self.got.at[:, :, cols(j, self.width)],
                      self.send.at[self.base + j], self.recv.at[self.base + j], self.partner)

    def put(self, j, value):
        self.part[:, :, :, cols(j, self.width)] = value.astype(BF).reshape(2, 2, 32, self.width)
        self.copy(j).start()

    def take(self, j):
        self.copy(j).wait_recv()
        total = self.part[:, self.c, :, cols(j, self.width)].astype(F32) + self.got[:, :, cols(j, self.width)].astype(F32)
        self.own[0:2, :, cols(j, self.width)] = total.astype(BF)

    def send_all(self, chunk):
        def body(j, carry):
            self.put(j, chunk(j))
            return carry
        lax.fori_loop(0, self.n, body, 0)

    def run(self, chunk, then=lambda j: None, lag=None):
        lag = lag or self.n

        def finish(j):
            self.take(j)
            then(j)

        def body(j, carry):
            self.put(j, chunk(j))
            if lag < self.n:
                @pl.when(j >= lag)
                def _():
                    finish(j - lag)
            return carry
        lax.fori_loop(0, self.n, body, 0)
        for j in range(self.n - lag, self.n):
            finish(j)

    def drain(self):
        for j in range(self.n):
            self.copy(j).wait_send()


def rows16(fn):
    for b in range(2):
        for r in range(0, 32, 16):
            fn(b, slice(r, r + 16))


def norm_rows(x, gain):
    inv = lax.rsqrt(jnp.mean(x * x, axis=-1, keepdims=True) + RMS_EPS)
    return (x * inv * gain).astype(BF)


def norm_back(grad, x, gain):
    inv = lax.rsqrt(jnp.mean(x * x, axis=-1, keepdims=True) + RMS_EPS)
    normed = x * inv
    scaled = grad * gain
    back = inv * (scaled - normed * jnp.mean(scaled * normed, axis=-1, keepdims=True))
    return back, jnp.sum(grad * normed, axis=0, keepdims=True)


def spread(row):
    return jnp.transpose(jnp.broadcast_to(row, (SEQ, SEQ)))


def rope_pair(values, cos_tab, sin_tab):
    lane = lax.broadcasted_iota(jnp.int32, (SEQ, 128), 1)
    low = (lane % HD) < HD // 2
    other = jnp.where(low, pltpu.roll(values, 128 - HD // 2, 1), pltpu.roll(values, HD // 2, 1))
    return values * cos_tab + other * jnp.where(low, -sin_tab, sin_tab)


def stack(ref, g):
    return jnp.concatenate([ref[:, h * HD:(h + 1) * HD] for h in range(g * GROUP, (g + 1) * GROUP)], axis=0)


def unstack(ref, g, value, fix=lambda pair: pair):
    for i in range(0, GROUP, 2):
        lo = (g * GROUP + i) * HD
        pair = jnp.concatenate([value[i * SEQ:(i + 1) * SEQ], value[(i + 1) * SEQ:(i + 2) * SEQ]], axis=1)
        ref[:, lo:lo + 128] = fix(pair).astype(BF)


def probs_of(q, k):
    scores = nt(q, k) * SCALE
    shape = (GROUP * SEQ, SEQ)
    row = lax.broadcasted_iota(jnp.int32, shape, 0) % SEQ
    scores = jnp.where(row >= lax.broadcasted_iota(jnp.int32, shape, 1), scores, -1e30)
    e = jnp.exp(scores - jnp.max(scores, axis=-1, keepdims=True))
    return e / jnp.sum(e, axis=-1, keepdims=True)


def front_kernel(tok, pos, freq, gain_a, gain_m, gh, emb, wq, wk, wv, wo, wd, wg, wu,
                 n1_o, x0_o, qkv_o, cs_o, heads_o, h1_o, n2_o, act_o, ggate_o, gup_o, gfull_o, gn2_o,
                 wqkv_v, wo_v, wd_v,
                 tok_v, pos_v, freq_v, ga_v, gm_v, emb_v, wg_v, wu_v, wut_v, hot_v, gact_v,
                 p0, g0, s0, r0, p1, g1, s1, r1, p2, g2,
                 in_sem, emb_sem, w_sem, ps, pr, xs, xr, hs, hr):
    x, c, partner, cross = place()
    tp = 2 * x + c

    def fetch_emb(j):
        return pltpu.make_async_copy(emb.at[:, cols(j, WE)], emb_v.at[:, cols(j, WE)], emb_sem.at[j])

    get_q = pltpu.make_async_copy(wq, wqkv_v.at[pl.ds(0, QC)], w_sem.at[0])
    get_k = pltpu.make_async_copy(wk, wqkv_v.at[pl.ds(QC, KC)], w_sem.at[1])
    get_v = pltpu.make_async_copy(wv, wqkv_v.at[pl.ds(QC + KC, KC)], w_sem.at[2])
    get_out = pltpu.make_async_copy(wo, wo_v, emb_sem.at[0])
    get_down = pltpu.make_async_copy(wd, wd_v, emb_sem.at[1])
    get_gate = pltpu.make_async_copy(wg, wg_v, emb_sem.at[2])
    get_up = pltpu.make_async_copy(wu, wu_v, emb_sem.at[3])
    get_small = [pltpu.make_async_copy(src, dst, in_sem.at[i]) for i, (src, dst) in enumerate(
        ((tok, tok_v), (pos, pos_v), (freq, freq_v), (gain_a, ga_v), (gain_m, gm_v), (gh, gfull_o.at[x, c])))]
    get_small[0].start()
    for j in range(AHEAD):
        fetch_emb(j).start()
    for g in get_small[1:]:
        g.start()
    met = greet(partner, cross)
    get_small[0].wait()
    ids = spread(tok_v[...].astype(F32))
    base = (tp * VLOC).astype(F32)
    lane = lax.broadcasted_iota(jnp.int32, (SEQ, 128), 1).astype(F32)
    for v in range(VLOC // 128):
        hot_v[:, v * 128:(v + 1) * 128] = jnp.where(ids == lane + (base + float(v * 128)), 1.0, 0.0).astype(BF)

    met()

    def cross_copy(k, src, dst, j):
        cj = cols(j, WE if k == 0 else W)
        return remote(src.at[:, :, cj], dst.at[:, :, cj], xs.at[k * NE + j], xr.at[k * NE + j], cross)

    sum0 = PairSum(p0, g0, s0, (ps, pr), c, partner, NE)

    def lookup(j):
        fetch_emb(j).wait()

        @pl.when(j + AHEAD < NE)
        def _():
            fetch_emb(j + AHEAD).start()

        @pl.when(j == NE - AHEAD)
        def _():
            for g in (get_q, get_k, get_v):
                g.start()
        return nn(hot_v[...], emb_v[:, cols(j, WE)])

    sum0.run(lookup, lambda j: cross_copy(0, s0, r0, j).start(), LAG)
    for g in (get_out, get_up, get_down, get_gate):
        g.start()
    for g in get_small[1:]:
        g.wait()
    mine = gfull_o.at[x, c]
    to_cross = remote(mine, mine, hs.at[0], hr.at[0], cross)
    to_partner = remote(mine, mine, hs.at[1], hr.at[1], partner)
    to_partner.start()
    angle = spread(pos_v[...].astype(F32)) * freq_v[...]
    cs_o[0] = jnp.cos(angle)
    cs_o[1] = jnp.sin(angle)

    wqkvt_v = wut_v
    for g in (get_q, get_k, get_v):
        g.wait()

    def turn_qkv(j, carry):
        rj = pl.ds(pl.multiple_of(j * 256, 256), 256)
        wqkvt_v[:, rj] = jnp.transpose(wqkv_v[rj, :])
        return carry
    lax.fori_loop(0, QKV // 256, turn_qkv, 0)

    for j in range(NE):
        cross_copy(0, s0, r0, j).wait_recv()

    to_cross.start()

    def first(b, r):
        xv = s0[b, r].astype(F32) + r0[b, r].astype(F32)
        x0_o[b, r] = xv.astype(BF)
        n1_o[b, c, r] = norm_rows(xv, ga_v[...])
    rows16(first)
    share1 = remote(n1_o.at[:, c], n1_o.at[:, c], hs.at[2], hr.at[2], partner)
    share1.start()
    share1.wait_recv()

    n1 = n1_o[...].reshape(SEQ, DIM)
    cos_tab, sin_tab = cs_o[0], cs_o[1]

    lin = nn(n1, wqkvt_v[:, 0:QKV])
    for lo in range(0, QKV, 128):
        piece = lin[:, lo:lo + 128]
        if lo < QC + KC:
            piece = rope_pair(piece, cos_tab, sin_tab)
        qkv_o[:, lo:lo + 128] = piece.astype(BF)
    for g in range(KVLOC):
        k = qkv_o[:, QC + g * HD:QC + (g + 1) * HD]
        v = qkv_o[:, QC + KC + g * HD:QC + KC + (g + 1) * HD]
        unstack(heads_o, g, nn(probs_of(stack(qkv_o, g), k).astype(BF), v).astype(BF))
    get_out.wait()

    sum0.drain()
    sum1 = PairSum(p1, g1, s1, (ps, pr), c, partner)
    sum1.run(lambda j: nn(heads_o[...], wo_v[:, cols(j)]), lambda j: cross_copy(1, s1, r1, j).start())

    to_cross.wait_recv()
    onward = remote(gfull_o.at[1 - x, c], gfull_o.at[1 - x, c], hs.at[3], hr.at[3], partner)
    onward.start()
    get_up.wait()

    def turn_up(j, carry):
        wut_v[:, cols(j, WB)] = jnp.transpose(wu_v[cols(j, WB), :])
        return carry
    lax.fori_loop(0, NB2, turn_up, 0)

    to_partner.wait_recv()
    onward.wait_recv()
    get_down.wait()
    get_gate.wait()
    gfull = gfull_o[...].reshape(SEQ, DIM)
    wgt_v = emb_v

    def grad_act(j, carry):
        gact_v[:, cols(j, WB)] = nt(gfull, wd_v[cols(j, WB), :]).astype(BF)
        wgt_v[:, cols(j, WB)] = jnp.transpose(wg_v[cols(j, WB), :])
        return carry
    lax.fori_loop(0, NB2, grad_act, 0)

    for j in range(NC):
        cross_copy(1, s1, r1, j).wait_recv()

    def second(b, r):
        total = s1[b, r].astype(F32) + r1[b, r].astype(F32)
        h1 = (x0_o[b, r].astype(F32) + total).astype(BF)
        h1_o[b, r] = h1
        n2_o[b, c, r] = norm_rows(h1.astype(F32), gm_v[...])
    rows16(second)
    share1.wait_send()
    share2 = remote(n2_o.at[:, c], n2_o.at[:, c], hs.at[2], hr.at[2], partner)
    share2.start()
    share2.wait_recv()
    n2 = n2_o[...].reshape(SEQ, DIM)

    gate = nn(n2, wg_v[...])
    up = nn(n2, wu_v[...])
    sig = jax.nn.sigmoid(gate)
    gate_act = gate * sig
    act_o[...] = (gate_act * up).astype(BF)
    grad = gact_v[...].astype(F32)
    gup_o[...] = (grad * gate_act).astype(BF)
    ggate_o[...] = (grad * up * sig * (1.0 + gate * (1.0 - sig))).astype(BF)

    sum1.drain()
    sum2 = PairSum(p2, g2, gn2_o, (ps, pr), c, partner, NB2)
    sum2.run(lambda j: nn(ggate_o[...], wgt_v[:, cols(j, WB)]) + nn(gup_o[...], wut_v[:, cols(j, WB)]))

    sum2.drain()
    for j in range(NE):
        cross_copy(0, s0, r0, j).wait_send()
    for j in range(NC):
        cross_copy(1, s1, r1, j).wait_send()
    for copy in (to_cross, to_partner, onward, share2):
        copy.wait_send()


def middle_kernel(gn2_own, gn2_got, part, h1, gfull, gain_m, qkv, cs, wqkv, wo, token,
                  gh1_o, gqkv_o, give_o, keep_o, gain_o,
                  gheads_v, probs_v, g0, s0, p1, g1, ps, pr, hs, hr):
    x, c, partner, cross = place()
    met = greet(partner)
    gains = []

    def first(b, r):
        grad = (gn2_own[b, r].astype(F32) + gn2_got[b, r].astype(F32)).astype(BF).astype(F32)
        back, part = norm_back(grad, h1[b, r].astype(F32), gain_m[...])
        gh1_o[b, c, r] = (gfull[b, c, r].astype(F32) + back).astype(BF)
        gains.append(part)
    rows16(first)
    met()
    share = remote(gh1_o.at[:, c], gh1_o.at[:, c], hs.at[0], hr.at[0], partner)
    share.start()
    gain_o[...] = gains[0] + gains[1] + gains[2] + gains[3]
    sum0 = PairSum(part, g0, s0, (ps, pr), c, partner, 1)
    sum0.copy(0).start()
    for g in range(KVLOC):
        probs_v[g] = probs_of(stack(qkv, g), qkv[:, QC + g * HD:QC + (g + 1) * HD])
    share.wait_recv()

    gh1 = gh1_o[...].reshape(SEQ, DIM)
    gheads_v[...] = nt(gh1, wo[...]).astype(BF)

    cos_tab, sin_tab = cs[0], -cs[1]
    turn_back = lambda pair: rope_pair(pair.astype(F32), cos_tab, sin_tab)
    gks, gvs = [], []
    for g in range(KVLOC):
        k = qkv[:, QC + g * HD:QC + (g + 1) * HD]
        v = qkv[:, QC + KC + g * HD:QC + KC + (g + 1) * HD]
        q, gh = stack(qkv, g), stack(gheads_v, g)
        probs = probs_v[g]
        gp = nt(gh, v).astype(BF).astype(F32)
        gvs.append(tn(probs.astype(BF), gh).astype(BF))
        gs = (probs * (gp - jnp.sum(gp * probs, axis=-1, keepdims=True)) * SCALE).astype(BF)
        gks.append(tn(gs, q).astype(BF).astype(F32))
        unstack(gqkv_o, g, nn(gs, k).astype(BF), turn_back)
    gqkv_o[:, QC:QC + KC] = rope_pair(jnp.concatenate(gks, axis=1), cos_tab, sin_tab).astype(BF)
    gqkv_o[:, QC + KC:] = jnp.concatenate(gvs, axis=1)

    sum1 = PairSum(p1, g1, give_o, (ps, pr), c, partner, NB2, 1)
    sum1.send_all(lambda j: nn(gqkv_o[...], wqkv[:, cols(j, WB)]))
    sum0.take(0)
    give_o[2] = s0[1 - x]
    keep_o[...] = s0[x]
    for j in range(NB2):
        sum1.take(j)
    sum0.drain()
    sum1.drain()
    share.wait_send()


def back_kernel(give, got, keep, h1, x0, gh1, gain_a, gain_mp, token, gx_o, gain_o, hid_o, gbuf, hs, hr):
    x, c, partner, cross = place()
    met = greet(partner)
    gains = []

    def first(b, r):
        grad = (give[b, r].astype(F32) + got[b, r].astype(F32)).astype(BF).astype(F32)
        back, part = norm_back(grad, x0[b, r].astype(F32), gain_a[...])
        gx_o[b, c, r] = (gh1[b, c, r].astype(F32) + back).astype(BF)
        gains.append(part)
    rows16(first)
    met()
    share = remote(gx_o.at[:, c], gx_o.at[:, c], hs.at[0], hr.at[0], partner)
    share.start()
    gbuf[c, 0:1] = gains[0] + gains[1] + gains[2] + gains[3]
    gbuf[c, 1:2] = gain_mp[...]
    share_gain = remote(gbuf.at[c], gbuf.at[c], hs.at[1], hr.at[1], partner)
    share_gain.start()
    hid_o[...] = (h1[x].astype(F32) + (keep[...].astype(F32) + got[2].astype(F32))).astype(BF)
    share_gain.wait_recv()
    gain_o[...] = gbuf[0, 0:2] + gbuf[1, 0:2]
    share.wait_recv()
    share.wait_send()
    share_gain.wait_send()


def vm(n):
    return [pl.BlockSpec(memory_space=VMEM)] * n


def hb(n):
    return [pl.BlockSpec(memory_space=HBM)] * n


def on(shape, dtype=BF):
    return pltpu.VMEM(shape, dtype)


NB = 5
BM = 256
UP_FIRST = 768
RAMP = ((0, 64), (64, 64), (128, 128))
EB = 256
ENB = 4


def outer_kernel(spec, n_in, n_held, side, *refs):
    n_out = 1 + max(o for _, _, _, o, _, _ in spec)
    ins, outs = refs[:n_in], refs[n_in + n_held:n_in + n_held + n_out]
    *part, token, buf, sem, ramp, ramp_sem = refs[n_in + n_held + n_out:]
    token[...] = jnp.zeros_like(token)
    done = 0
    flying = {}
    small = []
    for l, r, off, o, row, rows in spec:
        lhs, rhs, out = ins[l], ins[r], outs[o]
        if not small:
            for i, (lo, size) in enumerate(RAMP):
                ramp[lo:lo + size] = tn(lhs[:, off + lo:off + lo + size], rhs[...])
                small.append(pltpu.make_async_copy(
                    ramp.at[pl.ds(lo, size)], out.at[pl.ds(row + lo, size)], ramp_sem.at[i]))
                small[-1].start()
            off, row, rows = off + BM, row + BM, rows - BM
        bm = min(BM, rows)
        steps = rows // bm

        def copy(i, out=out, done=done, bm=bm, row=row):
            slot = lax.rem(i + done, NB)
            where = pl.ds(pl.multiple_of(row + i * bm, bm), bm)
            return pltpu.make_async_copy(buf.at[slot, pl.ds(0, bm)], out.at[where], sem.at[slot])

        def compute(i, lhs=lhs, rhs=rhs, off=off, done=done, bm=bm):
            a = lhs[:, pl.ds(pl.multiple_of(off + i * bm, 128), bm)]
            buf[lax.rem(i + done, NB), 0:bm] = tn(a, rhs[...])

        free = [(done + i) % NB for i in range(min(NB, steps))]
        uniform = steps >= NB and all(flying.get(k, bm) == bm for k in range(NB)) and (not flying or len(flying) == NB)
        if uniform:
            def step(i, carry, copy=copy, compute=compute, waiting=bool(flying)):
                if waiting:
                    copy(i).wait()
                else:
                    @pl.when(i >= NB)
                    def _():
                        copy(i).wait()
                compute(i)
                copy(i).start()
                return carry
            lax.fori_loop(0, steps, step, 0)
            flying = {k: bm for k in range(NB)}
        else:
            for i in range(steps):
                slot = (done + i) % NB
                if slot in flying:
                    size = flying[slot]
                    pltpu.make_async_copy(buf.at[slot, pl.ds(0, size)], outs[0].at[pl.ds(0, size)], sem.at[slot]).wait()
                compute(i)
                copy(i).start()
                flying[slot] = bm
        done += steps
        if side and done == steps:
            for j in range(NB2):
                lo, hi = j * WB, (j + 1) * WB
                out = nn(ins[side[0]][...], ins[side[1]][:, lo:hi])
                part[0][:, :, :, lo:hi] = out.astype(BF).reshape(2, 2, 32, WB)
    for copy in small:
        copy.wait()
    for slot, size in flying.items():
        pltpu.make_async_copy(buf.at[slot, pl.ds(0, size)], outs[0].at[pl.ds(0, size)], sem.at[slot]).wait()


def outer(ins, spec, rows, held=(), side=()):
    total = sum(n for *_, n in spec)
    extra = (on(FULL),) if side else ()
    return pl.pallas_call(
        functools.partial(outer_kernel, spec, len(ins), len(held), side),
        out_shape=tuple(jax.ShapeDtypeStruct((m, DIM), F32) for m in rows) + extra + (on((8, 128), F32),),
        in_specs=vm(len(ins)) + hb(len(held)),
        out_specs=tuple(hb(len(rows)) + vm(1 + len(extra))),
        scratch_shapes=[pltpu.VMEM((NB, BM, DIM), F32), dma(NB), pltpu.VMEM((BM, DIM), F32), dma(len(RAMP))],
        input_output_aliases={len(ins) + i: o for i, (_, o) in enumerate(held)},
        cost_estimate=pl.CostEstimate(flops=2 * total * DIM * SEQ, bytes_accessed=4 * total * DIM, transcendentals=0),
        compiler_params=pltpu.CompilerParams(vmem_limit_bytes=24 * 2 ** 20),
    )(*ins, *[h for h, _ in held])


def emb_kernel(tok, gx, gains, hid, out, ga_o, gm_o, hid_o, buf, sem, out_sem, ramp, ramp_sem):
    base = lax.axis_index("tp") * VLOC
    ids = jnp.broadcast_to(tok[...], (EB, SEQ)) - base
    row = lax.broadcasted_iota(jnp.int32, (EB, SEQ), 0)
    grad = gx[...].reshape(SEQ, DIM)

    small = []
    for i, (lo, size) in enumerate(RAMP):
        hot = jnp.where(ids[:size] == row[:size] + lo, 1.0, 0.0).astype(BF)
        ramp[lo:lo + size] = nn(hot, grad)
        small.append(pltpu.make_async_copy(ramp.at[pl.ds(lo, size)], out.at[pl.ds(lo, size)], ramp_sem.at[i]))
        small[-1].start()
    extra = (
        pltpu.make_async_copy(gains.at[pl.ds(0, 1)], ga_o, out_sem.at[0]),
        pltpu.make_async_copy(gains.at[pl.ds(1, 1)], gm_o, out_sem.at[1]),
        pltpu.make_async_copy(hid, hid_o, out_sem.at[2]),
    )
    for e in extra:
        e.start()

    def copy(i):
        slot = lax.rem(i - 1, ENB)
        return pltpu.make_async_copy(buf.at[slot], out.at[pl.ds(pl.multiple_of(i * EB, EB), EB)], sem.at[slot])

    def step(i, carry):
        @pl.when(i >= ENB + 1)
        def _():
            copy(i).wait()
        hot = jnp.where(ids == row + i * EB, 1.0, 0.0).astype(BF)
        buf[lax.rem(i - 1, ENB)] = nn(hot, grad)
        copy(i).start()
        return carry
    steps = VLOC // EB
    lax.fori_loop(1, steps, step, 0)
    for k in range(steps - ENB, steps):
        copy(k).wait()
    for e in (*small, *extra):
        e.wait()


def sds(shape, dtype=BF):
    return jax.ShapeDtypeStruct(shape, dtype)


FULL = (2, 2, 32, DIM)
MINE = (2, 32, DIM)


def device_fn(tokens, positions, emb, gain_a, gain_m, wq, wk, wv, wo, wg, wu, wd, gh):
    inv_freq = (ROPE_THETA ** (-np.arange(HD // 2, dtype=np.float32) * np.float32(2.0 / HD))).astype(np.float32)
    freq = jnp.asarray(np.tile(inv_freq, 4)[None, :])
    ga, gm = gain_a.reshape(1, DIM), gain_m.reshape(1, DIM)
    flat = lambda w: jnp.transpose(w, (1, 2, 0)).reshape(-1, DIM)
    wqt, wkt, wvt = flat(wq), flat(wk), flat(wv)
    wo2 = wo.reshape(QC, DIM)
    gh2 = gh.reshape(32, DIM)

    n1, x0, qkv, cs, heads, h1, n2, act, ggate, gup, gfull, gn2, wqkv_v, wo_v, wd_v = pl.pallas_call(
        front_kernel,
        out_shape=(on(FULL), on(MINE), on((SEQ, QKV)), on((2, SEQ, 128), F32), on((SEQ, QC)), on(MINE),
                   on(FULL), on((SEQ, FLOC)), on((SEQ, FLOC)), on((SEQ, FLOC)), on(FULL), on(MINE),
                   on((QKV, DIM)), on((QC, DIM)), on((FLOC, DIM))),
        in_specs=hb(14),
        out_specs=tuple(vm(15)),
        scratch_shapes=[
            pltpu.VMEM((1, SEQ), jnp.int32), pltpu.VMEM((1, SEQ), jnp.int32), pltpu.VMEM((1, SEQ), F32),
            pltpu.VMEM((1, DIM), F32), pltpu.VMEM((1, DIM), F32),
            pltpu.VMEM((VLOC, DIM), BF), pltpu.VMEM((DIM, FLOC), BF), pltpu.VMEM((DIM, FLOC), BF),
            pltpu.VMEM((FLOC, DIM), BF),
            pltpu.VMEM((SEQ, VLOC), BF), pltpu.VMEM((SEQ, FLOC), BF),
            pltpu.VMEM(FULL, BF), pltpu.VMEM(MINE, BF), pltpu.VMEM(MINE, BF), pltpu.VMEM(MINE, BF),
            pltpu.VMEM(FULL, BF), pltpu.VMEM(MINE, BF), pltpu.VMEM(MINE, BF), pltpu.VMEM(MINE, BF),
            pltpu.VMEM(FULL, BF), pltpu.VMEM(MINE, BF),
            dma(6), dma(NE), dma(3), dma(NE), dma(NE), dma(NE + NC), dma(NE + NC), dma(4), dma(4)],
        compiler_params=pltpu.CompilerParams(collective_id=0, has_side_effects=True, vmem_limit_bytes=44 * 2 ** 20),
    )(tokens, positions, freq, ga, gm, gh2, emb, wqt, wkt, wvt, wo2, wd, wg, wu)

    swap = [(i, i ^ 2) for i in range(4)]
    gn2_got = lax.ppermute(gn2, 'tp', swap)
    gfull2 = gfull.reshape(SEQ, DIM)
    n2f = n2.reshape(SEQ, DIM)
    g_gate, g_up, part, token = outer(
        (n2f, ggate, gup, act, wd_v), ((0, 1, 0, 0, 0, DIM), (0, 2, 0, 1, 0, UP_FIRST)), (DIM, DIM), side=(3, 4))

    gh1, gqkv, give, keep, gain_mp = pl.pallas_call(
        middle_kernel,
        out_shape=(on(FULL), on((SEQ, QKV)), on((3, 32, DIM)), on((32, DIM)), on((1, DIM), F32)),
        in_specs=vm(11),
        out_specs=tuple(vm(5)),
        scratch_shapes=[
            pltpu.VMEM((SEQ, QC), BF), pltpu.VMEM((KVLOC, GROUP * SEQ, SEQ), F32),
            pltpu.VMEM(MINE, BF), pltpu.VMEM(MINE, BF), pltpu.VMEM(FULL, BF), pltpu.VMEM(MINE, BF),
            dma(1 + NB2), dma(1 + NB2), dma(1), dma(1)],
        compiler_params=pltpu.CompilerParams(collective_id=1, has_side_effects=True, vmem_limit_bytes=8 * 2 ** 20),
    )(gn2, gn2_got, part, h1, gfull, gm, qkv, cs, wqkv_v, wo_v, token)

    got = lax.ppermute(give, 'tp', swap)
    g_up, g_down, g_out, g_q, g_k, g_v, token2 = outer(
        (n2f, gup, act, gfull2, heads, gh1.reshape(SEQ, DIM), gqkv, n1.reshape(SEQ, DIM)),
        ((0, 1, UP_FIRST, 0, UP_FIRST, DIM - UP_FIRST), (2, 3, 0, 1, 0, FLOC), (4, 5, 0, 2, 0, QC),
         (6, 7, 0, 3, 0, QC), (6, 7, QC, 4, 0, KC), (6, 7, QC + KC, 5, 0, KC)),
        (DIM, FLOC, QC, QC, KC, KC), ((g_up, 0),))

    gx, gains, hid = pl.pallas_call(
        back_kernel,
        out_shape=(on(FULL), on((2, DIM), F32), on((32, DIM))),
        in_specs=vm(9),
        out_specs=tuple(vm(3)),
        scratch_shapes=[pltpu.VMEM((2, 8, DIM), F32), dma(2), dma(2)],
        compiler_params=pltpu.CompilerParams(collective_id=2, has_side_effects=True, vmem_limit_bytes=8 * 2 ** 20),
    )(give, got, keep, h1, x0, gh1, ga, gain_mp, token2)

    g_emb, gain_1, gain_2, hidden = pl.pallas_call(
        emb_kernel,
        out_shape=(sds((VLOC, DIM), F32), sds((1, DIM), F32), sds((1, DIM), F32), sds((32, DIM))),
        in_specs=vm(4),
        out_specs=tuple(hb(4)),
        scratch_shapes=[pltpu.VMEM((ENB, EB, DIM), F32), dma(ENB), dma(3), pltpu.VMEM((EB, DIM), F32), dma(len(RAMP))],
        compiler_params=pltpu.CompilerParams(vmem_limit_bytes=24 * 2 ** 20),
    )(tokens, gx, gains, hid)

    back3 = lambda g: jnp.transpose(g.reshape(-1, HD, DIM), (2, 0, 1))
    return (hidden.reshape(1, 32, DIM), g_emb, back3(g_q), back3(g_k), back3(g_v), g_out.reshape(HLOC, HD, DIM),
            g_gate, g_up, g_down, gain_1.reshape(DIM), gain_2.reshape(DIM))


def solution(mesh):
    in_specs = (P('dp', None), P('dp', None), P('tp', None), P(None), P(None),
                P(None, 'tp', None), P(None, 'tp', None), P(None, 'tp', None), P('tp', None, None),
                P(None, 'tp'), P(None, 'tp'), P('tp', None), P('dp', 'tp', None))
    out_specs = (P('dp', 'tp', None), P(('dp', 'tp'), None),
                 P('dp', 'tp', None), P('dp', 'tp', None), P('dp', 'tp', None), P(('dp', 'tp'), None, None),
                 P('dp', 'tp'), P('dp', 'tp'), P(('dp', 'tp'), None), P('dp'), P('dp'))
    return jax.shard_map(device_fn, mesh=mesh, in_specs=in_specs, out_specs=out_specs, check_vma=False)
```
